32 devices in a mesh: rows: 16 (over z, x, core), feat: 2 (over y).
Axes of the slice: x: 2, y: 2, z: 4, core: 2. Of those that a mesh axis runs over, the one named last changes fastest.
Arguments:
- train_cells: bfloat16 [1024, 1536], P('rows', 'feat'), may hold values from -24 to 24
- test_cells: bfloat16 [512, 1536], P('rows', 'feat'), may hold values from -24 to 24
- feat_weights: bfloat16 [4, 192, 192], replicated
- row_weights: bfloat16 [4, 192, 192], replicated
- mlp_up: bfloat16 [192, 768], replicated, may hold values from -0.4375 to 0.4375
- mlp_down: bfloat16 [768, 192], replicated, may hold values from -0.21875 to 0.21875
Outputs:
- train_out: bfloat16 [1024, 1536], P('rows', 'feat')
- test_out: bfloat16 [512, 1536], P('rows', 'feat')
The draws below stay inside these ranges and needn't reach their ends.
All inputs are finite; a program needn't handle non-finite values.
Results may differ from the reference program's by a relative error of at most 0.017.
Values may be sent and summed in bfloat16 or wider, within the bound.
A program may use at most 128 MiB of HBM per device.

```python
import math
import jax
import jax.numpy as jnp
from jax import lax

E = 192
HEADS = 6
HD = 32
HID = 768
F = 8
TRAIN = 1024
TEST = 512


def attention_weights(key, query_gain):
    split_keys = jax.random.split(key, 4)
    spread = E ** (-0.5)
    query_w = jax.random.normal(split_keys[0], (E, E), jnp.float32) * query_gain * spread
    key_w = jax.random.normal(split_keys[1], (E, E), jnp.float32) * spread
    value_w = jax.random.normal(split_keys[2], (E, E), jnp.float32) * spread
    output_w = jax.random.normal(split_keys[3], (E, E), jnp.float32) * spread
    return jnp.stack([query_w, key_w, value_w, output_w]).astype(jnp.bfloat16)


def draw_feat_weights(key, part):
    return attention_weights(jax.random.fold_in(key, 3), 1.5)


def draw_row_weights(key, part):
    return attention_weights(jax.random.fold_in(key, 5), 2.5)


def train_table(key):
    key_base = jax.random.fold_in(key, 0)
    table = jax.random.normal(key_base, (TRAIN, F, E), jnp.float32)
    return jnp.clip(table, -24.0, 24.0)


def draw_train_cells(key, part):
    return train_table(jax.random.fold_in(key, 11)).reshape(TRAIN, F * E).astype(jnp.bfloat16)


def draw_test_cells(key, part):
    fresh = jax.random.normal(jax.random.fold_in(key, 13), (TEST, F, E), jnp.float32)
    return jnp.clip(fresh, -24.0, 24.0).reshape(TEST, F * E).astype(jnp.bfloat16)


def bell_draw(key, dims, scale, limit, kind=jnp.bfloat16):
    values = scale * jax.random.normal(key, dims, jnp.float32)
    return jnp.clip(values, min=-limit, max=limit).astype(kind)


def setup_inputs(seed: int = 0) -> dict:
    key_list = jax.random.split(jax.random.key(seed), 7)
    train_cells = draw_train_cells(jax.random.fold_in(key_list[6], 71), 0)
    test_cells = draw_test_cells(jax.random.fold_in(key_list[6], 71), 0)
    feat_weights = draw_feat_weights(jax.random.fold_in(key_list[6], 71), 0)
    row_weights = draw_row_weights(jax.random.fold_in(key_list[6], 71), 0)
    mlp_up = bell_draw(key_list[4], (E, HID), E ** -0.5, 0.4375)
    mlp_down = bell_draw(key_list[5], (HID, E), HID ** -0.5, 0.21875)
    return dict(train_cells=train_cells, test_cells=test_cells, feat_weights=feat_weights, row_weights=row_weights, mlp_up=mlp_up, mlp_down=mlp_down)


eps_norm = 1e-05

def layer_norm(values_in):
    centred = values_in - lax.optimization_barrier(jnp.mean(values_in, axis=-1, keepdims=True))
    spread = lax.optimization_barrier(jnp.mean(centred * centred, axis=-1, keepdims=True))
    return centred * lax.rsqrt(spread + eps_norm)

def project(normed, weight):
    return jnp.dot(normed.reshape(-1, E), weight, preferred_element_type=jnp.float32)

def round_back(values_in):
    return lax.optimization_barrier(values_in.astype(jnp.bfloat16)).astype(jnp.float32)

def feature_attention(queries, key_heads, value_heads):
    scores = jnp.einsum('rqhd,rkhd->rhqk', queries.astype(jnp.float32), key_heads.astype(jnp.float32)) * HD ** (-0.5)
    row_peak = lax.optimization_barrier(jnp.max(scores, axis=-1, keepdims=True))
    weights = jnp.exp(scores - row_peak)
    totals = lax.optimization_barrier(jnp.sum(weights, axis=-1))
    mixture = jnp.einsum('rhqk,rkhd->rqhd', round_back(weights), value_heads.astype(jnp.float32))
    return (mixture / jnp.transpose(totals, (0, 2, 1))[..., None]).astype(jnp.bfloat16)

def row_attention(queries, key_heads, value_heads):
    total_rows = queries.shape[0]
    block_rows = math.gcd(total_rows, 1024)
    query_feat = jnp.transpose(queries, (1, 0, 2, 3)).reshape(F, total_rows // block_rows, block_rows, HEADS, HD)
    key_feat = jnp.transpose(key_heads, (1, 0, 2, 3))
    value_feat = jnp.transpose(value_heads, (1, 0, 2, 3))

    def one_feature(inputs):
        query_blocks, key_one, value_one = inputs
        key_float = key_one.astype(jnp.float32)
        value_float = value_one.astype(jnp.float32)

        def one_block(query_block):
            scores = jnp.einsum('qhd,khd->hqk', query_block.astype(jnp.float32), key_float) * HD ** (-0.5)
            row_peak = lax.optimization_barrier(jnp.max(scores, axis=-1, keepdims=True))
            weights = jnp.exp(scores - row_peak)
            totals = lax.optimization_barrier(jnp.sum(weights, axis=-1))
            mixture = jnp.einsum('hqk,khd->qhd', round_back(weights), value_float)
            return (mixture / jnp.transpose(totals)[..., None]).astype(jnp.bfloat16)
        return lax.map(one_block, query_blocks).reshape(total_rows, HEADS, HD)
    mixture = lax.map(one_feature, (query_feat, key_feat, value_feat))
    return jnp.transpose(mixture, (1, 0, 2, 3))

def reference(train_cells, test_cells, feat_weights, row_weights, mlp_up, mlp_down):
    joined = jnp.concatenate([train_cells, test_cells], axis=0)
    height = joined.shape[0]
    start_cells = joined.astype(jnp.float32).reshape(height, F, E)
    normed_one = layer_norm(start_cells).astype(jnp.bfloat16)
    feat_query = project(normed_one, feat_weights[0]).astype(jnp.bfloat16).reshape(height, F, HEADS, HD)
    feat_key = project(normed_one, feat_weights[1]).astype(jnp.bfloat16).reshape(height, F, HEADS, HD)
    feat_value = project(normed_one, feat_weights[2]).astype(jnp.bfloat16).reshape(height, F, HEADS, HD)
    feat_mix = feature_attention(feat_query, feat_key, feat_value)
    feat_out = project(feat_mix, feat_weights[3]).astype(jnp.bfloat16).reshape(height, F, E)
    after_feat = start_cells + feat_out.astype(jnp.float32)
    normed_two = layer_norm(after_feat).astype(jnp.bfloat16)
    row_query = project(normed_two, row_weights[0]).astype(jnp.bfloat16).reshape(height, F, HEADS, HD)
    train_normed = normed_two[:TRAIN]
    row_key = project(train_normed, row_weights[1]).astype(jnp.bfloat16).reshape(TRAIN, F, HEADS, HD)
    row_value = project(train_normed, row_weights[2]).astype(jnp.bfloat16).reshape(TRAIN, F, HEADS, HD)
    row_mix = row_attention(row_query, row_key, row_value)
    after_row = after_feat + project(row_mix, row_weights[3]).reshape(height, F, E)
    normed_three = layer_norm(after_row).astype(jnp.bfloat16)
    hidden = jax.nn.gelu(jnp.dot(normed_three.reshape(-1, E), mlp_up, preferred_element_type=jnp.float32), approximate=False).astype(jnp.bfloat16)
    lowered = jnp.dot(hidden, mlp_down, preferred_element_type=jnp.float32).reshape(height, F, E)
    result = (after_row + lowered).astype(jnp.bfloat16).reshape(height, F * E)
    return (result[:TRAIN], result[TRAIN:])
```

```python
import functools

import jax
import jax.numpy as jnp
from jax import lax
from jax.experimental import pallas as pl
from jax.experimental.pallas import tpu as pltpu
from jax.sharding import PartitionSpec as P

HD = 32
EPS = 1e-05
LOG2E = 1.4426950408889634
MESH = pl.DeviceIdType.MESH
BF = jnp.bfloat16
F32 = jnp.float32


def layer_norm(x):
    centred = x - jnp.mean(x, axis=-1, keepdims=True)
    spread = jnp.mean(centred * centred, axis=-1, keepdims=True)
    return centred * lax.rsqrt(spread + EPS)


def dot(a, b):
    return jnp.dot(a, b, preferred_element_type=F32)


def dot_t(a, b):
    return lax.dot_general(a, b, (((1,), (1,)), ((), ())), preferred_element_type=F32)


def pack(x):
    n = x.shape[0]
    low = jnp.concatenate([x[: n // 2, 128:], x[n // 2 :, 128:]], axis=1)
    return jnp.concatenate([x[:, :128], low], axis=0)


def unpack(p):
    n = p.shape[0] * 2 // 3
    low = p[n:]
    high = jnp.concatenate([low[:, :64], low[:, 64:]], axis=0)
    return jnp.concatenate([p[:n], high], axis=1)


def gelu(x):
    return 0.5 * x * (1.0 + lax.erf(x * (0.5**0.5)))


def kernel(
    rows_n,
    feats_n,
    train_hbm,
    test_hbm,
    fw_hbm,
    rw_hbm,
    up_hbm,
    down_hbm,
    back_in,
    fw,
    rw,
    up,
    down,
    train_ref,
    test_ref,
    o_train,
    o_test,
    outbox,
    inbox,
    t_outbox,
    t_inbox,
    ring,
    scores,
    values,
    queries,
    back_out,
    w_sem,
    f_send,
    f_recv,
    q_send,
    q_recv,
    r_send,
    r_recv,
    b_send,
    b_recv,
):
    width = fw.shape[-1]
    quad = t_outbox.shape[0]
    heads = width // HD
    groups_n = rows_n // quad
    half = groups_n // 2
    n_train = train_ref.shape[0]
    n_test = test_ref.shape[0]
    n_half = n_train // 2
    scale = LOG2E * HD ** (-0.5)

    my_row = lax.axis_index("rows")
    my_feat = lax.axis_index("feat")
    member = lax.rem(my_row, quad)
    group = my_row // quad

    def partner(k):
        low, high = lax.rem(member, 2), member // 2
        return (1 - high if k // 2 else high) * 2 + (1 - low if k % 2 else low)

    def mate(k):
        return group * quad + partner(k)

    right = lax.rem(group + 1, groups_n) * quad + member
    left = lax.rem(group + groups_n - 1, groups_n) * quad + member
    other = lax.rem(my_feat + 1, feats_n)

    loads = [
        pltpu.make_async_copy(s, d, w_sem.at[i])
        for i, (s, d) in enumerate(
            [
                (train_hbm, train_ref),
                (fw_hbm, fw),
                (test_hbm, test_ref),
                (rw_hbm, rw),
                (up_hbm, up),
                (down_hbm, down),
            ]
        )
    ]
    for c in loads:
        c.start()

    barrier = pltpu.get_barrier_semaphore()
    pl.semaphore_signal(barrier, inc=1, device_id={"feat": other}, device_id_type=MESH)
    for k in range(1, quad):
        pl.semaphore_signal(barrier, inc=1, device_id={"rows": mate(k)}, device_id_type=MESH)
    for d in (right, left):
        pl.semaphore_signal(barrier, inc=1, device_id={"rows": d}, device_id_type=MESH)
    pl.semaphore_wait(barrier, quad + 2)

    halves = [pl.ds(p * n_half, n_half) for p in range(2)]
    swaps = [
        pltpu.make_async_remote_copy(
            src_ref=s,
            dst_ref=d,
            send_sem=f_send.at[i],
            recv_sem=f_recv.at[i],
            device_id={"feat": other},
            device_id_type=MESH,
        )
        for i, (s, d) in enumerate(
            [(train_hbm.at[r], o_train.at[r]) for r in halves] + [(test_hbm, o_test)]
        )
    ]
    for c in swaps:
        c.start()

    def feature_rows(table):
        return jnp.concatenate(
            [table[:, f * width : (f + 1) * width].astype(F32) for f in range(quad)], axis=0
        )

    def split(x):
        n = x.shape[0] // quad
        return [x[f * n : (f + 1) * n] for f in range(quad)]

    def key_value(normed):
        return split(dot(normed, fw[1]).astype(BF)), split(dot(normed, fw[2]).astype(BF))

    same = (
        lax.broadcasted_iota(jnp.int32, (width, width), 0) // HD
        == lax.broadcasted_iota(jnp.int32, (width, width), 1) // HD
    )
    spread = jnp.where(same, 1.0, 0.0).astype(BF)

    def own_side(table):
        cells = feature_rows(table)
        normed = layer_norm(cells).astype(BF)
        q = split((dot(normed, fw[0]) * scale).astype(BF))
        ks, vs = key_value(normed)
        return cells, q, ks, vs

    def feature_attention(own, table):
        cells, q, ks, vs = own
        n = table.shape[0]
        more_k, more_v = key_value(layer_norm(feature_rows(table)).astype(BF))
        ks, vs = ks + more_k, vs + more_v
        mixes = []
        for f in range(quad):
            prod = jnp.concatenate([q[f] * k for k in ks], axis=0)
            s = dot(prod, spread)
            s = [s[g * n : (g + 1) * n] for g in range(len(ks))]
            top = functools.reduce(jnp.maximum, s)
            total = None
            mix = None
            for g in range(len(ks)):
                e = jnp.exp2(s[g] - top)
                t = e * vs[g].astype(F32)
                total = e if total is None else total + e
                mix = t if mix is None else mix + t
            mixes.append((mix / total).astype(BF))
        feat_out = dot(jnp.concatenate(mixes, axis=0), fw[3])
        return split((cells + feat_out).astype(BF))

    def to_mates(box, landing, stage):
        copies = {}
        for k in (2, 3, 1):
            copies[k] = pltpu.make_async_remote_copy(
                src_ref=box.at[partner(k)],
                dst_ref=landing.at[k],
                send_sem=q_send.at[stage, k],
                recv_sem=q_recv.at[stage, k],
                device_id={"rows": mate(k)},
                device_id_type=MESH,
            )
            copies[k].start()
        landing[0] = box[member]
        return copies

    loads[0].wait()
    loads[1].wait()
    own = [own_side(train_ref[p * n_half : (p + 1) * n_half]) for p in range(2)]
    moved = []
    boxes = [(outbox.at[p], inbox.at[p]) for p in range(2)] + [(t_outbox, t_inbox)]
    for p in range(2):
        swaps[p].wait()
        for f, x in enumerate(feature_attention(own[p], o_train[p * n_half : (p + 1) * n_half])):
            outbox[p, f] = pack(x)
        moved.append(to_mates(*boxes[p], p))
    loads[2].wait()
    own_test = own_side(test_ref[...])
    swaps[2].wait()
    for f, x in enumerate(feature_attention(own_test, o_test[...])):
        t_outbox[f] = pack(x)
    moved.append(to_mates(*boxes[2], 2))

    def hop(way, h, p):
        last = h == half - 1
        src = 0 if h == 0 else 2 * h - 1 + way
        dst = 2 * half - 1 if last else 1 + 2 * h + way
        return pltpu.make_async_remote_copy(
            src_ref=ring.at[src, p],
            dst_ref=ring.at[dst, p],
            send_sem=r_send.at[way, h, p],
            recv_sem=r_recv.at[way, h, p],
            device_id={"rows": left if way else right},
            device_id_type=MESH,
        )

    def pieces(way, h):
        return (way,) if h == half - 1 else (way, 1 - way)

    hops = {}
    after = []
    normed = []

    def arrive(stage):
        for k in range(1, quad):
            moved[stage][k].wait_recv()
        landing = boxes[stage][1]
        after.append(
            jnp.concatenate([unpack(landing[k]) for k in range(quad)], axis=0).astype(F32)
        )
        normed.append(layer_norm(after[stage]).astype(BF))

    for p in range(2):
        arrive(p)
        ring[0, p] = pack(normed[p])
        for way in (p, 1 - p):
            if p in pieces(way, 0):
                hops[way, 0, p] = hop(way, 0, p)
                hops[way, 0, p].start()

    loads[3].wait()
    lane_head = lax.broadcasted_iota(jnp.int32, (1, width), 1) // HD
    n_query = quad * (n_train + n_test)
    n_side = n_query // 2
    sizes = [2 * n_half, 2 * n_half, 2 * n_test]
    begins = [0, 2 * n_half, 4 * n_half]
    all_rows = [slice(0, n_query)]
    train_rows = [slice(i * n_side, i * n_side + begins[2]) for i in range(2)]
    test_rows = [slice(i * n_side + begins[2], (i + 1) * n_side) for i in range(2)]
    span = quad * n_train
    values[:, width:] = jnp.ones_like(values[:, width:])

    def ask(stage):
        q_all = (dot(normed[stage], rw[0]) * scale).astype(BF)
        n = sizes[stage]
        for h in range(heads):
            one = jnp.where(lane_head == h, q_all, jnp.zeros_like(q_all))
            for i in range(2):
                at = i * n_side + begins[stage]
                queries[h, at : at + n] = one[(1 - i) * n : (2 - i) * n]

    def take(slot, column):
        x = jnp.concatenate([unpack(ring[slot, 0]), unpack(ring[slot, 1])], axis=0)
        values[column * span : (column + 1) * span, :width] = dot(x, rw[2]).astype(BF)
        return dot(x, rw[1]).astype(BF)

    def score(key, column, rows):
        for h in range(heads):
            for r in rows:
                scores[h, r, column * span : (column + 1) * span] = dot_t(queries[h, r], key)

    def attend(h, rows, columns, carried):
        s = scores[h, rows, columns]
        top = jnp.max(s, axis=-1, keepdims=True)
        if carried is not None:
            top = jnp.maximum(top, carried[0])
        e = jnp.exp2(s - top).astype(BF)
        out = dot(e, values[columns])
        if carried is not None:
            out = out + carried[1] * jnp.exp2(carried[0] - top)
        return top, out

    ask(0)
    ask(1)
    everything = slice(0, n_query)
    if half <= 2:
        own_key = take(0, 0)
        score(own_key, 0, train_rows)
    arrive(2)
    ask(2)
    if half <= 2:
        score(own_key, 0, test_rows)
        states = [attend(h, everything, slice(0, span), None) for h in range(heads)]

    for h in range(half - 1):
        for way in range(2):
            for p in pieces(way, h + 1):
                hops[way, h, p].wait_recv()
                hops[way, h + 1, p] = hop(way, h + 1, p)
                hops[way, h + 1, p].start()
        for way in range(2):
            for p in pieces(way, h):
                if p not in pieces(way, h + 1):
                    hops[way, h, p].wait_recv()

    if half == 2:
        for slot in (1, 2):
            score(take(slot, slot), slot, all_rows)
        states = [
            attend(h, everything, slice(span, 3 * span), states[h]) for h in range(heads)
        ]

    for way in range(2):
        for p in pieces(way, half - 1):
            hops[way, half - 1, p].wait_recv()

    if half <= 2:
        last = 2 * half - 1
        last_key = take(last, last)
        columns = slice(last * span, (last + 1) * span)
    else:
        per = scores.shape[2] // span

        def step(i, states):
            for j in range(per):
                score(take(i * per + j, j), j, all_rows)
            return [attend(h, everything, slice(0, per * span), states[h]) for h in range(heads)]

        start = [
            (
                jnp.full((n_query, 1), -1e30, F32),
                jnp.zeros((n_query, values.shape[1]), F32),
            )
            for _ in range(heads)
        ]
        states = lax.fori_loop(0, groups_n // per, step, start)

    for c in loads[4:]:
        c.wait()
    returns = []
    for i, pair in enumerate(((2, 3), (0, 1))):
        rows = slice(i * n_side, (i + 1) * n_side)
        side = [tuple(x[rows] for x in states[h]) for h in range(heads)]
        if half <= 2:
            score(last_key, last, [rows])
            side = [attend(h, rows, columns, side[h]) for h in range(heads)]
        mixed = None
        for h in range(heads):
            out = side[h][1]
            part = out[:, :width] * (1.0 / out[:, width : width + 1])
            mixed = part if h == 0 else jnp.where(lane_head == h, part, mixed)
        before = [x[(1 - i) * n : (2 - i) * n] for x, n in zip(after, sizes)]
        after_row = jnp.concatenate(before, axis=0) + dot(mixed.astype(BF), rw[3])
        hidden = gelu(dot(layer_norm(after_row).astype(BF), up[...])).astype(BF)
        done = (after_row + dot_t(hidden, down[...])).astype(BF)
        for j, k in enumerate(pair):
            block = pack(
                jnp.concatenate(
                    [
                        done[b + j * (n // 2) : b + (j + 1) * (n // 2)]
                        for b, n in zip(begins, sizes)
                    ],
                    axis=0,
                )
            )
            back_out[k] = block
            if k == 0:
                c = pltpu.make_async_copy(back_out.at[0], back_in.at[member], b_send.at[0])
                c.start()
                returns.append(c)
                continue
            c = pltpu.make_async_remote_copy(
                src_ref=back_out.at[k],
                dst_ref=back_in.at[member],
                send_sem=b_send.at[k],
                recv_sem=b_recv.at[k],
                device_id={"rows": mate(k)},
                device_id_type=MESH,
            )
            c.start()
            returns.append(c)
    for c in returns:
        c.wait()
    for c in [*hops.values(), *(c for m in moved for c in m.values())]:
        c.wait_send()


def unpack_blocks(p):
    n = p.shape[1] * 2 // 3
    count = p.shape[0]
    low = p[:, n:]
    high = jnp.concatenate([low[:, :, :64], low[:, :, 64:]], axis=1)
    first = p[:, :n].reshape(count * n, 128)
    return jnp.concatenate([first, high.reshape(count * n, 64)], axis=1)


def plane_kernel(
    rows_n,
    feats_n,
    train_hbm,
    test_hbm,
    fw_hbm,
    rw_hbm,
    up_hbm,
    down_hbm,
    back_in,
    fw,
    rw,
    up,
    down,
    train_ref,
    test_ref,
    o_train,
    o_test,
    zbox,
    abox,
    a_in,
    t_box,
    t_in,
    ring,
    scores,
    values,
    queries,
    back_out,
    w_sem,
    f_send,
    f_recv,
    a_send,
    a_recv,
    r_send,
    r_recv,
    b_send,
    b_recv,
    gate,
):
    width = fw.shape[-1]
    quad = t_box.shape[0]
    heads = width // HD
    groups_n = rows_n // quad
    n_train = train_ref.shape[0]
    n_test = test_ref.shape[0]
    n_half = n_train // 2
    scale = LOG2E * HD ** (-0.5)

    my_row = lax.axis_index("rows")
    my_feat = lax.axis_index("feat")
    member = lax.rem(my_row, quad)
    group = my_row // quad

    def partner(k):
        low, high = lax.rem(member, 2), member // 2
        return (1 - high if k // 2 else high) * 2 + (1 - low if k % 2 else low)

    def mate(k):
        return group * quad + partner(k)

    right_group = lax.rem(group + 1, groups_n)
    left_group = lax.rem(group + groups_n - 1, groups_n)
    right = right_group * quad + member
    left = left_group * quad + member
    other = lax.rem(my_feat + 1, feats_n)

    loads = [
        pltpu.make_async_copy(s, d, w_sem.at[i])
        for i, (s, d) in enumerate(
            [
                (train_hbm, train_ref),
                (fw_hbm, fw),
                (test_hbm, test_ref),
                (rw_hbm, rw),
                (up_hbm, up),
                (down_hbm, down),
            ]
        )
    ]
    for c in loads:
        c.start()

    barrier = pltpu.get_barrier_semaphore()
    even = lax.rem(member, 2) == 0

    def greet(**where):
        pl.semaphore_signal(barrier, inc=1, device_id=where, device_id_type=MESH)

    def tell(i):
        pl.semaphore_signal(
            gate.at[i], inc=1, device_id={"rows": mate(1)}, device_id_type=MESH
        )

    @pl.when(even)
    def _():
        greet(rows=my_row, feat=other)
        for g in (group, right_group, left_group):
            for m in range(1, quad, 2):
                greet(rows=g * quad + m)
        pl.semaphore_wait(barrier, 3)
        tell(0)

    @pl.when(jnp.logical_not(even))
    def _():
        greet(rows=mate(1))
        greet(rows=mate(1), feat=other)
        greet(rows=mate(2))
        for g in (right_group, left_group):
            for m in range(1, quad, 2):
                greet(rows=g * quad + m)
        pl.semaphore_wait(gate.at[0], 1)

    swaps = [
        pltpu.make_async_remote_copy(
            src_ref=s,
            dst_ref=d,
            send_sem=f_send.at[i],
            recv_sem=f_recv.at[i],
            device_id={"feat": other},
            device_id_type=MESH,
        )
        for i, (s, d) in enumerate([(train_hbm, o_train), (test_hbm, o_test)])
    ]
    for c in swaps:
        c.start()

    def feature_rows(table):
        return jnp.concatenate(
            [table[:, f * width : (f + 1) * width].astype(F32) for f in range(quad)], axis=0
        )

    def split(x):
        n = x.shape[0] // quad
        return [x[f * n : (f + 1) * n] for f in range(quad)]

    lane_head = lax.broadcasted_iota(jnp.int32, (1, width), 1) // HD

    def by_head(q):
        return [jnp.where(lane_head == h, q, jnp.zeros_like(q)) for h in range(heads)]

    def join_heads(outs):
        mixed = None
        for h, out in enumerate(outs):
            part = out[:, :width] * (1.0 / out[:, width : width + 1])
            mixed = part if h == 0 else jnp.where(lane_head == h, part, mixed)
        return mixed.astype(BF)

    def own_side(table):
        cells = feature_rows(table)
        normed = layer_norm(cells).astype(BF)
        q = (dot(normed, fw[0]) * scale).astype(BF)
        return cells, q, dot(normed, fw[1]).astype(BF), dot(normed, fw[2]).astype(BF)

    tile = 16
    n_cells = 2 * quad * tile
    same_row = (
        lax.broadcasted_iota(jnp.int32, (heads * quad * tile, n_cells), 0) % tile
        == lax.broadcasted_iota(jnp.int32, (heads * quad * tile, n_cells), 1) % tile
    )
    ones = jnp.ones((n_cells, 256 - width), BF)

    def feature_attention(own, table):
        cells, q, k, v = own
        n = table.shape[0]
        normed = layer_norm(feature_rows(table)).astype(BF)
        more_k, more_v = dot(normed, fw[1]).astype(BF), dot(normed, fw[2]).astype(BF)
        mixes = []
        for b in range(n // tile):

            def rows(x):
                return [x[f * n + b * tile : f * n + (b + 1) * tile] for f in range(quad)]

            one = jnp.concatenate(by_head(jnp.concatenate(rows(q), axis=0)), axis=0)
            s = dot_t(one, jnp.concatenate(rows(k) + rows(more_k), axis=0))
            s = jnp.where(same_row, s, -1e30)
            e = jnp.exp2(s - jnp.max(s, axis=-1, keepdims=True)).astype(BF)
            vals = jnp.concatenate(rows(v) + rows(more_v), axis=0)
            out = dot(e, jnp.concatenate([vals, ones], axis=1))
            m = quad * tile
            mixes.append(join_heads([out[h * m : (h + 1) * m] for h in range(heads)]))
        mix = jnp.concatenate(
            [x[f * tile : (f + 1) * tile] for f in range(quad) for x in mixes], axis=0
        )
        return cells + dot(mix, fw[3])

    def to_mates(box, landing, stage):
        copies = []
        for k in (2, 3, 1):
            copies.append(
                pltpu.make_async_remote_copy(
                    src_ref=box.at[partner(k)],
                    dst_ref=landing.at[k],
                    send_sem=a_send.at[stage, k],
                    recv_sem=a_recv.at[stage, k],
                    device_id={"rows": mate(k)},
                    device_id_type=MESH,
                )
            )
            copies[-1].start()
        landing[0] = box[member]
        return copies

    def to_group(way, p, k):
        g = left_group if way else right_group
        return pltpu.make_async_remote_copy(
            src_ref=zbox.at[p, partner(k)],
            dst_ref=ring.at[way, p, k],
            send_sem=r_send.at[way, 0, p],
            recv_sem=r_recv.at[way, 0, p],
            device_id={"rows": g * quad + partner(k)},
            device_id_type=MESH,
        )

    def whole(way, h, p):
        return pltpu.make_async_remote_copy(
            src_ref=ring.at[way, p],
            dst_ref=ring.at[2 if h else way, p],
            send_sem=r_send.at[way, h, p],
            recv_sem=r_recv.at[way, h, p],
            device_id={"rows": left if way else right},
            device_id_type=MESH,
        )

    loads[0].wait()
    loads[1].wait()
    own = own_side(train_ref[...])

    @pl.when(jnp.logical_not(even))
    def _():
        pl.semaphore_wait(barrier, 3 * quad - 1)
        tell(1)

    swaps[0].wait()
    after_own = feature_attention(own, o_train[...])
    for f, x in enumerate(split(layer_norm(after_own).astype(BF))):
        for p in range(2):
            zbox[p, f] = pack(x[p * n_half : (p + 1) * n_half])

    @pl.when(even)
    def _():
        pl.semaphore_wait(gate.at[1], 1)

    for way, p in ((0, 0), (1, 1), (0, 1), (1, 0)):
        for k in range(quad):
            to_group(way, p, k).start()
    for f, x in enumerate(split(after_own.astype(BF))):
        abox[f] = pack(x)
    moved = [to_mates(abox, a_in, 0)]
    loads[2].wait()
    own_test = own_side(test_ref[...])
    swaps[1].wait()
    for f, x in enumerate(split(feature_attention(own_test, o_test[...]).astype(BF))):
        t_box[f] = pack(x)
    moved.append(to_mates(t_box, t_in, 1))

    after = []
    normed = []

    def arrive(stage):
        for c in moved[stage]:
            c.wait_recv()
        landing = (a_in, t_in)[stage]
        after.append(
            jnp.concatenate([unpack(landing[k]) for k in range(quad)], axis=0).astype(F32)
        )
        normed.append(layer_norm(after[stage]).astype(BF))

    n_query = quad * (n_train + n_test)
    n_side = n_query // 2
    sizes = [2 * n_train, 2 * n_test]
    begins = [0, 2 * n_train]
    train_rows = [slice(i * n_side, i * n_side + begins[1]) for i in range(2)]
    test_rows = [slice(i * n_side + begins[1], (i + 1) * n_side) for i in range(2)]
    everything = slice(0, n_query)
    span = quad * n_train

    def ask(stage):
        q_all = (dot(normed[stage], rw[0]) * scale).astype(BF)
        n = sizes[stage]
        for h, one in enumerate(by_head(q_all)):
            for i in range(2):
                at = i * n_side + begins[stage]
                queries[h, at : at + n] = one[(1 - i) * n : (2 - i) * n]

    def take(x, column):
        values[column * span : (column + 1) * span, :width] = dot(x, rw[2]).astype(BF)
        return dot(x, rw[1]).astype(BF)

    def landed(slot):
        return jnp.concatenate(
            [unpack_blocks(ring[slot - 1, 0]), unpack_blocks(ring[slot - 1, 1])], axis=0
        )

    def score(key, column, rows):
        for h in range(heads):
            for r in rows:
                scores[h, r, column * span : (column + 1) * span] = dot_t(queries[h, r], key)

    def attend(h, rows, columns, carried):
        s = scores[h, rows, columns]
        top = jnp.max(s, axis=-1, keepdims=True)
        if carried is not None:
            top = jnp.maximum(top, carried[0])
        e = jnp.exp2(s - top).astype(BF)
        out = dot(e, values[columns])
        if carried is not None:
            out = out + carried[1] * jnp.exp2(carried[0] - top)
        return top, out

    values[:, width:] = jnp.ones_like(values[:, width:])
    loads[3].wait()
    arrive(0)
    ask(0)
    own_key = take(normed[0], 0)
    score(own_key, 0, train_rows)

    def relay(way):
        whole(way, 0, way).wait_recv()
        whole(way, 1, way).start()

    for way in range(2):
        relay(way)
    arrive(1)
    ask(1)
    score(own_key, 0, test_rows)
    states = [attend(h, everything, slice(0, span), None) for h in range(heads)]

    for way in range(2):
        whole(way, 0, 1 - way).wait_recv()
    for slot in (1, 2):
        score(take(landed(slot), slot), slot, [everything])
    states = [attend(h, everything, slice(span, 3 * span), states[h]) for h in range(heads)]

    for way in range(2):
        whole(way, 1, way).wait_recv()
    last_key = take(landed(3), 3)
    columns = slice(3 * span, 4 * span)

    for c in loads[4:]:
        c.wait()
    returns = []
    for i, pair in enumerate(((2, 3), (0, 1))):
        rows = slice(i * n_side, (i + 1) * n_side)
        score(last_key, 3, [rows])
        side = [
            attend(h, rows, columns, tuple(x[rows] for x in states[h])) for h in range(heads)
        ]
        before = [x[(1 - i) * n : (2 - i) * n] for x, n in zip(after, sizes)]
        mixed = join_heads([out for _, out in side])
        after_row = jnp.concatenate(before, axis=0) + dot(mixed, rw[3])
        hidden = gelu(dot(layer_norm(after_row).astype(BF), up[...])).astype(BF)
        done = (after_row + dot_t(hidden, down[...])).astype(BF)
        for j, k in enumerate(pair):
            back_out[k] = pack(
                jnp.concatenate(
                    [
                        done[b + j * (n // 2) : b + (j + 1) * (n // 2)]
                        for b, n in zip(begins, sizes)
                    ],
                    axis=0,
                )
            )
            if k == 0:
                c = pltpu.make_async_copy(back_out.at[0], back_in.at[member], b_send.at[0])
            else:
                c = pltpu.make_async_remote_copy(
                    src_ref=back_out.at[k],
                    dst_ref=back_in.at[member],
                    send_sem=b_send.at[k],
                    recv_sem=b_recv.at[k],
                    device_id={"rows": mate(k)},
                    device_id_type=MESH,
                )
            c.start()
            returns.append(c)
    for c in returns:
        c.wait()
    for c in [*moved[0], *moved[1]]:
        c.wait_send()
    for way in range(2):
        for p in range(2):
            whole(way, 0, p).wait_send()
        whole(way, 1, way).wait_send()


def place(back_ref, train_out, test_out):
    quad = back_ref.shape[0]
    result = jnp.concatenate([unpack(back_ref[f]) for f in range(quad)], axis=1)
    n_train = train_out.shape[0]
    train_out[...] = result[:n_train]
    test_out[...] = result[n_train:]


def solution(mesh):
    rows_n = mesh.shape["rows"]
    feats_n = mesh.shape["feat"]

    def body(train, test, fw, rw, up, down):
        width = fw.shape[-1]
        quad = train.shape[1] // width
        heads = width // HD
        n_train, n_test = train.shape[0], test.shape[0]
        cell_rows = n_train + n_test
        groups_n = rows_n // quad
        half = groups_n // 2
        span = quad * n_train
        keys = min(groups_n, 4) * span
        packed = cell_rows * width // 128
        vmem = pltpu.VMEM
        dma = pltpu.SemaphoreType.DMA
        vspec = pl.BlockSpec(memory_space=pltpu.VMEM)
        aspec = pl.BlockSpec(memory_space=pl.ANY)
        if groups_n == 4 and quad == 4 and n_train % 32 == 0 and n_test % 16 == 0:
            body_fn = plane_kernel
            boxes = [
                vmem((2, quad, n_train * width // 256, 128), BF),
                vmem((quad, n_train * width // 128, 128), BF),
                vmem((quad, n_train * width // 128, 128), BF),
                vmem((quad, n_test * width // 128, 128), BF),
                vmem((quad, n_test * width // 128, 128), BF),
                vmem((3, 2, quad, n_train * width // 256, 128), BF),
            ]
            flags = [
                dma((2,)),
                dma((2,)),
                dma((2, quad)),
                dma((2, quad)),
                dma((2, 2, 2)),
                dma((2, 2, 2)),
                dma((quad,)),
                dma((quad,)),
                pltpu.SemaphoreType.REGULAR((2,)),
            ]
        else:
            body_fn = kernel
            boxes = [
                vmem((2, quad, n_train * width // 256, 128), BF),
                vmem((2, quad, n_train * width // 256, 128), BF),
                vmem((quad, n_test * width // 128, 128), BF),
                vmem((quad, n_test * width // 128, 128), BF),
                vmem((groups_n, 2, span * width // 256, 128), BF),
            ]
            flags = [
                dma((3,)),
                dma((3,)),
                dma((3, quad)),
                dma((3, quad)),
                dma((2, half, 2)),
                dma((2, half, 2)),
                dma((quad,)),
                dma((quad,)),
            ]
        back = pl.pallas_call(
            functools.partial(body_fn, rows_n, feats_n),
            out_shape=pltpu.VMEM((quad, packed, 128), BF),
            in_specs=[aspec, aspec, aspec, aspec, aspec, aspec],
            out_specs=vspec,
            scratch_shapes=[
                vmem(fw.shape, BF),
                vmem(rw.shape, BF),
                vmem(up.shape, BF),
                vmem(down.shape[::-1], BF),
                vmem(train.shape, BF),
                vmem(test.shape, BF),
                vmem(train.shape, BF),
                vmem(test.shape, BF),
                *boxes,
                vmem((heads, quad * cell_rows, keys), F32),
                vmem((keys, 256), BF),
                vmem((heads, quad * cell_rows, width), BF),
                vmem((quad, packed, 128), BF),
                dma((6,)),
                *flags,
            ],
            compiler_params=pltpu.CompilerParams(
                collective_id=0, has_side_effects=True, vmem_limit_bytes=60 * 1024 * 1024
            ),
            name="layer",
        )(train, test, fw, rw, up, down.T)
        return pl.pallas_call(
            place,
            out_shape=(
                jax.ShapeDtypeStruct(train.shape, BF),
                jax.ShapeDtypeStruct(test.shape, BF),
            ),
            in_specs=[vspec],
            out_specs=(vspec, vspec),
            name="place",
        )(pltpu.with_memory_space_constraint(back, pltpu.VMEM))

    return jax.shard_map(
        body,
        mesh=mesh,
        in_specs=(P("rows", "feat"), P("rows", "feat"), P(), P(), P(), P()),
        out_specs=(P("rows", "feat"), P("rows", "feat")),
        check_vma=False,
    )
```

```python
import functools

import jax
import jax.numpy as jnp
from jax import lax
from jax.experimental import pallas as pl
from jax.experimental.pallas import tpu as pltpu
from jax.sharding import PartitionSpec as P

HD = 32
EPS = 1e-05
LOG2E = 1.4426950408889634
MESH = pl.DeviceIdType.MESH
BF = jnp.bfloat16
F32 = jnp.float32


def layer_norm(x):
    centred = x - jnp.mean(x, axis=-1, keepdims=True)
    spread = jnp.mean(centred * centred, axis=-1, keepdims=True)
    return centred * lax.rsqrt(spread + EPS)


def dot(a, b):
    return jnp.dot(a, b, preferred_element_type=F32)


def dot_t(a, b):
    return lax.dot_general(a, b, (((1,), (1,)), ((), ())), preferred_element_type=F32)


def pack(x):
    n = x.shape[0]
    low = jnp.concatenate([x[: n // 2, 128:], x[n // 2 :, 128:]], axis=1)
    return jnp.concatenate([x[:, :128], low], axis=0)


def unpack(p):
    n = p.shape[0] * 2 // 3
    low = p[n:]
    high = jnp.concatenate([low[:, :64], low[:, 64:]], axis=0)
    return jnp.concatenate([p[:n], high], axis=1)


def gelu(x):
    return 0.5 * x * (1.0 + lax.erf(x * (0.5**0.5)))


def kernel(
    rows_n,
    feats_n,
    train_hbm,
    test_hbm,
    fw_hbm,
    rw_hbm,
    up_hbm,
    down_hbm,
    back_in,
    fw,
    rw,
    up,
    down,
    train_ref,
    test_ref,
    o_train,
    o_test,
    outbox,
    inbox,
    t_outbox,
    t_inbox,
    ring,
    scores,
    values,
    queries,
    back_out,
    w_sem,
    f_send,
    f_recv,
    q_send,
    q_recv,
    r_send,
    r_recv,
    b_send,
    b_recv,
):
    width = fw.shape[-1]
    quad = t_outbox.shape[0]
    heads = width // HD
    groups_n = rows_n // quad
    half = groups_n // 2
    n_train = train_ref.shape[0]
    n_test = test_ref.shape[0]
    n_half = n_train // 2
    scale = LOG2E * HD ** (-0.5)

    my_row = lax.axis_index("rows")
    my_feat = lax.axis_index("feat")
    member = lax.rem(my_row, quad)
    group = my_row // quad

    def partner(k):
        low, high = lax.rem(member, 2), member // 2
        return (1 - high if k // 2 else high) * 2 + (1 - low if k % 2 else low)

    def mate(k):
        return group * quad + partner(k)

    right = lax.rem(group + 1, groups_n) * quad + member
    left = lax.rem(group + groups_n - 1, groups_n) * quad + member
    other = lax.rem(my_feat + 1, feats_n)

    loads = [
        pltpu.make_async_copy(s, d, w_sem.at[i])
        for i, (s, d) in enumerate(
            [
                (train_hbm, train_ref),
                (fw_hbm, fw),
                (test_hbm, test_ref),
                (rw_hbm, rw),
                (up_hbm, up),
                (down_hbm, down),
            ]
        )
    ]
    for c in loads:
        c.start()

    barrier = pltpu.get_barrier_semaphore()
    pl.semaphore_signal(barrier, inc=1, device_id={"feat": other}, device_id_type=MESH)
    for k in range(1, quad):
        pl.semaphore_signal(barrier, inc=1, device_id={"rows": mate(k)}, device_id_type=MESH)
    for d in (right, left):
        pl.semaphore_signal(barrier, inc=1, device_id={"rows": d}, device_id_type=MESH)
    pl.semaphore_wait(barrier, quad + 2)

    halves = [pl.ds(p * n_half, n_half) for p in range(2)]
    swaps = [
        pltpu.make_async_remote_copy(
            src_ref=s,
            dst_ref=d,
            send_sem=f_send.at[i],
            recv_sem=f_recv.at[i],
            device_id={"feat": other},
            device_id_type=MESH,
        )
        for i, (s, d) in enumerate(
            [(train_hbm.at[r], o_train.at[r]) for r in halves] + [(test_hbm, o_test)]
        )
    ]
    for c in swaps:
        c.start()

    def feature_rows(table):
        return jnp.concatenate(
            [table[:, f * width : (f + 1) * width].astype(F32) for f in range(quad)], axis=0
        )

    def split(x):
        n = x.shape[0] // quad
        return [x[f * n : (f + 1) * n] for f in range(quad)]

    def key_value(normed):
        return split(dot(normed, fw[1]).astype(BF)), split(dot(normed, fw[2]).astype(BF))

    same = (
        lax.broadcasted_iota(jnp.int32, (width, width), 0) // HD
        == lax.broadcasted_iota(jnp.int32, (width, width), 1) // HD
    )
    spread = jnp.where(same, 1.0, 0.0).astype(BF)

    def own_side(table):
        cells = feature_rows(table)
        normed = layer_norm(cells).astype(BF)
        q = split((dot(normed, fw[0]) * scale).astype(BF))
        ks, vs = key_value(normed)
        return cells, q, ks, vs

    def feature_attention(own, table):
        cells, q, ks, vs = own
        n = table.shape[0]
        more_k, more_v = key_value(layer_norm(feature_rows(table)).astype(BF))
        ks, vs = ks + more_k, vs + more_v
        mixes = []
        for f in range(quad):
            prod = jnp.concatenate([q[f] * k for k in ks], axis=0)
            s = dot(prod, spread)
            s = [s[g * n : (g + 1) * n] for g in range(len(ks))]
            top = functools.reduce(jnp.maximum, s)
            total = None
            mix = None
            for g in range(len(ks)):
                e = jnp.exp2(s[g] - top)
                t = e * vs[g].astype(F32)
                total = e if total is None else total + e
                mix = t if mix is None else mix + t
            mixes.append((mix / total).astype(BF))
        feat_out = dot(jnp.concatenate(mixes, axis=0), fw[3])
        return split((cells + feat_out).astype(BF))

    def to_mates(box, landing, stage):
        copies = {}
        for k in (2, 3, 1):
            copies[k] = pltpu.make_async_remote_copy(
                src_ref=box.at[partner(k)],
                dst_ref=landing.at[k],
                send_sem=q_send.at[stage, k],
                recv_sem=q_recv.at[stage, k],
                device_id={"rows": mate(k)},
                device_id_type=MESH,
            )
            copies[k].start()
        landing[0] = box[member]
        return copies

    loads[0].wait()
    loads[1].wait()
    own = [own_side(train_ref[p * n_half : (p + 1) * n_half]) for p in range(2)]
    moved = []
    boxes = [(outbox.at[p], inbox.at[p]) for p in range(2)] + [(t_outbox, t_inbox)]
    for p in range(2):
        swaps[p].wait()
        for f, x in enumerate(feature_attention(own[p], o_train[p * n_half : (p + 1) * n_half])):
            outbox[p, f] = pack(x)
        moved.append(to_mates(*boxes[p], p))
    loads[2].wait()
    own_test = own_side(test_ref[...])
    swaps[2].wait()
    for f, x in enumerate(feature_attention(own_test, o_test[...])):
        t_outbox[f] = pack(x)
    moved.append(to_mates(*boxes[2], 2))

    def hop(way, h, p):
        last = h == half - 1
        src = 0 if h == 0 else 2 * h - 1 + way
        dst = 2 * half - 1 if last else 1 + 2 * h + way
        return pltpu.make_async_remote_copy(
            src_ref=ring.at[src, p],
            dst_ref=ring.at[dst, p],
            send_sem=r_send.at[way, h, p],
            recv_sem=r_recv.at[way, h, p],
            device_id={"rows": left if way else right},
            device_id_type=MESH,
        )

    def pieces(way, h):
        return (way,) if h == half - 1 else (way, 1 - way)

    hops = {}
    after = []
    normed = []

    def arrive(stage):
        for k in range(1, quad):
            moved[stage][k].wait_recv()
        landing = boxes[stage][1]
        after.append(
            jnp.concatenate([unpack(landing[k]) for k in range(quad)], axis=0).astype(F32)
        )
        normed.append(layer_norm(after[stage]).astype(BF))

    for p in range(2):
        arrive(p)
        ring[0, p] = pack(normed[p])
        for way in (p, 1 - p):
            if p in pieces(way, 0):
                hops[way, 0, p] = hop(way, 0, p)
                hops[way, 0, p].start()

    loads[3].wait()
    lane_head = lax.broadcasted_iota(jnp.int32, (1, width), 1) // HD
    n_query = quad * (n_train + n_test)
    n_side = n_query // 2
    sizes = [2 * n_half, 2 * n_half, 2 * n_test]
    begins = [0, 2 * n_half, 4 * n_half]
    all_rows = [slice(0, n_query)]
    train_rows = [slice(i * n_side, i * n_side + begins[2]) for i in range(2)]
    test_rows = [slice(i * n_side + begins[2], (i + 1) * n_side) for i in range(2)]
    span = quad * n_train
    values[:, width:] = jnp.ones_like(values[:, width:])

    def ask(stage):
        q_all = (dot(normed[stage], rw[0]) * scale).astype(BF)
        n = sizes[stage]
        for h in range(heads):
            one = jnp.where(lane_head == h, q_all, jnp.zeros_like(q_all))
            for i in range(2):
                at = i * n_side + begins[stage]
                queries[h, at : at + n] = one[(1 - i) * n : (2 - i) * n]

    def take(slot, column):
        x = jnp.concatenate([unpack(ring[slot, 0]), unpack(ring[slot, 1])], axis=0)
        values[column * span : (column + 1) * span, :width] = dot(x, rw[2]).astype(BF)
        return dot(x, rw[1]).astype(BF)

    def score(key, column, rows):
        for h in range(heads):
            for r in rows:
                scores[h, r, column * span : (column + 1) * span] = dot_t(queries[h, r], key)

    def attend(h, rows, columns, carried):
        s = scores[h, rows, columns]
        top = jnp.max(s, axis=-1, keepdims=True)
        if carried is not None:
            top = jnp.maximum(top, carried[0])
        e = jnp.exp2(s - top).astype(BF)
        out = dot(e, values[columns])
        if carried is not None:
            out = out + carried[1] * jnp.exp2(carried[0] - top)
        return top, out

    ask(0)
    ask(1)
    everything = slice(0, n_query)
    if half <= 2:
        own_key = take(0, 0)
        score(own_key, 0, train_rows)
    arrive(2)
    ask(2)
    if half <= 2:
        score(own_key, 0, test_rows)
        states = [attend(h, everything, slice(0, span), None) for h in range(heads)]

    for h in range(half - 1):
        for way in range(2):
            for p in pieces(way, h + 1):
                hops[way, h, p].wait_recv()
                hops[way, h + 1, p] = hop(way, h + 1, p)
                hops[way, h + 1, p].start()
        for way in range(2):
            for p in pieces(way, h):
                if p not in pieces(way, h + 1):
                    hops[way, h, p].wait_recv()

    if half == 2:
        for slot in (1, 2):
            score(take(slot, slot), slot, all_rows)
        states = [
            attend(h, everything, slice(span, 3 * span), states[h]) for h in range(heads)
        ]

    for way in range(2):
        for p in pieces(way, half - 1):
            hops[way, half - 1, p].wait_recv()

    if half <= 2:
        last = 2 * half - 1
        last_key = take(last, last)
        columns = slice(last * span, (last + 1) * span)
    else:
        per = scores.shape[2] // span

        def step(i, states):
            for j in range(per):
                score(take(i * per + j, j), j, all_rows)
            return [attend(h, everything, slice(0, per * span), states[h]) for h in range(heads)]

        start = [
            (
                jnp.full((n_query, 1), -1e30, F32),
                jnp.zeros((n_query, values.shape[1]), F32),
            )
            for _ in range(heads)
        ]
        states = lax.fori_loop(0, groups_n // per, step, start)

    for c in loads[4:]:
        c.wait()
    returns = []
    for i, pair in enumerate(((2, 3), (0, 1))):
        rows = slice(i * n_side, (i + 1) * n_side)
        side = [tuple(x[rows] for x in states[h]) for h in range(heads)]
        if half <= 2:
            score(last_key, last, [rows])
            side = [attend(h, rows, columns, side[h]) for h in range(heads)]
        mixed = None
        for h in range(heads):
            out = side[h][1]
            part = out[:, :width] * (1.0 / out[:, width : width + 1])
            mixed = part if h == 0 else jnp.where(lane_head == h, part, mixed)
        before = [x[(1 - i) * n : (2 - i) * n] for x, n in zip(after, sizes)]
        after_row = jnp.concatenate(before, axis=0) + dot(mixed.astype(BF), rw[3])
        hidden = gelu(dot(layer_norm(after_row).astype(BF), up[...])).astype(BF)
        done = (after_row + dot_t(hidden, down[...])).astype(BF)
        for j, k in enumerate(pair):
            block = pack(
                jnp.concatenate(
                    [
                        done[b + j * (n // 2) : b + (j + 1) * (n // 2)]
                        for b, n in zip(begins, sizes)
                    ],
                    axis=0,
                )
            )
            back_out[k] = block
            if k == 0:
                c = pltpu.make_async_copy(back_out.at[0], back_in.at[member], b_send.at[0])
                c.start()
                returns.append(c)
                continue
            c = pltpu.make_async_remote_copy(
                src_ref=back_out.at[k],
                dst_ref=back_in.at[member],
                send_sem=b_send.at[k],
                recv_sem=b_recv.at[k],
                device_id={"rows": mate(k)},
                device_id_type=MESH,
            )
            c.start()
            returns.append(c)
    for c in returns:
        c.wait()
    for c in [*hops.values(), *(c for m in moved for c in m.values())]:
        c.wait_send()


def unpack_blocks(p):
    n = p.shape[1] * 2 // 3
    count = p.shape[0]
    low = p[:, n:]
    high = jnp.concatenate([low[:, :, :64], low[:, :, 64:]], axis=1)
    first = p[:, :n].reshape(count * n, 128)
    return jnp.concatenate([first, high.reshape(count * n, 64)], axis=1)


def plane_kernel(
    rows_n,
    feats_n,
    train_hbm,
    test_hbm,
    fw_hbm,
    rw_hbm,
    up_hbm,
    down_hbm,
    back_in,
    fw,
    rw,
    up,
    down,
    train_ref,
    test_ref,
    o_train,
    o_test,
    zbox,
    abox,
    a_in,
    t_box,
    t_in,
    ring,
    early_q,
    late_q,
    early_x,
    late_x,
    fw_t,
    f_cells,
    f_x,
    t_cells,
    t_x,
    fq,
    fk,
    fv,
    fs,
    fe,
    fm,
    rw_t,
    up_t,
    early_s,
    late_s,
    early_e,
    late_e,
    early_sum,
    late_sum,
    early_top,
    late_top,
    keys,
    vals,
    raised,
    hidden,
    back_out,
    w_sem,
    f_send,
    f_recv,
    a_send,
    a_recv,
    r_send,
    r_recv,
    b_send,
    b_recv,
    gate,
):
    width = fw.shape[-1]
    quad = t_box.shape[1]
    heads = width // HD
    groups_n = rows_n // quad
    n_train = train_ref.shape[0]
    n_test = test_ref.shape[0]
    n_half, n_quart = n_train // 2, n_test // 2
    scale = LOG2E * HD ** (-0.5)

    my_row = lax.axis_index("rows")
    my_feat = lax.axis_index("feat")
    member = lax.rem(my_row, quad)
    group = my_row // quad

    def partner(k):
        low, high = lax.rem(member, 2), member // 2
        return (1 - high if k // 2 else high) * 2 + (1 - low if k % 2 else low)

    def mate(k):
        return group * quad + partner(k)

    right_group = lax.rem(group + 1, groups_n)
    left_group = lax.rem(group + groups_n - 1, groups_n)
    right = right_group * quad + member
    left = left_group * quad + member
    other = lax.rem(my_feat + 1, feats_n)

    loads = [
        pltpu.make_async_copy(s, d, w_sem.at[i])
        for i, (s, d) in enumerate(
            [
                (train_hbm, train_ref),
                (fw_hbm, fw),
                (test_hbm, test_ref),
                (rw_hbm, rw),
                (up_hbm, up),
                (down_hbm, down),
            ]
        )
    ]
    for c in loads:
        c.start()

    barrier = pltpu.get_barrier_semaphore()
    even = lax.rem(member, 2) == 0

    def greet(**where):
        pl.semaphore_signal(barrier, inc=1, device_id=where, device_id_type=MESH)

    def tell(i):
        pl.semaphore_signal(
            gate.at[i], inc=1, device_id={"rows": mate(1)}, device_id_type=MESH
        )

    @pl.when(even)
    def _():
        greet(rows=my_row, feat=other)
        for g in (group, right_group, left_group):
            for m in range(1, quad, 2):
                for y in (my_feat, other):
                    greet(rows=g * quad + m, feat=y)
        pl.semaphore_wait(barrier, 3)
        tell(0)

    @pl.when(jnp.logical_not(even))
    def _():
        greet(rows=mate(1))
        greet(rows=mate(1), feat=other)
        greet(rows=my_row, feat=other)
        for y in (my_feat, other):
            greet(rows=mate(2), feat=y)
            for g in (right_group, left_group):
                for m in range(1, quad, 2):
                    greet(rows=g * quad + m, feat=y)
        pl.semaphore_wait(gate.at[0], 1)

    swaps = [
        pltpu.make_async_remote_copy(
            src_ref=s,
            dst_ref=d,
            send_sem=f_send.at[i],
            recv_sem=f_recv.at[i],
            device_id={"feat": other},
            device_id_type=MESH,
        )
        for i, (s, d) in enumerate(
            [
                (train_hbm.at[pl.ds(pl.multiple_of(other * n_half, n_half), n_half)], o_train),
                (test_hbm.at[pl.ds(pl.multiple_of(other * n_quart, n_quart), n_quart)], o_test),
            ]
        )
    ]
    for c in swaps:
        c.start()

    tile = 16
    cell = quad * tile
    pair = 2 * cell
    lines = HD + 16
    same_row = (
        lax.broadcasted_iota(jnp.int32, (pair, heads * pair), 0) % tile
        == lax.broadcasted_iota(jnp.int32, (pair, heads * pair), 1) % tile
    )

    def fill(table, side, cells_ref, x_ref):
        n = table.shape[0] // tile
        cells = jnp.concatenate(
            [
                table[b * tile : (b + 1) * tile, f * width : (f + 1) * width].astype(F32)
                for b in range(n)
                for f in range(quad)
            ],
            axis=0,
        )
        normed = layer_norm(cells).astype(BF)
        for b in range(n):
            to = slice((2 * b + side) * cell, (2 * b + side + 1) * cell)
            cells_ref[to] = cells[b * cell : (b + 1) * cell]
            x_ref[to] = normed[b * cell : (b + 1) * cell]

    def normed_columns(x):
        centred = x - jnp.mean(x, axis=0, keepdims=True)
        spread = jnp.mean(centred * centred, axis=0, keepdims=True)
        return centred * lax.rsqrt(spread + EPS)

    def feature_attention(cells_ref, x_ref):
        n = x_ref.shape[0]
        blocks = [slice(b * pair, (b + 1) * pair) for b in range(n // pair)]
        x = x_ref[...]
        q = (dot_t(fw_t[0], x) * scale).astype(BF)
        fk[:n] = dot(x, fw[1]).astype(BF)
        v = dot_t(fw_t[2], x).astype(BF)
        for h in range(heads):
            rows = slice(h * HD, (h + 1) * HD)
            fv[h * lines : h * lines + HD, :n] = v[rows]
            for b, at in enumerate(blocks):
                fq[rows, (b * heads + h) * pair : (b * heads + h + 1) * pair] = q[rows, at]
        for b, at in enumerate(blocks):
            fs[at] = dot(fk[at], fq[:, b * heads * pair : (b + 1) * heads * pair])
        for at in blocks:
            s = jnp.where(same_row, fs[at], -1e30)
            fe[at] = jnp.exp2(s - jnp.max(s, axis=0, keepdims=True)).astype(BF)
        for at in blocks:
            for h in range(heads):
                out = dot(
                    fv[h * lines : (h + 1) * lines, at], fe[at, h * pair : (h + 1) * pair]
                )
                part = out[:HD] * (1.0 / out[HD : HD + 1])
                fm[h * HD : (h + 1) * HD, at] = part.astype(BF)
        after = cells_ref[...].T + dot(fw_t[3], fm[:, :n])
        return after, normed_columns(after)

    def sides(x):
        n = x.shape[0] // pair
        for j in range(2):
            for f in range(quad):
                at = [(2 * b + j) * cell + f * tile for b in range(n)]
                yield j, f, jnp.concatenate([x[i : i + tile] for i in at], axis=0)

    feats = (my_feat, other)

    def to_mates(box, landing, stage):
        copies = []
        for k, j in ((2, 0), (0, 1), (3, 0), (1, 1), (2, 1), (3, 1), (1, 0)):
            copies.append(
                pltpu.make_async_remote_copy(
                    src_ref=box.at[j, partner(k)],
                    dst_ref=landing.at[j, k],
                    send_sem=a_send.at[stage, j, k],
                    recv_sem=a_recv.at[stage, j, k],
                    device_id={"rows": mate(k), "feat": feats[j]},
                    device_id_type=MESH,
                )
            )
            copies[-1].start()
        landing[0, 0] = box[0, member]
        return copies

    inner = jnp.logical_and(group > 0, group < groups_n - 1)

    def to_group(way, p, k):
        g = jnp.where(way == 1, left_group, right_group)
        return pltpu.make_async_remote_copy(
            src_ref=zbox.at[p, partner(k)],
            dst_ref=ring.at[way, p, k],
            send_sem=r_send.at[way, p],
            recv_sem=r_recv.at[way, p],
            device_id={"rows": g * quad + partner(k), "feat": feats[p]},
            device_id_type=MESH,
        )

    def whole(slot, p):
        return pltpu.make_async_remote_copy(
            src_ref=ring.at[slot, p],
            dst_ref=ring.at[slot, p],
            send_sem=r_send.at[slot, p],
            recv_sem=r_recv.at[slot, p],
            device_id={"rows": right},
            device_id_type=MESH,
        )

    def onward(way, p):
        return pltpu.make_async_remote_copy(
            src_ref=ring.at[way, p],
            dst_ref=ring.at[2, p],
            send_sem=r_send.at[2 + way, p],
            recv_sem=r_recv.at[2, p],
            device_id={"rows": left if way else right},
            device_id_type=MESH,
        )

    def relay(p):
        @pl.when(inner)
        def _():
            for way in range(2):
                whole(way, p).wait_recv()
                onward(way, p).start()

    loads[0].wait()
    loads[1].wait()
    fill(train_ref[pl.ds(pl.multiple_of(my_feat * n_half, n_half), n_half)], 0, f_cells, f_x)
    for i in (0, 2, 3):
        fw_t[i] = fw[i].astype(F32).T.astype(BF)
    loads[2].wait()
    fill(test_ref[pl.ds(pl.multiple_of(my_feat * n_quart, n_quart), n_quart)], 0, t_cells, t_x)
    fq[...] = jnp.zeros_like(fq)
    fv[...] = jnp.ones_like(fv)

    @pl.when(jnp.logical_not(even))
    def _():
        pl.semaphore_wait(barrier, 6 * quad - 1)
        tell(1)

    swaps[0].wait()
    fill(o_train[...], 1, f_cells, f_x)
    after_own, normed_own = feature_attention(f_cells, f_x)
    for j, f, x in sides(normed_own.T):
        zbox[j, f] = pack(x.astype(BF))

    @pl.when(even)
    def _():
        pl.semaphore_wait(gate.at[1], 1)

    near = jnp.where(group == groups_n - 1, 1, 0)
    for way in (near, 1 - near):
        for p in range(2):
            for k in range(quad):
                to_group(way, p, k).start()
    for j, f, x in sides(after_own.T):
        abox[j, f] = pack(x.astype(BF))
    moved = [to_mates(abox, a_in, 0)]
    swaps[1].wait()
    fill(o_test[...], 1, t_cells, t_x)
    after_own, _ = feature_attention(t_cells, t_x)
    for j, f, x in sides(after_own.T):
        t_box[j, f] = pack(x.astype(BF))
    moved.append(to_mates(t_box, t_in, 1))

    loads[3].wait()
    for i in (0, 2, 3):
        rw_t[i] = rw[i].astype(F32).T.astype(BF)
    loads[4].wait()
    up_t[...] = up[...].astype(F32).T.astype(BF)
    vals[...] = jnp.ones_like(vals)
    early_q[...] = jnp.zeros_like(early_q)
    late_q[...] = jnp.zeros_like(late_q)

    def arrive(stage):
        for c in moved[stage]:
            c.wait_recv()
        landing = (a_in, t_in)[stage]
        x = jnp.concatenate(
            [unpack(landing[j, k]) for k in range(quad) for j in range(2)], axis=0
        ).astype(F32)
        normed = layer_norm(x).astype(BF)
        return x, normed, (dot_t(rw_t[0], normed) * scale).astype(BF)

    n_mid = 2 * n_train
    n_late = 2 * n_train
    n_early = n_mid + quad * n_test

    def place_queries(q, into, size, at):
        n = q.shape[1]
        for h in range(heads):
            rows = slice(h * HD, (h + 1) * HD)
            into[rows, h * size + at : h * size + at + n] = q[rows]

    late = (late_q, late_s, late_e, late_sum, late_top, n_late)
    early = (early_q, early_s, early_e, early_sum, early_top, n_early)

    def key_value_rows(x, i):
        keys[i] = dot(x, rw[1]).astype(BF)
        value = dot_t(rw_t[2], x).astype(BF)
        for h in range(heads):
            vals[i, h * lines : h * lines + HD] = value[h * HD : (h + 1) * HD]

    def attend(asked, i, first=False):
        per_head = [
            (part, h, slice(h * part[5], (h + 1) * part[5]), slice(h * lines, (h + 1) * lines))
            for part in asked
            for h in range(heads)
        ]
        key = keys[i]
        for (q, s, _, _, _, _), h, c, _ in per_head:
            s[:, c] = dot(key, q[:, c])
        for (_, s, e, total, tops, _), h, c, r in per_head:
            top = jnp.max(s[:, c], axis=0, keepdims=True)
            if not first:
                old = tops[0:1, c]
                top = jnp.maximum(top, old)
                total[r] = total[r] * jnp.exp2(old - top)
            e[:, c] = jnp.exp2(s[:, c] - top).astype(BF)
            tops[0:1, c] = top
        for (_, _, e, total, _, _), h, c, r in per_head:
            out = dot(vals[i, r], e[:, c])
            total[r] = out if first else total[r] + out

    def finish(part, before):
        total = part[3]
        mix = jnp.concatenate(
            [
                total[h * lines : h * lines + HD]
                * (1.0 / total[h * lines + HD : h * lines + HD + 1])
                for h in range(heads)
            ],
            axis=0,
        ).astype(BF)
        after_row = before + dot(rw_t[3], mix)
        normed = normed_columns(after_row).astype(BF)
        n = normed.shape[1]
        raised[:, :n] = dot(up_t[...], normed)
        hidden[:, :n] = gelu(raised[:, :n]).astype(BF)
        return (after_row + dot(down[...], hidden[:, :n])).T.astype(BF)

    relay(0)
    relay(1)
    x, normed, q = arrive(0)
    place_queries(q[:, n_mid:], early_q, n_early, 0)
    place_queries(q[:, :n_late], late_q, n_late, 0)
    early_x[:, :n_mid] = x[n_late:].T
    late_x[...] = x[:n_late].T
    key_value_rows(normed, 0)
    attend([late], 0, True)
    x, _, q = arrive(1)
    place_queries(q, early_q, n_early, n_mid)
    early_x[:, n_mid:] = x.T
    attend([early], 0, True)

    at_start, at_end = group == 0, group == groups_n - 1
    order = (
        jnp.where(at_start, 1, 0),
        jnp.where(at_start, 2, jnp.where(at_end, 2, 1)),
        jnp.where(at_start, 0, jnp.where(at_end, 1, 2)),
    )

    def fetch(i):
        slot = order[i]

        @pl.when(jnp.logical_not(jnp.logical_and(inner, slot < 2)))
        def _():
            for p in range(2):
                whole(slot, p).wait_recv()

        x = jnp.concatenate([unpack_blocks(ring[slot, p]) for p in range(2)], axis=0)
        key_value_rows(x, (i + 1) % 2)

    for i in range(2):
        fetch(i)
        attend([late, early], (i + 1) % 2)
    fetch(2)
    loads[5].wait()

    returns = []

    def give_back(k, done, tests):
        block = jnp.concatenate([done, tests[k * n_test : (k + 1) * n_test]], axis=0)
        back_out[k] = pack(block)
        if k == 0:
            c = pltpu.make_async_copy(back_out.at[0], back_in.at[member], b_send.at[0])
        else:
            c = pltpu.make_async_remote_copy(
                src_ref=back_out.at[k],
                dst_ref=back_in.at[member],
                send_sem=b_send.at[k],
                recv_sem=b_recv.at[k],
                device_id={"rows": mate(k)},
                device_id_type=MESH,
            )
        c.start()
        returns.append(c)

    attend([early], 1)
    done = finish(early, early_x[...])
    tests = done[n_mid:]
    for k in (2, 3):
        give_back(k, done[(k - 2) * n_train : (k - 1) * n_train], tests)
    attend([late], 1)
    done = finish(late, late_x[...])
    for k in (1, 0):
        give_back(k, done[k * n_train : (k + 1) * n_train], tests)
    for c in returns:
        c.wait()
    for c in [*moved[0], *moved[1]]:
        c.wait_send()
    for way in range(2):
        for p in range(2):
            whole(way, p).wait_send()

    @pl.when(inner)
    def _():
        for way in range(2):
            for p in range(2):
                onward(way, p).wait_send()


def place_halves(back_ref, train_out, test_out):
    quad = back_ref.shape[0]
    result = jnp.concatenate([unpack(back_ref[f]) for f in range(quad)], axis=1)
    in_order = lax.axis_index("feat") == 0
    begin = 0
    for out in (train_out, test_out):
        half = out.shape[0] // 2
        one, two = (result[begin + j * half : begin + (j + 1) * half] for j in range(2))
        out[:half] = jnp.where(in_order, one, two)
        out[half:] = jnp.where(in_order, two, one)
        begin += 2 * half


def place(back_ref, train_out, test_out):
    quad = back_ref.shape[0]
    result = jnp.concatenate([unpack(back_ref[f]) for f in range(quad)], axis=1)
    n_train = train_out.shape[0]
    train_out[...] = result[:n_train]
    test_out[...] = result[n_train:]


def solution(mesh):
    rows_n = mesh.shape["rows"]
    feats_n = mesh.shape["feat"]

    def body(train, test, fw, rw, up, down):
        width = fw.shape[-1]
        quad = train.shape[1] // width
        heads = width // HD
        n_train, n_test = train.shape[0], test.shape[0]
        cell_rows = n_train + n_test
        groups_n = rows_n // quad
        half = groups_n // 2
        span = quad * n_train
        keys = min(groups_n, 4) * span
        packed = cell_rows * width // 128
        vmem = pltpu.VMEM
        dma = pltpu.SemaphoreType.DMA
        vspec = pl.BlockSpec(memory_space=pltpu.VMEM)
        aspec = pl.BlockSpec(memory_space=pl.ANY)
        weights = (fw, rw, up, down.T)
        place_fn = place
        fits = groups_n == 4 and quad == 4 and feats_n == 2
        if fits and n_train % 32 == 0 and n_test % 32 == 0:
            body_fn, place_fn = plane_kernel, place_halves
            n_half, n_quart = n_train // 2, n_test // 2
            swapped = [vmem((n_half, quad * width), BF), vmem((n_quart, quad * width), BF)]
            both = 2 * quad
            pair = both * 16
            lines = heads * (HD + 16)
            early, late = 2 * n_train + quad * n_test, 2 * n_train
            work = [
                vmem((width, heads * early), BF),
                vmem((width, heads * late), BF),
                vmem((width, early), F32),
                vmem((width, late), F32),
                vmem(fw.shape, BF),
                vmem((both * n_half, width), F32),
                vmem((both * n_half, width), BF),
                vmem((both * n_quart, width), F32),
                vmem((both * n_quart, width), BF),
                vmem((width, heads * both * n_half), BF),
                vmem((both * n_half, width), BF),
                vmem((lines, both * n_half), BF),
                vmem((both * n_half, heads * pair), F32),
                vmem((both * n_half, heads * pair), BF),
                vmem((width, both * n_half), BF),
                vmem(rw.shape, BF),
                vmem(up.shape[::-1], BF),
                vmem((span, heads * early), F32),
                vmem((span, heads * late), F32),
                vmem((span, heads * early), BF),
                vmem((span, heads * late), BF),
                vmem((heads * (HD + 16), early), F32),
                vmem((heads * (HD + 16), late), F32),
                vmem((8, heads * early), F32),
                vmem((8, heads * late), F32),
                vmem((2, span, width), BF),
                vmem((2, heads * (HD + 16), span), BF),
                vmem((up.shape[1], early), F32),
                vmem((up.shape[1], early), BF),
            ]
            boxes = [
                vmem((2, quad, n_train * width // 256, 128), BF),
                vmem((2, quad, n_train * width // 256, 128), BF),
                vmem((2, quad, n_train * width // 256, 128), BF),
                vmem((2, quad, n_test * width // 256, 128), BF),
                vmem((2, quad, n_test * width // 256, 128), BF),
                vmem((3, 2, quad, n_train * width // 256, 128), BF),
            ]
            flags = [
                dma((2,)),
                dma((2,)),
                dma((2, 2, quad)),
                dma((2, 2, quad)),
                dma((4, 2)),
                dma((3, 2)),
                dma((quad,)),
                dma((quad,)),
                pltpu.SemaphoreType.REGULAR((2,)),
            ]
        else:
            body_fn = kernel
            swapped = [vmem(train.shape, BF), vmem(test.shape, BF)]
            work = [
                vmem((heads, quad * cell_rows, keys), F32),
                vmem((keys, 256), BF),
                vmem((heads, quad * cell_rows, width), BF),
            ]
            boxes = [
                vmem((2, quad, n_train * width // 256, 128), BF),
                vmem((2, quad, n_train * width // 256, 128), BF),
                vmem((quad, n_test * width // 128, 128), BF),
                vmem((quad, n_test * width // 128, 128), BF),
                vmem((groups_n, 2, span * width // 256, 128), BF),
            ]
            flags = [
                dma((3,)),
                dma((3,)),
                dma((3, quad)),
                dma((3, quad)),
                dma((2, half, 2)),
                dma((2, half, 2)),
                dma((quad,)),
                dma((quad,)),
            ]
        back = pl.pallas_call(
            functools.partial(body_fn, rows_n, feats_n),
            out_shape=pltpu.VMEM((quad, packed, 128), BF),
            in_specs=[aspec, aspec, aspec, aspec, aspec, aspec],
            out_specs=vspec,
            scratch_shapes=[
                *(vmem(w.shape, BF) for w in weights),
                vmem(train.shape, BF),
                vmem(test.shape, BF),
                *swapped,
                *boxes,
                *work,
                vmem((quad, packed, 128), BF),
                dma((6,)),
                *flags,
            ],
            compiler_params=pltpu.CompilerParams(
                collective_id=0, has_side_effects=True, vmem_limit_bytes=60 * 1024 * 1024
            ),
            name="layer",
        )(train, test, *weights)
        return pl.pallas_call(
            place_fn,
            out_shape=(
                jax.ShapeDtypeStruct(train.shape, BF),
                jax.ShapeDtypeStruct(test.shape, BF),
            ),
            in_specs=[vspec],
            out_specs=(vspec, vspec),
            name="place",
        )(pltpu.with_memory_space_constraint(back, pltpu.VMEM))

    return jax.shard_map(
        body,
        mesh=mesh,
        in_specs=(P("rows", "feat"), P("rows", "feat"), P(), P(), P(), P()),
        out_specs=(P("rows", "feat"), P("rows", "feat")),
        check_vma=False,
    )
```

```python
import functools

import jax
import jax.numpy as jnp
from jax import lax
from jax.experimental import pallas as pl
from jax.experimental.pallas import tpu as pltpu
from jax.sharding import PartitionSpec as P

HD = 32
EPS = 1e-05
LOG2E = 1.4426950408889634
MESH = pl.DeviceIdType.MESH
BF = jnp.bfloat16
F32 = jnp.float32


def layer_norm(x):
    centred = x - jnp.mean(x, axis=-1, keepdims=True)
    spread = jnp.mean(centred * centred, axis=-1, keepdims=True)
    return centred * lax.rsqrt(spread + EPS)


def dot(a, b):
    return jnp.dot(a, b, preferred_element_type=F32)


def dot_t(a, b):
    return lax.dot_general(a, b, (((1,), (1,)), ((), ())), preferred_element_type=F32)


def pack(x):
    n = x.shape[0]
    low = jnp.concatenate([x[: n // 2, 128:], x[n // 2 :, 128:]], axis=1)
    return jnp.concatenate([x[:, :128], low], axis=0)


def unpack(p):
    n = p.shape[0] * 2 // 3
    low = p[n:]
    high = jnp.concatenate([low[:, :64], low[:, 64:]], axis=0)
    return jnp.concatenate([p[:n], high], axis=1)


def gelu(x):
    return 0.5 * x * (1.0 + lax.erf(x * (0.5**0.5)))


def kernel(
    rows_n,
    feats_n,
    train_hbm,
    test_hbm,
    fw_hbm,
    rw_hbm,
    up_hbm,
    down_hbm,
    back_in,
    fw,
    rw,
    up,
    down,
    train_ref,
    test_ref,
    o_train,
    o_test,
    outbox,
    inbox,
    t_outbox,
    t_inbox,
    ring,
    scores,
    values,
    queries,
    back_out,
    w_sem,
    f_send,
    f_recv,
    q_send,
    q_recv,
    r_send,
    r_recv,
    b_send,
    b_recv,
):
    width = fw.shape[-1]
    quad = t_outbox.shape[0]
    heads = width // HD
    groups_n = rows_n // quad
    half = groups_n // 2
    n_train = train_ref.shape[0]
    n_test = test_ref.shape[0]
    n_half = n_train // 2
    scale = LOG2E * HD ** (-0.5)

    my_row = lax.axis_index("rows")
    my_feat = lax.axis_index("feat")
    member = lax.rem(my_row, quad)
    group = my_row // quad

    def partner(k):
        low, high = lax.rem(member, 2), member // 2
        return (1 - high if k // 2 else high) * 2 + (1 - low if k % 2 else low)

    def mate(k):
        return group * quad + partner(k)

    right = lax.rem(group + 1, groups_n) * quad + member
    left = lax.rem(group + groups_n - 1, groups_n) * quad + member
    other = lax.rem(my_feat + 1, feats_n)

    loads = [
        pltpu.make_async_copy(s, d, w_sem.at[i])
        for i, (s, d) in enumerate(
            [
                (train_hbm, train_ref),
                (fw_hbm, fw),
                (test_hbm, test_ref),
                (rw_hbm, rw),
                (up_hbm, up),
                (down_hbm, down),
            ]
        )
    ]
    for c in loads:
        c.start()

    barrier = pltpu.get_barrier_semaphore()
    pl.semaphore_signal(barrier, inc=1, device_id={"feat": other}, device_id_type=MESH)
    for k in range(1, quad):
        pl.semaphore_signal(barrier, inc=1, device_id={"rows": mate(k)}, device_id_type=MESH)
    for d in (right, left):
        pl.semaphore_signal(barrier, inc=1, device_id={"rows": d}, device_id_type=MESH)
    pl.semaphore_wait(barrier, quad + 2)

    halves = [pl.ds(p * n_half, n_half) for p in range(2)]
    swaps = [
        pltpu.make_async_remote_copy(
            src_ref=s,
            dst_ref=d,
            send_sem=f_send.at[i],
            recv_sem=f_recv.at[i],
            device_id={"feat": other},
            device_id_type=MESH,
        )
        for i, (s, d) in enumerate(
            [(train_hbm.at[r], o_train.at[r]) for r in halves] + [(test_hbm, o_test)]
        )
    ]
    for c in swaps:
        c.start()

    def feature_rows(table):
        return jnp.concatenate(
            [table[:, f * width : (f + 1) * width].astype(F32) for f in range(quad)], axis=0
        )

    def split(x):
        n = x.shape[0] // quad
        return [x[f * n : (f + 1) * n] for f in range(quad)]

    def key_value(normed):
        return split(dot(normed, fw[1]).astype(BF)), split(dot(normed, fw[2]).astype(BF))

    same = (
        lax.broadcasted_iota(jnp.int32, (width, width), 0) // HD
        == lax.broadcasted_iota(jnp.int32, (width, width), 1) // HD
    )
    spread = jnp.where(same, 1.0, 0.0).astype(BF)

    def own_side(table):
        cells = feature_rows(table)
        normed = layer_norm(cells).astype(BF)
        q = split((dot(normed, fw[0]) * scale).astype(BF))
        ks, vs = key_value(normed)
        return cells, q, ks, vs

    def feature_attention(own, table):
        cells, q, ks, vs = own
        n = table.shape[0]
        more_k, more_v = key_value(layer_norm(feature_rows(table)).astype(BF))
        ks, vs = ks + more_k, vs + more_v
        mixes = []
        for f in range(quad):
            prod = jnp.concatenate([q[f] * k for k in ks], axis=0)
            s = dot(prod, spread)
            s = [s[g * n : (g + 1) * n] for g in range(len(ks))]
            top = functools.reduce(jnp.maximum, s)
            total = None
            mix = None
            for g in range(len(ks)):
                e = jnp.exp2(s[g] - top)
                t = e * vs[g].astype(F32)
                total = e if total is None else total + e
                mix = t if mix is None else mix + t
            mixes.append((mix / total).astype(BF))
        feat_out = dot(jnp.concatenate(mixes, axis=0), fw[3])
        return split((cells + feat_out).astype(BF))

    def to_mates(box, landing, stage):
        copies = {}
        for k in (2, 3, 1):
            copies[k] = pltpu.make_async_remote_copy(
                src_ref=box.at[partner(k)],
                dst_ref=landing.at[k],
                send_sem=q_send.at[stage, k],
                recv_sem=q_recv.at[stage, k],
                device_id={"rows": mate(k)},
                device_id_type=MESH,
            )
            copies[k].start()
        landing[0] = box[member]
        return copies

    loads[0].wait()
    loads[1].wait()
    own = [own_side(train_ref[p * n_half : (p + 1) * n_half]) for p in range(2)]
    moved = []
    boxes = [(outbox.at[p], inbox.at[p]) for p in range(2)] + [(t_outbox, t_inbox)]
    for p in range(2):
        swaps[p].wait()
        for f, x in enumerate(feature_attention(own[p], o_train[p * n_half : (p + 1) * n_half])):
            outbox[p, f] = pack(x)
        moved.append(to_mates(*boxes[p], p))
    loads[2].wait()
    own_test = own_side(test_ref[...])
    swaps[2].wait()
    for f, x in enumerate(feature_attention(own_test, o_test[...])):
        t_outbox[f] = pack(x)
    moved.append(to_mates(*boxes[2], 2))

    def hop(way, h, p):
        last = h == half - 1
        src = 0 if h == 0 else 2 * h - 1 + way
        dst = 2 * half - 1 if last else 1 + 2 * h + way
        return pltpu.make_async_remote_copy(
            src_ref=ring.at[src, p],
            dst_ref=ring.at[dst, p],
            send_sem=r_send.at[way, h, p],
            recv_sem=r_recv.at[way, h, p],
            device_id={"rows": left if way else right},
            device_id_type=MESH,
        )

    def pieces(way, h):
        return (way,) if h == half - 1 else (way, 1 - way)

    hops = {}
    after = []
    normed = []

    def arrive(stage):
        for k in range(1, quad):
            moved[stage][k].wait_recv()
        landing = boxes[stage][1]
        after.append(
            jnp.concatenate([unpack(landing[k]) for k in range(quad)], axis=0).astype(F32)
        )
        normed.append(layer_norm(after[stage]).astype(BF))

    for p in range(2):
        arrive(p)
        ring[0, p] = pack(normed[p])
        for way in (p, 1 - p):
            if p in pieces(way, 0):
                hops[way, 0, p] = hop(way, 0, p)
                hops[way, 0, p].start()

    loads[3].wait()
    lane_head = lax.broadcasted_iota(jnp.int32, (1, width), 1) // HD
    n_query = quad * (n_train + n_test)
    n_side = n_query // 2
    sizes = [2 * n_half, 2 * n_half, 2 * n_test]
    begins = [0, 2 * n_half, 4 * n_half]
    all_rows = [slice(0, n_query)]
    train_rows = [slice(i * n_side, i * n_side + begins[2]) for i in range(2)]
    test_rows = [slice(i * n_side + begins[2], (i + 1) * n_side) for i in range(2)]
    span = quad * n_train
    values[:, width:] = jnp.ones_like(values[:, width:])

    def ask(stage):
        q_all = (dot(normed[stage], rw[0]) * scale).astype(BF)
        n = sizes[stage]
        for h in range(heads):
            one = jnp.where(lane_head == h, q_all, jnp.zeros_like(q_all))
            for i in range(2):
                at = i * n_side + begins[stage]
                queries[h, at : at + n] = one[(1 - i) * n : (2 - i) * n]

    def take(slot, column):
        x = jnp.concatenate([unpack(ring[slot, 0]), unpack(ring[slot, 1])], axis=0)
        values[column * span : (column + 1) * span, :width] = dot(x, rw[2]).astype(BF)
        return dot(x, rw[1]).astype(BF)

    def score(key, column, rows):
        for h in range(heads):
            for r in rows:
                scores[h, r, column * span : (column + 1) * span] = dot_t(queries[h, r], key)

    def attend(h, rows, columns, carried):
        s = scores[h, rows, columns]
        top = jnp.max(s, axis=-1, keepdims=True)
        if carried is not None:
            top = jnp.maximum(top, carried[0])
        e = jnp.exp2(s - top).astype(BF)
        out = dot(e, values[columns])
        if carried is not None:
            out = out + carried[1] * jnp.exp2(carried[0] - top)
        return top, out

    ask(0)
    ask(1)
    everything = slice(0, n_query)
    if half <= 2:
        own_key = take(0, 0)
        score(own_key, 0, train_rows)
    arrive(2)
    ask(2)
    if half <= 2:
        score(own_key, 0, test_rows)
        states = [attend(h, everything, slice(0, span), None) for h in range(heads)]

    for h in range(half - 1):
        for way in range(2):
            for p in pieces(way, h + 1):
                hops[way, h, p].wait_recv()
                hops[way, h + 1, p] = hop(way, h + 1, p)
                hops[way, h + 1, p].start()
        for way in range(2):
            for p in pieces(way, h):
                if p not in pieces(way, h + 1):
                    hops[way, h, p].wait_recv()

    if half == 2:
        for slot in (1, 2):
            score(take(slot, slot), slot, all_rows)
        states = [
            attend(h, everything, slice(span, 3 * span), states[h]) for h in range(heads)
        ]

    for way in range(2):
        for p in pieces(way, half - 1):
            hops[way, half - 1, p].wait_recv()

    if half <= 2:
        last = 2 * half - 1
        last_key = take(last, last)
        columns = slice(last * span, (last + 1) * span)
    else:
        per = scores.shape[2] // span

        def step(i, states):
            for j in range(per):
                score(take(i * per + j, j), j, all_rows)
            return [attend(h, everything, slice(0, per * span), states[h]) for h in range(heads)]

        start = [
            (
                jnp.full((n_query, 1), -1e30, F32),
                jnp.zeros((n_query, values.shape[1]), F32),
            )
            for _ in range(heads)
        ]
        states = lax.fori_loop(0, groups_n // per, step, start)

    for c in loads[4:]:
        c.wait()
    returns = []
    for i, pair in enumerate(((2, 3), (0, 1))):
        rows = slice(i * n_side, (i + 1) * n_side)
        side = [tuple(x[rows] for x in states[h]) for h in range(heads)]
        if half <= 2:
            score(last_key, last, [rows])
            side = [attend(h, rows, columns, side[h]) for h in range(heads)]
        mixed = None
        for h in range(heads):
            out = side[h][1]
            part = out[:, :width] * (1.0 / out[:, width : width + 1])
            mixed = part if h == 0 else jnp.where(lane_head == h, part, mixed)
        before = [x[(1 - i) * n : (2 - i) * n] for x, n in zip(after, sizes)]
        after_row = jnp.concatenate(before, axis=0) + dot(mixed.astype(BF), rw[3])
        hidden = gelu(dot(layer_norm(after_row).astype(BF), up[...])).astype(BF)
        done = (after_row + dot_t(hidden, down[...])).astype(BF)
        for j, k in enumerate(pair):
            block = pack(
                jnp.concatenate(
                    [
                        done[b + j * (n // 2) : b + (j + 1) * (n // 2)]
                        for b, n in zip(begins, sizes)
                    ],
                    axis=0,
                )
            )
            back_out[k] = block
            if k == 0:
                c = pltpu.make_async_copy(back_out.at[0], back_in.at[member], b_send.at[0])
                c.start()
                returns.append(c)
                continue
            c = pltpu.make_async_remote_copy(
                src_ref=back_out.at[k],
                dst_ref=back_in.at[member],
                send_sem=b_send.at[k],
                recv_sem=b_recv.at[k],
                device_id={"rows": mate(k)},
                device_id_type=MESH,
            )
            c.start()
            returns.append(c)
    for c in returns:
        c.wait()
    for c in [*hops.values(), *(c for m in moved for c in m.values())]:
        c.wait_send()


def unpack_blocks(p):
    n = p.shape[1] * 2 // 3
    count = p.shape[0]
    low = p[:, n:]
    high = jnp.concatenate([low[:, :, :64], low[:, :, 64:]], axis=1)
    first = p[:, :n].reshape(count * n, 128)
    return jnp.concatenate([first, high.reshape(count * n, 64)], axis=1)


def plane_kernel(
    rows_n,
    feats_n,
    train_hbm,
    test_hbm,
    fw_hbm,
    rw_hbm,
    up_hbm,
    down_hbm,
    back_in,
    fw,
    rw,
    up,
    down,
    train_ref,
    test_ref,
    o_train,
    o_test,
    zbox,
    abox,
    a_in,
    t_box,
    t_in,
    ring,
    early_q,
    late_q,
    early_x,
    late_x,
    fw_t,
    f_cells,
    f_x,
    t_cells,
    t_x,
    fq,
    fk,
    fv,
    fs,
    fe,
    fm,
    rw_t,
    asks,
    up_t,
    early_s,
    late_s,
    early_e,
    late_e,
    early_sum,
    late_sum,
    early_top,
    late_top,
    keys,
    vals,
    raised,
    hidden,
    back_out,
    w_sem,
    f_send,
    f_recv,
    a_send,
    a_recv,
    r_send,
    r_recv,
    b_send,
    b_recv,
    gate,
):
    width = fw.shape[-1]
    quad = t_box.shape[1]
    heads = width // HD
    groups_n = rows_n // quad
    n_train = train_ref.shape[0]
    n_test = test_ref.shape[0]
    n_half, n_quart = n_train // 2, n_test // 2
    scale = LOG2E * HD ** (-0.5)

    my_row = lax.axis_index("rows")
    my_feat = lax.axis_index("feat")
    member = lax.rem(my_row, quad)
    group = my_row // quad

    def partner(k):
        low, high = lax.rem(member, 2), member // 2
        return (1 - high if k // 2 else high) * 2 + (1 - low if k % 2 else low)

    def mate(k):
        return group * quad + partner(k)

    right_group = lax.rem(group + 1, groups_n)
    left_group = lax.rem(group + groups_n - 1, groups_n)
    right = right_group * quad + member
    left = left_group * quad + member
    other = lax.rem(my_feat + 1, feats_n)

    loads = [
        pltpu.make_async_copy(s, d, w_sem.at[i])
        for i, (s, d) in enumerate(
            [
                (train_hbm, train_ref),
                (fw_hbm, fw),
                (test_hbm, test_ref),
                (rw_hbm, rw),
                (up_hbm, up),
                (down_hbm, down),
            ]
        )
    ]
    for c in loads:
        c.start()

    barrier = pltpu.get_barrier_semaphore()
    even = lax.rem(member, 2) == 0

    def greet(**where):
        pl.semaphore_signal(barrier, inc=1, device_id=where, device_id_type=MESH)

    def tell(i):
        pl.semaphore_signal(
            gate.at[i], inc=1, device_id={"rows": mate(1)}, device_id_type=MESH
        )

    @pl.when(even)
    def _():
        greet(rows=my_row, feat=other)
        for g in (group, right_group, left_group):
            for m in range(1, quad, 2):
                for y in (my_feat, other):
                    greet(rows=g * quad + m, feat=y)
        pl.semaphore_wait(barrier, 3)
        tell(0)

    @pl.when(jnp.logical_not(even))
    def _():
        greet(rows=mate(1))
        greet(rows=mate(1), feat=other)
        greet(rows=my_row, feat=other)
        for y in (my_feat, other):
            greet(rows=mate(2), feat=y)
            for g in (right_group, left_group):
                for m in range(1, quad, 2):
                    greet(rows=g * quad + m, feat=y)
        pl.semaphore_wait(gate.at[0], 1)

    swaps = [
        pltpu.make_async_remote_copy(
            src_ref=s,
            dst_ref=d,
            send_sem=f_send.at[i],
            recv_sem=f_recv.at[i],
            device_id={"feat": other},
            device_id_type=MESH,
        )
        for i, (s, d) in enumerate(
            [
                (train_hbm.at[pl.ds(pl.multiple_of(other * n_half, n_half), n_half)], o_train),
                (test_hbm.at[pl.ds(pl.multiple_of(other * n_quart, n_quart), n_quart)], o_test),
            ]
        )
    ]
    for c in swaps:
        c.start()

    tile = 16
    cell = quad * tile
    pair = 2 * cell
    lines = HD + 16
    same_row = (
        lax.broadcasted_iota(jnp.int32, (pair, heads * pair), 0) % tile
        == lax.broadcasted_iota(jnp.int32, (pair, heads * pair), 1) % tile
    )

    def fill(table, side, cells_ref, x_ref):
        n = table.shape[0] // tile
        cells = jnp.concatenate(
            [
                table[b * tile : (b + 1) * tile, f * width : (f + 1) * width].astype(F32)
                for b in range(n)
                for f in range(quad)
            ],
            axis=0,
        )
        normed = layer_norm(cells).astype(BF)
        for b in range(n):
            to = slice((2 * b + side) * cell, (2 * b + side + 1) * cell)
            cells_ref[to] = cells[b * cell : (b + 1) * cell]
            x_ref[to] = normed[b * cell : (b + 1) * cell]

    def normed_columns(x):
        centred = x - jnp.mean(x, axis=0, keepdims=True)
        spread = jnp.mean(centred * centred, axis=0, keepdims=True)
        return centred * lax.rsqrt(spread + EPS)

    def feature_attention(cells_ref, x_ref):
        n = x_ref.shape[0]
        blocks = [slice(b * pair, (b + 1) * pair) for b in range(n // pair)]
        x = x_ref[...]
        q = (dot_t(fw_t[0], x) * scale).astype(BF)
        fk[:n] = dot(x, fw[1]).astype(BF)
        v = dot_t(fw_t[2], x).astype(BF)
        for h in range(heads):
            rows = slice(h * HD, (h + 1) * HD)
            fv[h * lines : h * lines + HD, :n] = v[rows]
            for b, at in enumerate(blocks):
                fq[rows, (b * heads + h) * pair : (b * heads + h + 1) * pair] = q[rows, at]
        for b, at in enumerate(blocks):
            fs[at] = dot(fk[at], fq[:, b * heads * pair : (b + 1) * heads * pair])
        for at in blocks:
            s = jnp.where(same_row, fs[at], -1e30)
            fe[at] = jnp.exp2(s - jnp.max(s, axis=0, keepdims=True)).astype(BF)
        for at in blocks:
            for h in range(heads):
                out = dot(
                    fv[h * lines : (h + 1) * lines, at], fe[at, h * pair : (h + 1) * pair]
                )
                part = out[:HD] * (1.0 / out[HD : HD + 1])
                fm[h * HD : (h + 1) * HD, at] = part.astype(BF)
        after = cells_ref[...].T + dot(fw_t[3], fm[:, :n])
        return after, normed_columns(after)

    def sides(x):
        n = x.shape[0] // pair
        for j in range(2):
            for f in range(quad):
                at = [(2 * b + j) * cell + f * tile for b in range(n)]
                yield j, f, jnp.concatenate([x[i : i + tile] for i in at], axis=0)

    feats = (my_feat, other)

    def to_mates(box, landing, stage):
        copies = []
        for k, j in ((2, 0), (0, 1), (3, 0), (1, 1), (2, 1), (3, 1), (1, 0)):
            pltpu.make_async_remote_copy(
                src_ref=box.at[j, partner(k)],
                dst_ref=landing.at[j, k],
                send_sem=a_send.at[stage, j],
                recv_sem=a_recv.at[stage, j],
                device_id={"rows": mate(k), "feat": feats[j]},
                device_id_type=MESH,
            ).start()
        landing[0, 0] = box[0, member]
        return [
            pltpu.make_async_remote_copy(
                src_ref=part,
                dst_ref=part,
                send_sem=a_send.at[stage, j],
                recv_sem=a_recv.at[stage, j],
                device_id={"rows": mate(1)},
                device_id_type=MESH,
            )
            for j, part in enumerate((landing.at[0, pl.ds(1, quad - 1)], landing.at[1]))
        ]

    inner = jnp.logical_and(group > 0, group < groups_n - 1)

    def to_group(way, p, k):
        g = jnp.where(way == 1, left_group, right_group)
        return pltpu.make_async_remote_copy(
            src_ref=zbox.at[p, partner(k)],
            dst_ref=ring.at[way, p, k],
            send_sem=r_send.at[0],
            recv_sem=r_recv.at[way, p],
            device_id={"rows": g * quad + partner(k), "feat": feats[p]},
            device_id_type=MESH,
        )

    def whole(slot, p):
        return pltpu.make_async_remote_copy(
            src_ref=ring.at[slot, p],
            dst_ref=ring.at[slot, p],
            send_sem=r_send.at[0],
            recv_sem=r_recv.at[slot, p],
            device_id={"rows": right},
            device_id_type=MESH,
        )

    def onward(way, p):
        return pltpu.make_async_remote_copy(
            src_ref=ring.at[way, p],
            dst_ref=ring.at[2, p],
            send_sem=r_send.at[1],
            recv_sem=r_recv.at[2, p],
            device_id={"rows": left if way else right},
            device_id_type=MESH,
        )

    def relay(p):
        @pl.when(inner)
        def _():
            for way in range(2):
                whole(way, p).wait_recv()
                onward(way, p).start()

    loads[0].wait()
    loads[1].wait()
    fill(train_ref[pl.ds(pl.multiple_of(my_feat * n_half, n_half), n_half)], 0, f_cells, f_x)
    for i in (0, 2, 3):
        fw_t[i] = fw[i].astype(F32).T.astype(BF)
    loads[2].wait()
    fill(test_ref[pl.ds(pl.multiple_of(my_feat * n_quart, n_quart), n_quart)], 0, t_cells, t_x)
    fq[...] = jnp.zeros_like(fq)
    fv[...] = jnp.ones_like(fv)

    @pl.when(jnp.logical_not(even))
    def _():
        pl.semaphore_wait(barrier, 6 * quad - 1)
        tell(1)

    swaps[0].wait()
    fill(o_train[...], 1, f_cells, f_x)
    after_own, normed_own = feature_attention(f_cells, f_x)
    for j, f, x in sides(normed_own.T):
        zbox[j, f] = pack(x.astype(BF))

    @pl.when(even)
    def _():
        pl.semaphore_wait(gate.at[1], 1)

    near = jnp.where(group == groups_n - 1, 1, 0)
    for k in range(2):
        to_group(near, 0, k).start()
    for j, f, x in sides(after_own.T):
        abox[j, f] = pack(x.astype(BF))
    moved = [to_mates(abox, a_in, 0)]
    for way in (near, 1 - near):
        for p in range(2):
            for k in range(quad):
                if way is not near or p or k > 1:
                    to_group(way, p, k).start()
    swaps[1].wait()
    fill(o_test[...], 1, t_cells, t_x)
    after_own, _ = feature_attention(t_cells, t_x)
    for j, f, x in sides(after_own.T):
        t_box[j, f] = pack(x.astype(BF))
    moved.append(to_mates(t_box, t_in, 1))

    loads[3].wait()
    for i in (2, 3):
        rw_t[i] = rw[i].astype(F32).T.astype(BF)
    lane_head = lax.broadcasted_iota(jnp.int32, (1, width), 1) // HD
    for h in range(heads):
        one = jnp.where(lane_head == h, rw[1], jnp.zeros_like(rw[1]))
        asks[h * width : (h + 1) * width] = (dot_t(one, rw[0]) * scale).astype(BF)
    loads[4].wait()
    up_t[...] = up[...].astype(F32).T.astype(BF)
    vals[...] = jnp.ones_like(vals)

    def arrive(stage):
        for c in moved[stage]:
            c.wait_recv()
        landing = (a_in, t_in)[stage]
        x = jnp.concatenate(
            [unpack(landing[j, k]) for k in range(quad) for j in range(2)], axis=0
        ).astype(F32)
        normed = layer_norm(x).astype(BF)
        return x, normed, dot_t(asks[...], normed).astype(BF)

    n_mid = 2 * n_train
    n_late = 2 * n_train
    n_early = n_mid + quad * n_test

    def place_queries(q, into, size, at):
        n = q.shape[1]
        for h in range(heads):
            into[:, h * size + at : h * size + at + n] = q[h * width : (h + 1) * width]

    late = (late_q, late_s, late_e, late_sum, late_top, n_late)
    early = (early_q, early_s, early_e, early_sum, early_top, n_early)

    def key_value_rows(x, i):
        keys[i] = x
        value = dot_t(rw_t[2], x).astype(BF)
        for h in range(heads):
            vals[i, h * lines : h * lines + HD] = value[h * HD : (h + 1) * HD]

    def attend(asked, i, first=False):
        per_head = [
            (part, h, slice(h * part[5], (h + 1) * part[5]), slice(h * lines, (h + 1) * lines))
            for part in asked
            for h in range(heads)
        ]
        key = keys[i]
        for (q, s, _, _, _, _), h, c, _ in per_head:
            s[:, c] = dot(key, q[:, c])
        for (_, s, e, total, tops, _), h, c, r in per_head:
            top = jnp.max(s[:, c], axis=0, keepdims=True)
            if not first:
                old = tops[0:1, c]
                top = jnp.maximum(top, old)
                total[r] = total[r] * jnp.exp2(old - top)
            e[:, c] = jnp.exp2(s[:, c] - top).astype(BF)
            tops[0:1, c] = top
        for (_, _, e, total, _, _), h, c, r in per_head:
            out = dot(vals[i, r], e[:, c])
            total[r] = out if first else total[r] + out

    def finish(part, before):
        total = part[3]
        mix = jnp.concatenate(
            [
                total[h * lines : h * lines + HD]
                * (1.0 / total[h * lines + HD : h * lines + HD + 1])
                for h in range(heads)
            ],
            axis=0,
        ).astype(BF)
        after_row = before + dot(rw_t[3], mix)
        normed = normed_columns(after_row).astype(BF)
        n = normed.shape[1]
        raised[:, :n] = dot(up_t[...], normed)
        hidden[:, :n] = gelu(raised[:, :n]).astype(BF)
        return (after_row + dot(down[...], hidden[:, :n])).T.astype(BF)

    at_start = group == 0
    order = (jnp.where(at_start, 1, 0), jnp.where(at_start, 0, 1), 2)

    def landed(i):
        slot = order[i]

        @pl.when(jnp.logical_not(jnp.logical_and(inner, slot < 2)))
        def _():
            for p in range(2):
                whole(slot, p).wait_recv()

    def fetch(i):
        slot = order[i]
        x = jnp.concatenate([unpack_blocks(ring[slot, p]) for p in range(2)], axis=0)
        key_value_rows(x, (i + 1) % 2)

    relay(0)
    x, normed, q = arrive(0)
    place_queries(q[:, n_mid:], early_q, n_early, 0)
    place_queries(q[:, :n_late], late_q, n_late, 0)
    early_x[:, :n_mid] = x[n_late:].T
    late_x[...] = x[:n_late].T
    key_value_rows(normed, 0)
    relay(1)
    attend([late], 0, True)
    landed(0)
    x, _, q = arrive(1)
    place_queries(q, early_q, n_early, n_mid)
    early_x[:, n_mid:] = x.T
    fetch(0)
    attend([late], 1)
    attend([early], 0, True)
    attend([early], 1)
    landed(1)
    fetch(1)
    attend([late, early], 0)
    landed(2)
    fetch(2)
    loads[5].wait()

    def give_back(k, done, tests):
        block = jnp.concatenate([done, tests[k * n_test : (k + 1) * n_test]], axis=0)
        if k == 0:
            back_in[member] = pack(block)
            return
        back_out[k] = pack(block)
        pltpu.make_async_remote_copy(
            src_ref=back_out.at[k],
            dst_ref=back_in.at[member],
            send_sem=b_send.at[0],
            recv_sem=b_recv.at[0],
            device_id={"rows": mate(k)},
            device_id_type=MESH,
        ).start()

    attend([early], 1)
    done = finish(early, early_x[...])
    tests = done[n_mid:]
    for k in (2, 3):
        give_back(k, done[(k - 2) * n_train : (k - 1) * n_train], tests)
    attend([late], 1)
    done = finish(late, late_x[...])
    for k in (1, 0):
        give_back(k, done[k * n_train : (k + 1) * n_train], tests)
    pltpu.make_async_remote_copy(
        src_ref=back_out.at[pl.ds(1, quad - 1)],
        dst_ref=back_in.at[pl.ds(1, quad - 1)],
        send_sem=b_send.at[0],
        recv_sem=b_recv.at[0],
        device_id={"rows": mate(1)},
        device_id_type=MESH,
    ).wait()
    for c in [*moved[0], *moved[1]]:
        c.wait_send()

    def sent(i):
        pltpu.make_async_remote_copy(
            src_ref=ring.at[pl.ds(0, 2)],
            dst_ref=ring.at[pl.ds(0, 2)],
            send_sem=r_send.at[i],
            recv_sem=r_recv.at[0, 0],
            device_id={"rows": right},
            device_id_type=MESH,
        ).wait_send()

    sent(0)

    @pl.when(inner)
    def _():
        sent(1)


def place_halves(back_ref, train_out, test_out):
    quad = back_ref.shape[0]
    result = jnp.concatenate([unpack(back_ref[f]) for f in range(quad)], axis=1)
    in_order = lax.axis_index("feat") == 0
    begin = 0
    for out in (train_out, test_out):
        half = out.shape[0] // 2
        one, two = (result[begin + j * half : begin + (j + 1) * half] for j in range(2))
        out[:half] = jnp.where(in_order, one, two)
        out[half:] = jnp.where(in_order, two, one)
        begin += 2 * half


def place(back_ref, train_out, test_out):
    quad = back_ref.shape[0]
    result = jnp.concatenate([unpack(back_ref[f]) for f in range(quad)], axis=1)
    n_train = train_out.shape[0]
    train_out[...] = result[:n_train]
    test_out[...] = result[n_train:]


def solution(mesh):
    rows_n = mesh.shape["rows"]
    feats_n = mesh.shape["feat"]

    def body(train, test, fw, rw, up, down):
        width = fw.shape[-1]
        quad = train.shape[1] // width
        heads = width // HD
        n_train, n_test = train.shape[0], test.shape[0]
        cell_rows = n_train + n_test
        groups_n = rows_n // quad
        half = groups_n // 2
        span = quad * n_train
        keys = min(groups_n, 4) * span
        packed = cell_rows * width // 128
        vmem = pltpu.VMEM
        dma = pltpu.SemaphoreType.DMA
        vspec = pl.BlockSpec(memory_space=pltpu.VMEM)
        aspec = pl.BlockSpec(memory_space=pl.ANY)
        weights = (fw, rw, up, down.T)
        place_fn = place
        fits = groups_n == 4 and quad == 4 and feats_n == 2
        if fits and n_train % 32 == 0 and n_test % 32 == 0:
            body_fn, place_fn = plane_kernel, place_halves
            n_half, n_quart = n_train // 2, n_test // 2
            swapped = [vmem((n_half, quad * width), BF), vmem((n_quart, quad * width), BF)]
            both = 2 * quad
            pair = both * 16
            lines = heads * (HD + 16)
            early, late = 2 * n_train + quad * n_test, 2 * n_train
            work = [
                vmem((width, heads * early), BF),
                vmem((width, heads * late), BF),
                vmem((width, early), F32),
                vmem((width, late), F32),
                vmem(fw.shape, BF),
                vmem((both * n_half, width), F32),
                vmem((both * n_half, width), BF),
                vmem((both * n_quart, width), F32),
                vmem((both * n_quart, width), BF),
                vmem((width, heads * both * n_half), BF),
                vmem((both * n_half, width), BF),
                vmem((lines, both * n_half), BF),
                vmem((both * n_half, heads * pair), F32),
                vmem((both * n_half, heads * pair), BF),
                vmem((width, both * n_half), BF),
                vmem(rw.shape, BF),
                vmem((heads * width, width), BF),
                vmem(up.shape[::-1], BF),
                vmem((span, heads * early), F32),
                vmem((span, heads * late), F32),
                vmem((span, heads * early), BF),
                vmem((span, heads * late), BF),
                vmem((heads * (HD + 16), early), F32),
                vmem((heads * (HD + 16), late), F32),
                vmem((8, heads * early), F32),
                vmem((8, heads * late), F32),
                vmem((2, span, width), BF),
                vmem((2, heads * (HD + 16), span), BF),
                vmem((up.shape[1], early), F32),
                vmem((up.shape[1], early), BF),
            ]
            boxes = [
                vmem((2, quad, n_train * width // 256, 128), BF),
                vmem((2, quad, n_train * width // 256, 128), BF),
                vmem((2, quad, n_train * width // 256, 128), BF),
                vmem((2, quad, n_test * width // 256, 128), BF),
                vmem((2, quad, n_test * width // 256, 128), BF),
                vmem((3, 2, quad, n_train * width // 256, 128), BF),
            ]
            flags = [
                dma((2,)),
                dma((2,)),
                dma((2, 2)),
                dma((2, 2)),
                dma((2,)),
                dma((3, 2)),
                dma((1,)),
                dma((1,)),
                pltpu.SemaphoreType.REGULAR((2,)),
            ]
        else:
            body_fn = kernel
            swapped = [vmem(train.shape, BF), vmem(test.shape, BF)]
            work = [
                vmem((heads, quad * cell_rows, keys), F32),
                vmem((keys, 256), BF),
                vmem((heads, quad * cell_rows, width), BF),
            ]
            boxes = [
                vmem((2, quad, n_train * width // 256, 128), BF),
                vmem((2, quad, n_train * width // 256, 128), BF),
                vmem((quad, n_test * width // 128, 128), BF),
                vmem((quad, n_test * width // 128, 128), BF),
                vmem((groups_n, 2, span * width // 256, 128), BF),
            ]
            flags = [
                dma((3,)),
                dma((3,)),
                dma((3, quad)),
                dma((3, quad)),
                dma((2, half, 2)),
                dma((2, half, 2)),
                dma((quad,)),
                dma((quad,)),
            ]
        back = pl.pallas_call(
            functools.partial(body_fn, rows_n, feats_n),
            out_shape=pltpu.VMEM((quad, packed, 128), BF),
            in_specs=[aspec, aspec, aspec, aspec, aspec, aspec],
            out_specs=vspec,
            scratch_shapes=[
                *(vmem(w.shape, BF) for w in weights),
                vmem(train.shape, BF),
                vmem(test.shape, BF),
                *swapped,
                *boxes,
                *work,
                vmem((quad, packed, 128), BF),
                dma((6,)),
                *flags,
            ],
            compiler_params=pltpu.CompilerParams(
                collective_id=0, has_side_effects=True, vmem_limit_bytes=60 * 1024 * 1024
            ),
            name="layer",
        )(train, test, *weights)
        return pl.pallas_call(
            place_fn,
            out_shape=(
                jax.ShapeDtypeStruct(train.shape, BF),
                jax.ShapeDtypeStruct(test.shape, BF),
            ),
            in_specs=[vspec],
            out_specs=(vspec, vspec),
            name="place",
        )(pltpu.with_memory_space_constraint(back, pltpu.VMEM))

    return jax.shard_map(
        body,
        mesh=mesh,
        in_specs=(P("rows", "feat"), P("rows", "feat"), P(), P(), P(), P()),
        out_specs=(P("rows", "feat"), P("rows", "feat")),
        check_vma=False,
    )
```

```python
import functools

import jax
import jax.numpy as jnp
from jax import lax
from jax.experimental import pallas as pl
from jax.experimental.pallas import tpu as pltpu
from jax.sharding import PartitionSpec as P

HD = 32
EPS = 1e-05
LOG2E = 1.4426950408889634
MESH = pl.DeviceIdType.MESH
BF = jnp.bfloat16
F32 = jnp.float32


def layer_norm(x):
    centred = x - jnp.mean(x, axis=-1, keepdims=True)
    spread = jnp.mean(centred * centred, axis=-1, keepdims=True)
    return centred * lax.rsqrt(spread + EPS)


def dot(a, b):
    return jnp.dot(a, b, preferred_element_type=F32)


def dot_t(a, b):
    return lax.dot_general(a, b, (((1,), (1,)), ((), ())), preferred_element_type=F32)


def pack(x):
    n = x.shape[0]
    low = jnp.concatenate([x[: n // 2, 128:], x[n // 2 :, 128:]], axis=1)
    return jnp.concatenate([x[:, :128], low], axis=0)


def unpack(p):
    n = p.shape[0] * 2 // 3
    low = p[n:]
    high = jnp.concatenate([low[:, :64], low[:, 64:]], axis=0)
    return jnp.concatenate([p[:n], high], axis=1)


def gelu(x):
    return 0.5 * x * (1.0 + lax.erf(x * (0.5**0.5)))


def kernel(
    rows_n,
    feats_n,
    train_hbm,
    test_hbm,
    fw_hbm,
    rw_hbm,
    up_hbm,
    down_hbm,
    back_in,
    fw,
    rw,
    up,
    down,
    train_ref,
    test_ref,
    o_train,
    o_test,
    outbox,
    inbox,
    t_outbox,
    t_inbox,
    ring,
    scores,
    values,
    queries,
    back_out,
    w_sem,
    f_send,
    f_recv,
    q_send,
    q_recv,
    r_send,
    r_recv,
    b_send,
    b_recv,
):
    width = fw.shape[-1]
    quad = t_outbox.shape[0]
    heads = width // HD
    groups_n = rows_n // quad
    half = groups_n // 2
    n_train = train_ref.shape[0]
    n_test = test_ref.shape[0]
    n_half = n_train // 2
    scale = LOG2E * HD ** (-0.5)

    my_row = lax.axis_index("rows")
    my_feat = lax.axis_index("feat")
    member = lax.rem(my_row, quad)
    group = my_row // quad

    def partner(k):
        low, high = lax.rem(member, 2), member // 2
        return (1 - high if k // 2 else high) * 2 + (1 - low if k % 2 else low)

    def mate(k):
        return group * quad + partner(k)

    right = lax.rem(group + 1, groups_n) * quad + member
    left = lax.rem(group + groups_n - 1, groups_n) * quad + member
    other = lax.rem(my_feat + 1, feats_n)

    loads = [
        pltpu.make_async_copy(s, d, w_sem.at[i])
        for i, (s, d) in enumerate(
            [
                (train_hbm, train_ref),
                (fw_hbm, fw),
                (test_hbm, test_ref),
                (rw_hbm, rw),
                (up_hbm, up),
                (down_hbm, down),
            ]
        )
    ]
    for c in loads:
        c.start()

    barrier = pltpu.get_barrier_semaphore()
    pl.semaphore_signal(barrier, inc=1, device_id={"feat": other}, device_id_type=MESH)
    for k in range(1, quad):
        pl.semaphore_signal(barrier, inc=1, device_id={"rows": mate(k)}, device_id_type=MESH)
    for d in (right, left):
        pl.semaphore_signal(barrier, inc=1, device_id={"rows": d}, device_id_type=MESH)
    pl.semaphore_wait(barrier, quad + 2)

    halves = [pl.ds(p * n_half, n_half) for p in range(2)]
    swaps = [
        pltpu.make_async_remote_copy(
            src_ref=s,
            dst_ref=d,
            send_sem=f_send.at[i],
            recv_sem=f_recv.at[i],
            device_id={"feat": other},
            device_id_type=MESH,
        )
        for i, (s, d) in enumerate(
            [(train_hbm.at[r], o_train.at[r]) for r in halves] + [(test_hbm, o_test)]
        )
    ]
    for c in swaps:
        c.start()

    def feature_rows(table):
        return jnp.concatenate(
            [table[:, f * width : (f + 1) * width].astype(F32) for f in range(quad)], axis=0
        )

    def split(x):
        n = x.shape[0] // quad
        return [x[f * n : (f + 1) * n] for f in range(quad)]

    def key_value(normed):
        return split(dot(normed, fw[1]).astype(BF)), split(dot(normed, fw[2]).astype(BF))

    same = (
        lax.broadcasted_iota(jnp.int32, (width, width), 0) // HD
        == lax.broadcasted_iota(jnp.int32, (width, width), 1) // HD
    )
    spread = jnp.where(same, 1.0, 0.0).astype(BF)

    def own_side(table):
        cells = feature_rows(table)
        normed = layer_norm(cells).astype(BF)
        q = split((dot(normed, fw[0]) * scale).astype(BF))
        ks, vs = key_value(normed)
        return cells, q, ks, vs

    def feature_attention(own, table):
        cells, q, ks, vs = own
        n = table.shape[0]
        more_k, more_v = key_value(layer_norm(feature_rows(table)).astype(BF))
        ks, vs = ks + more_k, vs + more_v
        mixes = []
        for f in range(quad):
            prod = jnp.concatenate([q[f] * k for k in ks], axis=0)
            s = dot(prod, spread)
            s = [s[g * n : (g + 1) * n] for g in range(len(ks))]
            top = functools.reduce(jnp.maximum, s)
            total = None
            mix = None
            for g in range(len(ks)):
                e = jnp.exp2(s[g] - top)
                t = e * vs[g].astype(F32)
                total = e if total is None else total + e
                mix = t if mix is None else mix + t
            mixes.append((mix / total).astype(BF))
        feat_out = dot(jnp.concatenate(mixes, axis=0), fw[3])
        return split((cells + feat_out).astype(BF))

    def to_mates(box, landing, stage):
        copies = {}
        for k in (2, 3, 1):
            copies[k] = pltpu.make_async_remote_copy(
                src_ref=box.at[partner(k)],
                dst_ref=landing.at[k],
                send_sem=q_send.at[stage, k],
                recv_sem=q_recv.at[stage, k],
                device_id={"rows": mate(k)},
                device_id_type=MESH,
            )
            copies[k].start()
        landing[0] = box[member]
        return copies

    loads[0].wait()
    loads[1].wait()
    own = [own_side(train_ref[p * n_half : (p + 1) * n_half]) for p in range(2)]
    moved = []
    boxes = [(outbox.at[p], inbox.at[p]) for p in range(2)] + [(t_outbox, t_inbox)]
    for p in range(2):
        swaps[p].wait()
        for f, x in enumerate(feature_attention(own[p], o_train[p * n_half : (p + 1) * n_half])):
            outbox[p, f] = pack(x)
        moved.append(to_mates(*boxes[p], p))
    loads[2].wait()
    own_test = own_side(test_ref[...])
    swaps[2].wait()
    for f, x in enumerate(feature_attention(own_test, o_test[...])):
        t_outbox[f] = pack(x)
    moved.append(to_mates(*boxes[2], 2))

    def hop(way, h, p):
        last = h == half - 1
        src = 0 if h == 0 else 2 * h - 1 + way
        dst = 2 * half - 1 if last else 1 + 2 * h + way
        return pltpu.make_async_remote_copy(
            src_ref=ring.at[src, p],
            dst_ref=ring.at[dst, p],
            send_sem=r_send.at[way, h, p],
            recv_sem=r_recv.at[way, h, p],
            device_id={"rows": left if way else right},
            device_id_type=MESH,
        )

    def pieces(way, h):
        return (way,) if h == half - 1 else (way, 1 - way)

    hops = {}
    after = []
    normed = []

    def arrive(stage):
        for k in range(1, quad):
            moved[stage][k].wait_recv()
        landing = boxes[stage][1]
        after.append(
            jnp.concatenate([unpack(landing[k]) for k in range(quad)], axis=0).astype(F32)
        )
        normed.append(layer_norm(after[stage]).astype(BF))

    for p in range(2):
        arrive(p)
        ring[0, p] = pack(normed[p])
        for way in (p, 1 - p):
            if p in pieces(way, 0):
                hops[way, 0, p] = hop(way, 0, p)
                hops[way, 0, p].start()

    loads[3].wait()
    lane_head = lax.broadcasted_iota(jnp.int32, (1, width), 1) // HD
    n_query = quad * (n_train + n_test)
    n_side = n_query // 2
    sizes = [2 * n_half, 2 * n_half, 2 * n_test]
    begins = [0, 2 * n_half, 4 * n_half]
    all_rows = [slice(0, n_query)]
    train_rows = [slice(i * n_side, i * n_side + begins[2]) for i in range(2)]
    test_rows = [slice(i * n_side + begins[2], (i + 1) * n_side) for i in range(2)]
    span = quad * n_train
    values[:, width:] = jnp.ones_like(values[:, width:])

    def ask(stage):
        q_all = (dot(normed[stage], rw[0]) * scale).astype(BF)
        n = sizes[stage]
        for h in range(heads):
            one = jnp.where(lane_head == h, q_all, jnp.zeros_like(q_all))
            for i in range(2):
                at = i * n_side + begins[stage]
                queries[h, at : at + n] = one[(1 - i) * n : (2 - i) * n]

    def take(slot, column):
        x = jnp.concatenate([unpack(ring[slot, 0]), unpack(ring[slot, 1])], axis=0)
        values[column * span : (column + 1) * span, :width] = dot(x, rw[2]).astype(BF)
        return dot(x, rw[1]).astype(BF)

    def score(key, column, rows):
        for h in range(heads):
            for r in rows:
                scores[h, r, column * span : (column + 1) * span] = dot_t(queries[h, r], key)

    def attend(h, rows, columns, carried):
        s = scores[h, rows, columns]
        top = jnp.max(s, axis=-1, keepdims=True)
        if carried is not None:
            top = jnp.maximum(top, carried[0])
        e = jnp.exp2(s - top).astype(BF)
        out = dot(e, values[columns])
        if carried is not None:
            out = out + carried[1] * jnp.exp2(carried[0] - top)
        return top, out

    ask(0)
    ask(1)
    everything = slice(0, n_query)
    if half <= 2:
        own_key = take(0, 0)
        score(own_key, 0, train_rows)
    arrive(2)
    ask(2)
    if half <= 2:
        score(own_key, 0, test_rows)
        states = [attend(h, everything, slice(0, span), None) for h in range(heads)]

    for h in range(half - 1):
        for way in range(2):
            for p in pieces(way, h + 1):
                hops[way, h, p].wait_recv()
                hops[way, h + 1, p] = hop(way, h + 1, p)
                hops[way, h + 1, p].start()
        for way in range(2):
            for p in pieces(way, h):
                if p not in pieces(way, h + 1):
                    hops[way, h, p].wait_recv()

    if half == 2:
        for slot in (1, 2):
            score(take(slot, slot), slot, all_rows)
        states = [
            attend(h, everything, slice(span, 3 * span), states[h]) for h in range(heads)
        ]

    for way in range(2):
        for p in pieces(way, half - 1):
            hops[way, half - 1, p].wait_recv()

    if half <= 2:
        last = 2 * half - 1
        last_key = take(last, last)
        columns = slice(last * span, (last + 1) * span)
    else:
        per = scores.shape[2] // span

        def step(i, states):
            for j in range(per):
                score(take(i * per + j, j), j, all_rows)
            return [attend(h, everything, slice(0, per * span), states[h]) for h in range(heads)]

        start = [
            (
                jnp.full((n_query, 1), -1e30, F32),
                jnp.zeros((n_query, values.shape[1]), F32),
            )
            for _ in range(heads)
        ]
        states = lax.fori_loop(0, groups_n // per, step, start)

    for c in loads[4:]:
        c.wait()
    returns = []
    for i, pair in enumerate(((2, 3), (0, 1))):
        rows = slice(i * n_side, (i + 1) * n_side)
        side = [tuple(x[rows] for x in states[h]) for h in range(heads)]
        if half <= 2:
            score(last_key, last, [rows])
            side = [attend(h, rows, columns, side[h]) for h in range(heads)]
        mixed = None
        for h in range(heads):
            out = side[h][1]
            part = out[:, :width] * (1.0 / out[:, width : width + 1])
            mixed = part if h == 0 else jnp.where(lane_head == h, part, mixed)
        before = [x[(1 - i) * n : (2 - i) * n] for x, n in zip(after, sizes)]
        after_row = jnp.concatenate(before, axis=0) + dot(mixed.astype(BF), rw[3])
        hidden = gelu(dot(layer_norm(after_row).astype(BF), up[...])).astype(BF)
        done = (after_row + dot_t(hidden, down[...])).astype(BF)
        for j, k in enumerate(pair):
            block = pack(
                jnp.concatenate(
                    [
                        done[b + j * (n // 2) : b + (j + 1) * (n // 2)]
                        for b, n in zip(begins, sizes)
                    ],
                    axis=0,
                )
            )
            back_out[k] = block
            if k == 0:
                c = pltpu.make_async_copy(back_out.at[0], back_in.at[member], b_send.at[0])
                c.start()
                returns.append(c)
                continue
            c = pltpu.make_async_remote_copy(
                src_ref=back_out.at[k],
                dst_ref=back_in.at[member],
                send_sem=b_send.at[k],
                recv_sem=b_recv.at[k],
                device_id={"rows": mate(k)},
                device_id_type=MESH,
            )
            c.start()
            returns.append(c)
    for c in returns:
        c.wait()
    for c in [*hops.values(), *(c for m in moved for c in m.values())]:
        c.wait_send()


def unpack_blocks(p):
    n = p.shape[1] * 2 // 3
    count = p.shape[0]
    low = p[:, n:]
    high = jnp.concatenate([low[:, :, :64], low[:, :, 64:]], axis=1)
    first = p[:, :n].reshape(count * n, 128)
    return jnp.concatenate([first, high.reshape(count * n, 64)], axis=1)


def plane_kernel(
    rows_n,
    feats_n,
    train_hbm,
    test_hbm,
    fw_hbm,
    rw_hbm,
    up_hbm,
    down_hbm,
    back_in,
    fw,
    rw,
    up,
    down,
    train_ref,
    test_ref,
    o_train,
    o_test,
    zbox,
    abox,
    a_in,
    t_box,
    t_in,
    ring,
    early_q,
    late_q,
    early_x,
    late_x,
    fw_t,
    f_cells,
    f_x,
    t_cells,
    t_x,
    fq,
    fk,
    fv,
    fs,
    fe,
    fm,
    rw_t,
    asks,
    up_t,
    early_s,
    late_s,
    early_e,
    late_e,
    early_sum,
    late_sum,
    early_top,
    late_top,
    keys,
    vals,
    raised,
    hidden,
    back_out,
    w_sem,
    f_send,
    f_recv,
    a_send,
    a_recv,
    r_send,
    r_recv,
    b_send,
    b_recv,
    gate,
):
    width = fw.shape[-1]
    quad = t_box.shape[1]
    heads = width // HD
    groups_n = rows_n // quad
    n_train = train_ref.shape[0]
    n_test = test_ref.shape[0]
    n_half, n_quart = n_train // 2, n_test // 2
    scale = LOG2E * HD ** (-0.5)

    my_row = lax.axis_index("rows")
    my_feat = lax.axis_index("feat")
    member = lax.rem(my_row, quad)
    group = my_row // quad

    def partner(k):
        low, high = lax.rem(member, 2), member // 2
        return (1 - high if k // 2 else high) * 2 + (1 - low if k % 2 else low)

    def mate(k):
        return group * quad + partner(k)

    right_group = lax.rem(group + 1, groups_n)
    left_group = lax.rem(group + groups_n - 1, groups_n)
    right = right_group * quad + member
    left = left_group * quad + member
    other = lax.rem(my_feat + 1, feats_n)

    loads = [
        pltpu.make_async_copy(s, d, w_sem.at[i])
        for i, (s, d) in enumerate(
            [
                (train_hbm, train_ref),
                (fw_hbm, fw),
                (test_hbm, test_ref),
                (rw_hbm, rw),
                (up_hbm, up),
                (down_hbm, down),
            ]
        )
    ]
    for c in loads:
        c.start()

    barrier = pltpu.get_barrier_semaphore()
    even = lax.rem(member, 2) == 0

    def greet(**where):
        pl.semaphore_signal(barrier, inc=1, device_id=where, device_id_type=MESH)

    def tell(i):
        pl.semaphore_signal(
            gate.at[i], inc=1, device_id={"rows": mate(1)}, device_id_type=MESH
        )

    @pl.when(even)
    def _():
        greet(rows=my_row, feat=other)
        for g in (group, right_group, left_group):
            for m in range(1, quad, 2):
                for y in (my_feat, other):
                    greet(rows=g * quad + m, feat=y)
        pl.semaphore_wait(barrier, 3)
        tell(0)

    @pl.when(jnp.logical_not(even))
    def _():
        greet(rows=mate(1))
        greet(rows=mate(1), feat=other)
        greet(rows=my_row, feat=other)
        for y in (my_feat, other):
            greet(rows=mate(2), feat=y)
            for g in (right_group, left_group):
                for m in range(1, quad, 2):
                    greet(rows=g * quad + m, feat=y)
        pl.semaphore_wait(gate.at[0], 1)

    swaps = [
        pltpu.make_async_remote_copy(
            src_ref=s,
            dst_ref=d,
            send_sem=f_send.at[i],
            recv_sem=f_recv.at[i],
            device_id={"feat": other},
            device_id_type=MESH,
        )
        for i, (s, d) in enumerate(
            [
                (train_ref.at[pl.ds(pl.multiple_of(other * n_half, n_half), n_half)], o_train),
                (test_ref.at[pl.ds(pl.multiple_of(other * n_quart, n_quart), n_quart)], o_test),
            ]
        )
    ]
    for i in range(2):
        loads[2 * i].wait()
        swaps[i].start()

    tile = 16
    cell = quad * tile
    pair = 2 * cell
    lines = HD + 16
    same_row = (
        lax.broadcasted_iota(jnp.int32, (pair, heads * pair), 0) % tile
        == lax.broadcasted_iota(jnp.int32, (pair, heads * pair), 1) % tile
    )

    def fill(table, side, cells_ref, x_ref):
        n = table.shape[0] // tile
        cells = jnp.concatenate(
            [
                table[b * tile : (b + 1) * tile, f * width : (f + 1) * width].astype(F32)
                for b in range(n)
                for f in range(quad)
            ],
            axis=0,
        )
        normed = layer_norm(cells).astype(BF)
        for b in range(n):
            to = slice((2 * b + side) * cell, (2 * b + side + 1) * cell)
            cells_ref[to] = cells[b * cell : (b + 1) * cell]
            x_ref[to] = normed[b * cell : (b + 1) * cell]

    def normed_columns(x):
        centred = x - jnp.mean(x, axis=0, keepdims=True)
        spread = jnp.mean(centred * centred, axis=0, keepdims=True)
        return centred * lax.rsqrt(spread + EPS)

    def feature_attention(cells_ref, x_ref):
        n = x_ref.shape[0]
        blocks = [slice(b * pair, (b + 1) * pair) for b in range(n // pair)]
        x = x_ref[...]
        q = (dot_t(fw_t[0], x) * scale).astype(BF)
        fk[:n] = dot(x, fw[1]).astype(BF)
        v = dot_t(fw_t[2], x).astype(BF)
        for h in range(heads):
            rows = slice(h * HD, (h + 1) * HD)
            fv[h * lines : h * lines + HD, :n] = v[rows]
            for b, at in enumerate(blocks):
                fq[rows, (b * heads + h) * pair : (b * heads + h + 1) * pair] = q[rows, at]
        for b, at in enumerate(blocks):
            fs[at] = dot(fk[at], fq[:, b * heads * pair : (b + 1) * heads * pair])
        for at in blocks:
            s = jnp.where(same_row, fs[at], -1e30)
            fe[at] = jnp.exp2(s - jnp.max(s, axis=0, keepdims=True)).astype(BF)
        for at in blocks:
            for h in range(heads):
                out = dot(
                    fv[h * lines : (h + 1) * lines, at], fe[at, h * pair : (h + 1) * pair]
                )
                part = out[:HD] * (1.0 / out[HD : HD + 1])
                fm[h * HD : (h + 1) * HD, at] = part.astype(BF)
        after = cells_ref[...].T + dot(fw_t[3], fm[:, :n])
        return after, normed_columns(after)

    def sides(x):
        n = x.shape[0] // pair
        for j in range(2):
            for f in range(quad):
                at = [(2 * b + j) * cell + f * tile for b in range(n)]
                yield j, f, jnp.concatenate([x[i : i + tile] for i in at], axis=0)

    feats = (my_feat, other)

    def to_mates(box, landing, stage):
        copies = []
        for k, j in ((2, 0), (0, 1), (3, 0), (1, 1), (2, 1), (3, 1), (1, 0)):
            pltpu.make_async_remote_copy(
                src_ref=box.at[j, partner(k)],
                dst_ref=landing.at[j, k],
                send_sem=a_send.at[stage, j],
                recv_sem=a_recv.at[stage, j],
                device_id={"rows": mate(k), "feat": feats[j]},
                device_id_type=MESH,
            ).start()
        landing[0, 0] = box[0, member]
        return [
            pltpu.make_async_remote_copy(
                src_ref=part,
                dst_ref=part,
                send_sem=a_send.at[stage, j],
                recv_sem=a_recv.at[stage, j],
                device_id={"rows": mate(1)},
                device_id_type=MESH,
            )
            for j, part in enumerate((landing.at[0, pl.ds(1, quad - 1)], landing.at[1]))
        ]

    inner = jnp.logical_and(group > 0, group < groups_n - 1)

    def to_group(way, p, k):
        g = jnp.where(way == 1, left_group, right_group)
        return pltpu.make_async_remote_copy(
            src_ref=zbox.at[p, partner(k)],
            dst_ref=ring.at[way, p, k],
            send_sem=r_send.at[0],
            recv_sem=r_recv.at[way, p],
            device_id={"rows": g * quad + partner(k), "feat": feats[p]},
            device_id_type=MESH,
        )

    def whole(slot, p):
        return pltpu.make_async_remote_copy(
            src_ref=ring.at[slot, p],
            dst_ref=ring.at[slot, p],
            send_sem=r_send.at[0],
            recv_sem=r_recv.at[slot, p],
            device_id={"rows": right},
            device_id_type=MESH,
        )

    def onward(way, p):
        return pltpu.make_async_remote_copy(
            src_ref=ring.at[way, p],
            dst_ref=ring.at[2, p],
            send_sem=r_send.at[1],
            recv_sem=r_recv.at[2, p],
            device_id={"rows": left if way else right},
            device_id_type=MESH,
        )

    def relay(p):
        @pl.when(inner)
        def _():
            for way in range(2):
                whole(way, p).wait_recv()
                onward(way, p).start()

    loads[1].wait()
    fill(train_ref[pl.ds(pl.multiple_of(my_feat * n_half, n_half), n_half)], 0, f_cells, f_x)
    for i in (0, 2, 3):
        fw_t[i] = fw[i].astype(F32).T.astype(BF)
    fill(test_ref[pl.ds(pl.multiple_of(my_feat * n_quart, n_quart), n_quart)], 0, t_cells, t_x)
    fq[...] = jnp.zeros_like(fq)
    fv[...] = jnp.ones_like(fv)

    @pl.when(jnp.logical_not(even))
    def _():
        pl.semaphore_wait(barrier, 6 * quad - 1)
        tell(1)

    swaps[0].wait()
    fill(o_train[...], 1, f_cells, f_x)
    after_own, normed_own = feature_attention(f_cells, f_x)
    for j, f, x in sides(normed_own.T):
        zbox[j, f] = pack(x.astype(BF))

    @pl.when(even)
    def _():
        pl.semaphore_wait(gate.at[1], 1)

    near = jnp.where(group == groups_n - 1, 1, 0)
    at_end = group == groups_n - 1

    @pl.when(at_end)
    def _():
        for k in range(quad):
            pltpu.make_async_remote_copy(
                src_ref=zbox.at[my_feat, partner(k)],
                dst_ref=ring.at[0, my_feat, k],
                send_sem=r_send.at[0],
                recv_sem=r_recv.at[0, my_feat],
                device_id={"rows": right_group * quad + partner(k), "feat": 0},
                device_id_type=MESH,
            ).start()

    for k in range(2):
        to_group(near, 0, k).start()
    for j, f, x in sides(after_own.T):
        abox[j, f] = pack(x.astype(BF))
    moved = [to_mates(abox, a_in, 0)]
    for way in (near, 1 - near):
        for p in range(2):
            for k in range(quad):
                if way is near:
                    if p or k > 1:
                        to_group(way, p, k).start()
                    continue

                @pl.when(jnp.logical_not(jnp.logical_and(at_end, my_feat == p)))
                def _():
                    to_group(way, p, k).start()
    swaps[1].wait()
    fill(o_test[...], 1, t_cells, t_x)
    after_own, _ = feature_attention(t_cells, t_x)
    for j, f, x in sides(after_own.T):
        t_box[j, f] = pack(x.astype(BF))
    moved.append(to_mates(t_box, t_in, 1))

    loads[3].wait()
    for i in (2, 3):
        rw_t[i] = rw[i].astype(F32).T.astype(BF)
    lane_head = lax.broadcasted_iota(jnp.int32, (1, width), 1) // HD
    for h in range(heads):
        one = jnp.where(lane_head == h, rw[1], jnp.zeros_like(rw[1]))
        asks[h * width : (h + 1) * width] = (dot_t(one, rw[0]) * scale).astype(BF)
    loads[4].wait()
    up_t[...] = up[...].astype(F32).T.astype(BF)
    vals[...] = jnp.ones_like(vals)

    def arrived(landing):
        return [unpack(landing[j, k]) for k in range(quad) for j in range(2)]

    n_mid = 2 * n_train
    n_late = 2 * n_train
    n_early = n_mid + quad * n_test

    def place_queries(q, into, size, at):
        n = q.shape[1]
        for h in range(heads):
            into[:, h * size + at : h * size + at + n] = q[h * width : (h + 1) * width]

    late = (late_q, late_s, late_e, late_sum, late_top, n_late)
    early = (early_q, early_s, early_e, early_sum, early_top, n_early)

    def key_value_rows(x, i):
        keys[i] = x
        value = dot_t(rw_t[2], x).astype(BF)
        for h in range(heads):
            vals[i, h * lines : h * lines + HD] = value[h * HD : (h + 1) * HD]

    span = quad * n_train

    def attend(asked, slots, first=False):
        per_head = [
            (part, h, slice(h * part[5], (h + 1) * part[5]), slice(h * lines, (h + 1) * lines))
            for part in asked
            for h in range(heads)
        ]
        spans = [slice(n * span, (n + 1) * span) for n in range(len(slots))]
        for at, i in zip(spans, slots):
            key = keys[i]
            for (q, s, _, _, _, _), h, c, _ in per_head:
                s[at, c] = dot(key, q[:, c])
        whole_span = slice(0, len(slots) * span)
        for (_, s, e, total, tops, _), h, c, r in per_head:
            top = jnp.max(s[whole_span, c], axis=0, keepdims=True)
            if not first:
                old = tops[0:1, c]
                top = jnp.maximum(top, old)
                total[r] = total[r] * jnp.exp2(old - top)
            e[whole_span, c] = jnp.exp2(s[whole_span, c] - top).astype(BF)
            tops[0:1, c] = top
        for (_, _, e, total, _, _), h, c, r in per_head:
            out = None if first else total[r]
            for at, i in zip(spans, slots):
                part = dot(vals[i, r], e[at, c])
                out = part if out is None else out + part
            total[r] = out

    def finish(part, before):
        total = part[3]
        mix = jnp.concatenate(
            [
                total[h * lines : h * lines + HD]
                * (1.0 / total[h * lines + HD : h * lines + HD + 1])
                for h in range(heads)
            ],
            axis=0,
        ).astype(BF)
        after_row = before + dot(rw_t[3], mix)
        normed = normed_columns(after_row).astype(BF)
        n = normed.shape[1]
        raised[:, :n] = dot(up_t[...], normed)
        hidden[:, :n] = gelu(raised[:, :n]).astype(BF)
        return (after_row + dot(down[...], hidden[:, :n])).T.astype(BF)

    at_start = group == 0
    order = (jnp.where(at_start, 1, 0), jnp.where(at_start, 0, 1), 2)

    def landed(i):
        slot = order[i]

        @pl.when(jnp.logical_not(jnp.logical_and(inner, slot < 2)))
        def _():
            for p in range(2):
                whole(slot, p).wait_recv()

    def fetch(i):
        slot = order[i]
        x = jnp.concatenate([unpack_blocks(ring[slot, p]) for p in range(2)], axis=0)
        key_value_rows(x, (i + 1) % 2)

    relay(0)
    for c in moved[0]:
        c.wait_recv()
    relay(1)
    for c in moved[1]:
        c.wait_recv()
    landed(0)
    x = jnp.concatenate(arrived(a_in) + arrived(t_in), axis=0).astype(F32)
    early_x[...] = x[n_late:].T
    late_x[...] = x[:n_late].T
    for part, into, n in ((early_x, early_q, n_early), (late_x, late_q, n_late)):
        columns = normed_columns(part[...]).astype(BF)
        place_queries(dot(asks[...], columns).astype(BF), into, n, 0)
    key_value_rows(layer_norm(x[: quad * n_train]).astype(BF), 0)
    fetch(0)
    attend([late, early], (0, 1), True)
    landed(1)
    fetch(1)
    attend([late, early], (0,))
    landed(2)
    fetch(2)
    loads[5].wait()

    def give_back(k, done, tests):
        block = jnp.concatenate([done, tests[k * n_test : (k + 1) * n_test]], axis=0)
        if k == 0:
            back_in[member] = pack(block)
            return
        back_out[k] = pack(block)
        pltpu.make_async_remote_copy(
            src_ref=back_out.at[k],
            dst_ref=back_in.at[member],
            send_sem=b_send.at[0],
            recv_sem=b_recv.at[0],
            device_id={"rows": mate(k)},
            device_id_type=MESH,
        ).start()

    attend([early], (1,))
    done = finish(early, early_x[...])
    tests = done[n_mid:]
    for k in (2, 3):
        give_back(k, done[(k - 2) * n_train : (k - 1) * n_train], tests)
    attend([late], (1,))
    done = finish(late, late_x[...])
    for k in (1, 0):
        give_back(k, done[k * n_train : (k + 1) * n_train], tests)
    returned = pltpu.make_async_remote_copy(
        src_ref=back_out.at[pl.ds(1, quad - 1)],
        dst_ref=back_in.at[pl.ds(1, quad - 1)],
        send_sem=b_send.at[0],
        recv_sem=b_recv.at[0],
        device_id={"rows": mate(1)},
        device_id_type=MESH,
    )
    returned.wait()
    for c in [*moved[0], *moved[1]]:
        c.wait_send()

    def sent(i):
        pltpu.make_async_remote_copy(
            src_ref=ring.at[pl.ds(0, 2)],
            dst_ref=ring.at[pl.ds(0, 2)],
            send_sem=r_send.at[i],
            recv_sem=r_recv.at[0, 0],
            device_id={"rows": right},
            device_id_type=MESH,
        ).wait_send()

    sent(0)

    @pl.when(inner)
    def _():
        sent(1)


def place_halves(back_ref, train_out, test_out):
    quad = back_ref.shape[0]
    result = jnp.concatenate([unpack(back_ref[f]) for f in range(quad)], axis=1)
    in_order = lax.axis_index("feat") == 0
    begin = 0
    for out in (train_out, test_out):
        half = out.shape[0] // 2
        one, two = (result[begin + j * half : begin + (j + 1) * half] for j in range(2))
        out[:half] = jnp.where(in_order, one, two)
        out[half:] = jnp.where(in_order, two, one)
        begin += 2 * half


def place(back_ref, train_out, test_out):
    quad = back_ref.shape[0]
    result = jnp.concatenate([unpack(back_ref[f]) for f in range(quad)], axis=1)
    n_train = train_out.shape[0]
    train_out[...] = result[:n_train]
    test_out[...] = result[n_train:]


def solution(mesh):
    rows_n = mesh.shape["rows"]
    feats_n = mesh.shape["feat"]

    def body(train, test, fw, rw, up, down):
        width = fw.shape[-1]
        quad = train.shape[1] // width
        heads = width // HD
        n_train, n_test = train.shape[0], test.shape[0]
        cell_rows = n_train + n_test
        groups_n = rows_n // quad
        half = groups_n // 2
        span = quad * n_train
        keys = min(groups_n, 4) * span
        packed = cell_rows * width // 128
        vmem = pltpu.VMEM
        dma = pltpu.SemaphoreType.DMA
        vspec = pl.BlockSpec(memory_space=pltpu.VMEM)
        aspec = pl.BlockSpec(memory_space=pl.ANY)
        weights = (fw, rw, up, down.T)
        place_fn = place
        fits = groups_n == 4 and quad == 4 and feats_n == 2
        if fits and n_train % 32 == 0 and n_test % 32 == 0:
            body_fn, place_fn = plane_kernel, place_halves
            n_half, n_quart = n_train // 2, n_test // 2
            swapped = [vmem((n_half, quad * width), BF), vmem((n_quart, quad * width), BF)]
            both = 2 * quad
            pair = both * 16
            lines = heads * (HD + 16)
            early, late = 2 * n_train + quad * n_test, 2 * n_train
            work = [
                vmem((width, heads * early), BF),
                vmem((width, heads * late), BF),
                vmem((width, early), F32),
                vmem((width, late), F32),
                vmem(fw.shape, BF),
                vmem((both * n_half, width), F32),
                vmem((both * n_half, width), BF),
                vmem((both * n_quart, width), F32),
                vmem((both * n_quart, width), BF),
                vmem((width, heads * both * n_half), BF),
                vmem((both * n_half, width), BF),
                vmem((lines, both * n_half), BF),
                vmem((both * n_half, heads * pair), F32),
                vmem((both * n_half, heads * pair), BF),
                vmem((width, both * n_half), BF),
                vmem(rw.shape, BF),
                vmem((heads * width, width), BF),
                vmem(up.shape[::-1], BF),
                vmem((2 * span, heads * early), F32),
                vmem((2 * span, heads * late), F32),
                vmem((2 * span, heads * early), BF),
                vmem((2 * span, heads * late), BF),
                vmem((heads * (HD + 16), early), F32),
                vmem((heads * (HD + 16), late), F32),
                vmem((8, heads * early), F32),
                vmem((8, heads * late), F32),
                vmem((2, span, width), BF),
                vmem((2, heads * (HD + 16), span), BF),
                vmem((up.shape[1], early), F32),
                vmem((up.shape[1], early), BF),
            ]
            boxes = [
                vmem((2, quad, n_train * width // 256, 128), BF),
                vmem((2, quad, n_train * width // 256, 128), BF),
                vmem((2, quad, n_train * width // 256, 128), BF),
                vmem((2, quad, n_test * width // 256, 128), BF),
                vmem((2, quad, n_test * width // 256, 128), BF),
                vmem((3, 2, quad, n_train * width // 256, 128), BF),
            ]
            flags = [
                dma((2,)),
                dma((2,)),
                dma((2, 2)),
                dma((2, 2)),
                dma((2,)),
                dma((3, 2)),
                dma((1,)),
                dma((1,)),
                pltpu.SemaphoreType.REGULAR((2,)),
            ]
        else:
            body_fn = kernel
            swapped = [vmem(train.shape, BF), vmem(test.shape, BF)]
            work = [
                vmem((heads, quad * cell_rows, keys), F32),
                vmem((keys, 256), BF),
                vmem((heads, quad * cell_rows, width), BF),
            ]
            boxes = [
                vmem((2, quad, n_train * width // 256, 128), BF),
                vmem((2, quad, n_train * width // 256, 128), BF),
                vmem((quad, n_test * width // 128, 128), BF),
                vmem((quad, n_test * width // 128, 128), BF),
                vmem((groups_n, 2, span * width // 256, 128), BF),
            ]
            flags = [
                dma((3,)),
                dma((3,)),
                dma((3, quad)),
                dma((3, quad)),
                dma((2, half, 2)),
                dma((2, half, 2)),
                dma((quad,)),
                dma((quad,)),
            ]
        back = pl.pallas_call(
            functools.partial(body_fn, rows_n, feats_n),
            out_shape=pltpu.VMEM((quad, packed, 128), BF),
            in_specs=[aspec, aspec, aspec, aspec, aspec, aspec],
            out_specs=vspec,
            scratch_shapes=[
                *(vmem(w.shape, BF) for w in weights),
                vmem(train.shape, BF),
                vmem(test.shape, BF),
                *swapped,
                *boxes,
                *work,
                vmem((quad, packed, 128), BF),
                dma((6,)),
                *flags,
            ],
            compiler_params=pltpu.CompilerParams(
                collective_id=0, has_side_effects=True, vmem_limit_bytes=60 * 1024 * 1024
            ),
            name="layer",
        )(train, test, *weights)
        return pl.pallas_call(
            place_fn,
            out_shape=(
                jax.ShapeDtypeStruct(train.shape, BF),
                jax.ShapeDtypeStruct(test.shape, BF),
            ),
            in_specs=[vspec],
            out_specs=(vspec, vspec),
            name="place",
        )(pltpu.with_memory_space_constraint(back, pltpu.VMEM))

    return jax.shard_map(
        body,
        mesh=mesh,
        in_specs=(P("rows", "feat"), P("rows", "feat"), P(), P(), P(), P()),
        out_specs=(P("rows", "feat"), P("rows", "feat")),
        check_vma=False,
    )
```

```python
import functools

import jax
import jax.numpy as jnp
from jax import lax
from jax.experimental import pallas as pl
from jax.experimental.pallas import tpu as pltpu
from jax.sharding import PartitionSpec as P

HD = 32
EPS = 1e-05
LOG2E = 1.4426950408889634
MESH = pl.DeviceIdType.MESH
BF = jnp.bfloat16
F32 = jnp.float32


def layer_norm(x):
    centred = x - jnp.mean(x, axis=-1, keepdims=True)
    spread = jnp.mean(centred * centred, axis=-1, keepdims=True)
    return centred * lax.rsqrt(spread + EPS)


def dot(a, b):
    return jnp.dot(a, b, preferred_element_type=F32)


def dot_t(a, b):
    return lax.dot_general(a, b, (((1,), (1,)), ((), ())), preferred_element_type=F32)


def pack(x):
    n = x.shape[0]
    low = jnp.concatenate([x[: n // 2, 128:], x[n // 2 :, 128:]], axis=1)
    return jnp.concatenate([x[:, :128], low], axis=0)


def unpack(p):
    n = p.shape[0] * 2 // 3
    low = p[n:]
    high = jnp.concatenate([low[:, :64], low[:, 64:]], axis=0)
    return jnp.concatenate([p[:n], high], axis=1)


def gelu(x):
    return 0.5 * x * (1.0 + lax.erf(x * (0.5**0.5)))


def kernel(
    rows_n,
    feats_n,
    train_hbm,
    test_hbm,
    fw_hbm,
    rw_hbm,
    up_hbm,
    down_hbm,
    back_in,
    fw,
    rw,
    up,
    down,
    train_ref,
    test_ref,
    o_train,
    o_test,
    outbox,
    inbox,
    t_outbox,
    t_inbox,
    ring,
    scores,
    values,
    queries,
    back_out,
    w_sem,
    f_send,
    f_recv,
    q_send,
    q_recv,
    r_send,
    r_recv,
    b_send,
    b_recv,
):
    width = fw.shape[-1]
    quad = t_outbox.shape[0]
    heads = width // HD
    groups_n = rows_n // quad
    half = groups_n // 2
    n_train = train_ref.shape[0]
    n_test = test_ref.shape[0]
    n_half = n_train // 2
    scale = LOG2E * HD ** (-0.5)

    my_row = lax.axis_index("rows")
    my_feat = lax.axis_index("feat")
    member = lax.rem(my_row, quad)
    group = my_row // quad

    def partner(k):
        low, high = lax.rem(member, 2), member // 2
        return (1 - high if k // 2 else high) * 2 + (1 - low if k % 2 else low)

    def mate(k):
        return group * quad + partner(k)

    right = lax.rem(group + 1, groups_n) * quad + member
    left = lax.rem(group + groups_n - 1, groups_n) * quad + member
    other = lax.rem(my_feat + 1, feats_n)

    loads = [
        pltpu.make_async_copy(s, d, w_sem.at[i])
        for i, (s, d) in enumerate(
            [
                (train_hbm, train_ref),
                (fw_hbm, fw),
                (test_hbm, test_ref),
                (rw_hbm, rw),
                (up_hbm, up),
                (down_hbm, down),
            ]
        )
    ]
    for c in loads:
        c.start()

    barrier = pltpu.get_barrier_semaphore()
    pl.semaphore_signal(barrier, inc=1, device_id={"feat": other}, device_id_type=MESH)
    for k in range(1, quad):
        pl.semaphore_signal(barrier, inc=1, device_id={"rows": mate(k)}, device_id_type=MESH)
    for d in (right, left):
        pl.semaphore_signal(barrier, inc=1, device_id={"rows": d}, device_id_type=MESH)
    pl.semaphore_wait(barrier, quad + 2)

    halves = [pl.ds(p * n_half, n_half) for p in range(2)]
    swaps = [
        pltpu.make_async_remote_copy(
            src_ref=s,
            dst_ref=d,
            send_sem=f_send.at[i],
            recv_sem=f_recv.at[i],
            device_id={"feat": other},
            device_id_type=MESH,
        )
        for i, (s, d) in enumerate(
            [(train_hbm.at[r], o_train.at[r]) for r in halves] + [(test_hbm, o_test)]
        )
    ]
    for c in swaps:
        c.start()

    def feature_rows(table):
        return jnp.concatenate(
            [table[:, f * width : (f + 1) * width].astype(F32) for f in range(quad)], axis=0
        )

    def split(x):
        n = x.shape[0] // quad
        return [x[f * n : (f + 1) * n] for f in range(quad)]

    def key_value(normed):
        return split(dot(normed, fw[1]).astype(BF)), split(dot(normed, fw[2]).astype(BF))

    same = (
        lax.broadcasted_iota(jnp.int32, (width, width), 0) // HD
        == lax.broadcasted_iota(jnp.int32, (width, width), 1) // HD
    )
    spread = jnp.where(same, 1.0, 0.0).astype(BF)

    def own_side(table):
        cells = feature_rows(table)
        normed = layer_norm(cells).astype(BF)
        q = split((dot(normed, fw[0]) * scale).astype(BF))
        ks, vs = key_value(normed)
        return cells, q, ks, vs

    def feature_attention(own, table):
        cells, q, ks, vs = own
        n = table.shape[0]
        more_k, more_v = key_value(layer_norm(feature_rows(table)).astype(BF))
        ks, vs = ks + more_k, vs + more_v
        mixes = []
        for f in range(quad):
            prod = jnp.concatenate([q[f] * k for k in ks], axis=0)
            s = dot(prod, spread)
            s = [s[g * n : (g + 1) * n] for g in range(len(ks))]
            top = functools.reduce(jnp.maximum, s)
            total = None
            mix = None
            for g in range(len(ks)):
                e = jnp.exp2(s[g] - top)
                t = e * vs[g].astype(F32)
                total = e if total is None else total + e
                mix = t if mix is None else mix + t
            mixes.append((mix / total).astype(BF))
        feat_out = dot(jnp.concatenate(mixes, axis=0), fw[3])
        return split((cells + feat_out).astype(BF))

    def to_mates(box, landing, stage):
        copies = {}
        for k in (2, 3, 1):
            copies[k] = pltpu.make_async_remote_copy(
                src_ref=box.at[partner(k)],
                dst_ref=landing.at[k],
                send_sem=q_send.at[stage, k],
                recv_sem=q_recv.at[stage, k],
                device_id={"rows": mate(k)},
                device_id_type=MESH,
            )
            copies[k].start()
        landing[0] = box[member]
        return copies

    loads[0].wait()
    loads[1].wait()
    own = [own_side(train_ref[p * n_half : (p + 1) * n_half]) for p in range(2)]
    moved = []
    boxes = [(outbox.at[p], inbox.at[p]) for p in range(2)] + [(t_outbox, t_inbox)]
    for p in range(2):
        swaps[p].wait()
        for f, x in enumerate(feature_attention(own[p], o_train[p * n_half : (p + 1) * n_half])):
            outbox[p, f] = pack(x)
        moved.append(to_mates(*boxes[p], p))
    loads[2].wait()
    own_test = own_side(test_ref[...])
    swaps[2].wait()
    for f, x in enumerate(feature_attention(own_test, o_test[...])):
        t_outbox[f] = pack(x)
    moved.append(to_mates(*boxes[2], 2))

    def hop(way, h, p):
        last = h == half - 1
        src = 0 if h == 0 else 2 * h - 1 + way
        dst = 2 * half - 1 if last else 1 + 2 * h + way
        return pltpu.make_async_remote_copy(
            src_ref=ring.at[src, p],
            dst_ref=ring.at[dst, p],
            send_sem=r_send.at[way, h, p],
            recv_sem=r_recv.at[way, h, p],
            device_id={"rows": left if way else right},
            device_id_type=MESH,
        )

    def pieces(way, h):
        return (way,) if h == half - 1 else (way, 1 - way)

    hops = {}
    after = []
    normed = []

    def arrive(stage):
        for k in range(1, quad):
            moved[stage][k].wait_recv()
        landing = boxes[stage][1]
        after.append(
            jnp.concatenate([unpack(landing[k]) for k in range(quad)], axis=0).astype(F32)
        )
        normed.append(layer_norm(after[stage]).astype(BF))

    for p in range(2):
        arrive(p)
        ring[0, p] = pack(normed[p])
        for way in (p, 1 - p):
            if p in pieces(way, 0):
                hops[way, 0, p] = hop(way, 0, p)
                hops[way, 0, p].start()

    loads[3].wait()
    lane_head = lax.broadcasted_iota(jnp.int32, (1, width), 1) // HD
    n_query = quad * (n_train + n_test)
    n_side = n_query // 2
    sizes = [2 * n_half, 2 * n_half, 2 * n_test]
    begins = [0, 2 * n_half, 4 * n_half]
    all_rows = [slice(0, n_query)]
    train_rows = [slice(i * n_side, i * n_side + begins[2]) for i in range(2)]
    test_rows = [slice(i * n_side + begins[2], (i + 1) * n_side) for i in range(2)]
    span = quad * n_train
    values[:, width:] = jnp.ones_like(values[:, width:])

    def ask(stage):
        q_all = (dot(normed[stage], rw[0]) * scale).astype(BF)
        n = sizes[stage]
        for h in range(heads):
            one = jnp.where(lane_head == h, q_all, jnp.zeros_like(q_all))
            for i in range(2):
                at = i * n_side + begins[stage]
                queries[h, at : at + n] = one[(1 - i) * n : (2 - i) * n]

    def take(slot, column):
        x = jnp.concatenate([unpack(ring[slot, 0]), unpack(ring[slot, 1])], axis=0)
        values[column * span : (column + 1) * span, :width] = dot(x, rw[2]).astype(BF)
        return dot(x, rw[1]).astype(BF)

    def score(key, column, rows):
        for h in range(heads):
            for r in rows:
                scores[h, r, column * span : (column + 1) * span] = dot_t(queries[h, r], key)

    def attend(h, rows, columns, carried):
        s = scores[h, rows, columns]
        top = jnp.max(s, axis=-1, keepdims=True)
        if carried is not None:
            top = jnp.maximum(top, carried[0])
        e = jnp.exp2(s - top).astype(BF)
        out = dot(e, values[columns])
        if carried is not None:
            out = out + carried[1] * jnp.exp2(carried[0] - top)
        return top, out

    ask(0)
    ask(1)
    everything = slice(0, n_query)
    if half <= 2:
        own_key = take(0, 0)
        score(own_key, 0, train_rows)
    arrive(2)
    ask(2)
    if half <= 2:
        score(own_key, 0, test_rows)
        states = [attend(h, everything, slice(0, span), None) for h in range(heads)]

    for h in range(half - 1):
        for way in range(2):
            for p in pieces(way, h + 1):
                hops[way, h, p].wait_recv()
                hops[way, h + 1, p] = hop(way, h + 1, p)
                hops[way, h + 1, p].start()
        for way in range(2):
            for p in pieces(way, h):
                if p not in pieces(way, h + 1):
                    hops[way, h, p].wait_recv()

    if half == 2:
        for slot in (1, 2):
            score(take(slot, slot), slot, all_rows)
        states = [
            attend(h, everything, slice(span, 3 * span), states[h]) for h in range(heads)
        ]

    for way in range(2):
        for p in pieces(way, half - 1):
            hops[way, half - 1, p].wait_recv()

    if half <= 2:
        last = 2 * half - 1
        last_key = take(last, last)
        columns = slice(last * span, (last + 1) * span)
    else:
        per = scores.shape[2] // span

        def step(i, states):
            for j in range(per):
                score(take(i * per + j, j), j, all_rows)
            return [attend(h, everything, slice(0, per * span), states[h]) for h in range(heads)]

        start = [
            (
                jnp.full((n_query, 1), -1e30, F32),
                jnp.zeros((n_query, values.shape[1]), F32),
            )
            for _ in range(heads)
        ]
        states = lax.fori_loop(0, groups_n // per, step, start)

    for c in loads[4:]:
        c.wait()
    returns = []
    for i, pair in enumerate(((2, 3), (0, 1))):
        rows = slice(i * n_side, (i + 1) * n_side)
        side = [tuple(x[rows] for x in states[h]) for h in range(heads)]
        if half <= 2:
            score(last_key, last, [rows])
            side = [attend(h, rows, columns, side[h]) for h in range(heads)]
        mixed = None
        for h in range(heads):
            out = side[h][1]
            part = out[:, :width] * (1.0 / out[:, width : width + 1])
            mixed = part if h == 0 else jnp.where(lane_head == h, part, mixed)
        before = [x[(1 - i) * n : (2 - i) * n] for x, n in zip(after, sizes)]
        after_row = jnp.concatenate(before, axis=0) + dot(mixed.astype(BF), rw[3])
        hidden = gelu(dot(layer_norm(after_row).astype(BF), up[...])).astype(BF)
        done = (after_row + dot_t(hidden, down[...])).astype(BF)
        for j, k in enumerate(pair):
            block = pack(
                jnp.concatenate(
                    [
                        done[b + j * (n // 2) : b + (j + 1) * (n // 2)]
                        for b, n in zip(begins, sizes)
                    ],
                    axis=0,
                )
            )
            back_out[k] = block
            if k == 0:
                c = pltpu.make_async_copy(back_out.at[0], back_in.at[member], b_send.at[0])
                c.start()
                returns.append(c)
                continue
            c = pltpu.make_async_remote_copy(
                src_ref=back_out.at[k],
                dst_ref=back_in.at[member],
                send_sem=b_send.at[k],
                recv_sem=b_recv.at[k],
                device_id={"rows": mate(k)},
                device_id_type=MESH,
            )
            c.start()
            returns.append(c)
    for c in returns:
        c.wait()
    for c in [*hops.values(), *(c for m in moved for c in m.values())]:
        c.wait_send()


def unpack_blocks(p):
    n = p.shape[1] * 2 // 3
    count = p.shape[0]
    low = p[:, n:]
    high = jnp.concatenate([low[:, :, :64], low[:, :, 64:]], axis=1)
    first = p[:, :n].reshape(count * n, 128)
    return jnp.concatenate([first, high.reshape(count * n, 64)], axis=1)


def plane_kernel(
    rows_n,
    feats_n,
    train_hbm,
    test_hbm,
    fw_hbm,
    rw_hbm,
    up_hbm,
    down_hbm,
    back_in,
    fw,
    rw,
    up,
    down,
    train_ref,
    test_ref,
    o_train,
    o_test,
    zbox,
    abox,
    a_in,
    t_box,
    t_in,
    ring,
    early_q,
    late_q,
    early_x,
    late_x,
    fw_t,
    f_cells,
    f_x,
    t_cells,
    t_x,
    fq,
    fk,
    fv,
    fs,
    fe,
    fm,
    rw_t,
    asks,
    up_t,
    early_s,
    late_s,
    early_e,
    late_e,
    early_sum,
    late_sum,
    early_top,
    late_top,
    keys,
    vals,
    raised,
    hidden,
    back_out,
    w_sem,
    f_send,
    f_recv,
    a_send,
    a_recv,
    r_send,
    r_recv,
    b_send,
    b_recv,
    gate,
):
    width = fw.shape[-1]
    quad = t_box.shape[1]
    heads = width // HD
    groups_n = rows_n // quad
    n_train = train_ref.shape[0]
    n_test = test_ref.shape[0]
    n_half, n_quart = n_train // 2, n_test // 2
    scale = LOG2E * HD ** (-0.5)

    my_row = lax.axis_index("rows")
    my_feat = lax.axis_index("feat")
    member = lax.rem(my_row, quad)
    group = my_row // quad

    def partner(k):
        low, high = lax.rem(member, 2), member // 2
        return (1 - high if k // 2 else high) * 2 + (1 - low if k % 2 else low)

    def mate(k):
        return group * quad + partner(k)

    right_group = lax.rem(group + 1, groups_n)
    left_group = lax.rem(group + groups_n - 1, groups_n)
    right = right_group * quad + member
    left = left_group * quad + member
    other = lax.rem(my_feat + 1, feats_n)

    loads = [
        pltpu.make_async_copy(s, d, w_sem.at[i])
        for i, (s, d) in enumerate(
            [
                (train_hbm, train_ref),
                (fw_hbm, fw),
                (test_hbm, test_ref),
                (rw_hbm, rw),
                (up_hbm, up),
                (down_hbm, down),
            ]
        )
    ]
    for c in loads:
        c.start()

    barrier = pltpu.get_barrier_semaphore()
    even = lax.rem(member, 2) == 0

    def greet(**where):
        pl.semaphore_signal(barrier, inc=1, device_id=where, device_id_type=MESH)

    def tell(i):
        pl.semaphore_signal(
            gate.at[i], inc=1, device_id={"rows": mate(1)}, device_id_type=MESH
        )

    @pl.when(even)
    def _():
        greet(rows=my_row, feat=other)
        for g in (group, right_group, left_group):
            for m in range(1, quad, 2):
                for y in (my_feat, other):
                    greet(rows=g * quad + m, feat=y)
        pl.semaphore_wait(barrier, 3)
        tell(0)

    @pl.when(jnp.logical_not(even))
    def _():
        greet(rows=mate(1))
        greet(rows=mate(1), feat=other)
        greet(rows=my_row, feat=other)
        for y in (my_feat, other):
            greet(rows=mate(2), feat=y)
            for g in (right_group, left_group):
                for m in range(1, quad, 2):
                    greet(rows=g * quad + m, feat=y)
        pl.semaphore_wait(gate.at[0], 1)

    swaps = [
        pltpu.make_async_remote_copy(
            src_ref=s,
            dst_ref=d,
            send_sem=f_send.at[i],
            recv_sem=f_recv.at[i],
            device_id={"feat": other},
            device_id_type=MESH,
        )
        for i, (s, d) in enumerate(
            [
                (train_ref.at[pl.ds(pl.multiple_of(other * n_half, n_half), n_half)], o_train),
                (test_ref.at[pl.ds(pl.multiple_of(other * n_quart, n_quart), n_quart)], o_test),
            ]
        )
    ]
    for i in range(2):
        loads[2 * i].wait()
        swaps[i].start()

    tile = 16
    cell = quad * tile
    pair = 2 * cell
    lines = HD + 16
    same_row = (
        lax.broadcasted_iota(jnp.int32, (pair, heads * pair), 0) % tile
        == lax.broadcasted_iota(jnp.int32, (pair, heads * pair), 1) % tile
    )

    def fill(table, side, cells_ref, x_ref):
        n = table.shape[0] // tile
        cells = jnp.concatenate(
            [
                table[b * tile : (b + 1) * tile, f * width : (f + 1) * width].astype(F32)
                for b in range(n)
                for f in range(quad)
            ],
            axis=0,
        )
        normed = layer_norm(cells).astype(BF)
        for b in range(n):
            to = slice((2 * b + side) * cell, (2 * b + side + 1) * cell)
            cells_ref[to] = cells[b * cell : (b + 1) * cell].astype(BF)
            x_ref[to] = normed[b * cell : (b + 1) * cell]

    def normed_columns(x):
        centred = x - jnp.mean(x, axis=0, keepdims=True)
        spread = jnp.mean(centred * centred, axis=0, keepdims=True)
        return centred * lax.rsqrt(spread + EPS)

    def feature_attention(cells_ref, x_ref):
        n = x_ref.shape[0]
        blocks = [slice(b * pair, (b + 1) * pair) for b in range(n // pair)]
        x = x_ref[...]
        q = (dot_t(fw_t[0], x) * scale).astype(BF)
        fk[:n] = dot(x, fw[1]).astype(BF)
        v = dot_t(fw_t[2], x).astype(BF)
        for h in range(heads):
            rows = slice(h * HD, (h + 1) * HD)
            fv[h * lines : h * lines + HD, :n] = v[rows]
            for b, at in enumerate(blocks):
                fq[rows, (b * heads + h) * pair : (b * heads + h + 1) * pair] = q[rows, at]
        for b, at in enumerate(blocks):
            fs[at] = dot(fk[at], fq[:, b * heads * pair : (b + 1) * heads * pair])
        for at in blocks:
            s = jnp.where(same_row, fs[at], -1e30)
            fe[at] = jnp.exp2(s - jnp.max(s, axis=0, keepdims=True)).astype(BF)
        for at in blocks:
            for h in range(heads):
                out = dot(
                    fv[h * lines : (h + 1) * lines, at], fe[at, h * pair : (h + 1) * pair]
                )
                part = out[:HD] * (1.0 / out[HD : HD + 1])
                fm[h * HD : (h + 1) * HD, at] = part.astype(BF)
        after = cells_ref[...].T.astype(F32) + dot(fw_t[3], fm[:, :n])
        return after, normed_columns(after)

    def sides(x):
        n = x.shape[0] // pair
        for j in range(2):
            for f in range(quad):
                at = [(2 * b + j) * cell + f * tile for b in range(n)]
                yield j, f, jnp.concatenate([x[i : i + tile] for i in at], axis=0)

    feats = (my_feat, other)

    def to_mates(box, landing, stage):
        copies = []
        for k, j in ((2, 0), (0, 1), (3, 0), (1, 1), (2, 1), (3, 1), (1, 0)):
            pltpu.make_async_remote_copy(
                src_ref=box.at[j, partner(k)],
                dst_ref=landing.at[j, k],
                send_sem=a_send.at[stage, j],
                recv_sem=a_recv.at[stage, j],
                device_id={"rows": mate(k), "feat": feats[j]},
                device_id_type=MESH,
            ).start()
        landing[0, 0] = box[0, member]
        return [
            pltpu.make_async_remote_copy(
                src_ref=part,
                dst_ref=part,
                send_sem=a_send.at[stage, j],
                recv_sem=a_recv.at[stage, j],
                device_id={"rows": mate(1)},
                device_id_type=MESH,
            )
            for j, part in enumerate((landing.at[0, pl.ds(1, quad - 1)], landing.at[1]))
        ]

    inner = jnp.logical_and(group > 0, group < groups_n - 1)

    def to_group(way, p, k):
        g = jnp.where(way == 1, left_group, right_group)
        return pltpu.make_async_remote_copy(
            src_ref=zbox.at[p, partner(k)],
            dst_ref=ring.at[way, p, k],
            send_sem=r_send.at[0],
            recv_sem=r_recv.at[way, p],
            device_id={"rows": g * quad + partner(k), "feat": feats[p]},
            device_id_type=MESH,
        )

    def whole(slot, p):
        return pltpu.make_async_remote_copy(
            src_ref=ring.at[slot, p],
            dst_ref=ring.at[slot, p],
            send_sem=r_send.at[0],
            recv_sem=r_recv.at[slot, p],
            device_id={"rows": right},
            device_id_type=MESH,
        )

    def onward(way, p):
        return pltpu.make_async_remote_copy(
            src_ref=ring.at[way, p],
            dst_ref=ring.at[2, p],
            send_sem=r_send.at[1],
            recv_sem=r_recv.at[2, p],
            device_id={"rows": left if way else right},
            device_id_type=MESH,
        )

    def relay(p):
        @pl.when(inner)
        def _():
            for way in (1, 0):
                whole(way, p).wait_recv()
                onward(way, p).start()

    loads[1].wait()
    fill(train_ref[pl.ds(pl.multiple_of(my_feat * n_half, n_half), n_half)], 0, f_cells, f_x)
    for i in (0, 2, 3):
        fw_t[i] = fw[i].astype(F32).T.astype(BF)
    fill(test_ref[pl.ds(pl.multiple_of(my_feat * n_quart, n_quart), n_quart)], 0, t_cells, t_x)
    fq[...] = jnp.zeros_like(fq)
    fv[...] = jnp.ones_like(fv)

    @pl.when(jnp.logical_not(even))
    def _():
        pl.semaphore_wait(barrier, 6 * quad - 1)
        tell(1)

    swaps[0].wait()
    fill(o_train[...], 1, f_cells, f_x)
    after_own, normed_own = feature_attention(f_cells, f_x)
    for j, f, x in sides(normed_own.astype(BF).T):
        zbox[j, f] = pack(x)

    @pl.when(even)
    def _():
        pl.semaphore_wait(gate.at[1], 1)

    near = jnp.where(group >= 1, 1, 0)
    at_end = group == groups_n - 1

    @pl.when(at_end)
    def _():
        for k in range(quad):
            pltpu.make_async_remote_copy(
                src_ref=zbox.at[my_feat, partner(k)],
                dst_ref=ring.at[0, my_feat, k],
                send_sem=r_send.at[0],
                recv_sem=r_recv.at[0, my_feat],
                device_id={"rows": right_group * quad + partner(k), "feat": 0},
                device_id_type=MESH,
            ).start()

    for k in range(2):
        to_group(near, 0, k).start()
    for j, f, x in sides(after_own.astype(BF).T):
        abox[j, f] = pack(x)
    moved = [to_mates(abox, a_in, 0)]
    for way in (near, 1 - near):
        for p in range(2):
            for k in range(quad):
                if way is near:
                    if p or k > 1:
                        to_group(way, p, k).start()
                    continue

                @pl.when(jnp.logical_not(jnp.logical_and(at_end, my_feat == p)))
                def _():
                    to_group(way, p, k).start()
    swaps[1].wait()
    fill(o_test[...], 1, t_cells, t_x)
    after_own, _ = feature_attention(t_cells, t_x)
    for j, f, x in sides(after_own.astype(BF).T):
        t_box[j, f] = pack(x)
    moved.append(to_mates(t_box, t_in, 1))

    loads[3].wait()
    for i in (2, 3):
        rw_t[i] = rw[i].astype(F32).T.astype(BF)
    lane_head = lax.broadcasted_iota(jnp.int32, (1, width), 1) // HD
    for h in range(heads):
        one = jnp.where(lane_head == h, rw[1], jnp.zeros_like(rw[1]))
        asks[h * width : (h + 1) * width] = (dot_t(one, rw[0]) * scale).astype(BF)
    loads[4].wait()
    up_t[...] = up[...].astype(F32).T.astype(BF)
    vals[...] = jnp.ones_like(vals)

    def arrived(landing):
        return [unpack(landing[j, k]) for k in range(quad) for j in range(2)]

    n_mid = 2 * n_train
    n_late = 2 * n_train
    n_early = n_mid + quad * n_test

    def place_queries(q, into, size, at):
        n = q.shape[1]
        for h in range(heads):
            into[:, h * size + at : h * size + at + n] = q[h * width : (h + 1) * width]

    late = (late_q, late_s, late_e, late_sum, late_top, n_late)
    early = (early_q, early_s, early_e, early_sum, early_top, n_early)

    def key_value_rows(x, i):
        keys[i] = x
        value = dot_t(rw_t[2], x).astype(BF)
        for h in range(heads):
            vals[i, h * lines : h * lines + HD] = value[h * HD : (h + 1) * HD]

    span = quad * n_train

    def attend(asked, slots, first=False):
        per_head = [
            (part, h, slice(h * part[5], (h + 1) * part[5]), slice(h * lines, (h + 1) * lines))
            for part in asked
            for h in range(heads)
        ]
        spans = [slice(n * span, (n + 1) * span) for n in range(len(slots))]
        for at, i in zip(spans, slots):
            key = keys[i]
            for (q, s, _, _, _, _), h, c, _ in per_head:
                s[at, c] = dot(key, q[:, c])
        whole_span = slice(0, len(slots) * span)
        for (_, s, e, total, tops, _), h, c, r in per_head:
            top = jnp.max(s[whole_span, c], axis=0, keepdims=True)
            if not first:
                old = tops[0:1, c]
                top = jnp.maximum(top, old)
                total[r] = total[r] * jnp.exp2(old - top)
            e[whole_span, c] = jnp.exp2(s[whole_span, c] - top).astype(BF)
            tops[0:1, c] = top
        for (_, _, e, total, _, _), h, c, r in per_head:
            out = None if first else total[r]
            for at, i in zip(spans, slots):
                part = dot(vals[i, r], e[at, c])
                out = part if out is None else out + part
            total[r] = out

    def finish(part, before):
        total = part[3]
        mix = jnp.concatenate(
            [
                total[h * lines : h * lines + HD]
                * (1.0 / total[h * lines + HD : h * lines + HD + 1])
                for h in range(heads)
            ],
            axis=0,
        ).astype(BF)
        after_row = before + dot(rw_t[3], mix)
        normed = normed_columns(after_row).astype(BF)
        n = normed.shape[1]
        step = width
        for i in range(up_t.shape[0] // step):
            at = slice(i * step, (i + 1) * step)
            raised[at, :n] = dot(up_t[at], normed)
            hidden[at, :n] = gelu(raised[at, :n]).astype(BF)
        return (after_row + dot(down[...], hidden[:, :n])).astype(BF).T

    at_start = group == 0
    order = (jnp.where(at_start, 1, 0), jnp.where(at_start, 0, 1), 2)

    def landed(i):
        slot = order[i]

        @pl.when(jnp.logical_not(jnp.logical_and(inner, slot < 2)))
        def _():
            for p in range(2):
                whole(slot, p).wait_recv()

    def fetch(i):
        slot = order[i]
        x = jnp.concatenate([unpack_blocks(ring[slot, p]) for p in range(2)], axis=0)
        key_value_rows(x, (i + 1) % 2)

    relay(0)
    relay(1)
    for c in [*moved[0], *moved[1]]:
        c.wait_recv()
    landed(0)
    x = jnp.concatenate(arrived(a_in) + arrived(t_in), axis=0)
    early_x[...] = x[n_late:].T.astype(F32)
    late_x[...] = x[:n_late].T.astype(F32)
    for part, into, n in ((early_x, early_q, n_early), (late_x, late_q, n_late)):
        columns = normed_columns(part[...]).astype(BF)
        place_queries(dot(asks[...], columns).astype(BF), into, n, 0)
    key_value_rows(layer_norm(x[: quad * n_train].astype(F32)).astype(BF), 0)
    fetch(0)
    attend([late, early], (0, 1), True)
    landed(1)
    fetch(1)
    attend([late, early], (0,))
    landed(2)
    fetch(2)
    loads[5].wait()

    def give_back(k, done, tests):
        block = jnp.concatenate([done, tests[k * n_test : (k + 1) * n_test]], axis=0)
        if k == 0:
            back_in[member] = pack(block)
            return
        back_out[k] = pack(block)
        pltpu.make_async_remote_copy(
            src_ref=back_out.at[k],
            dst_ref=back_in.at[member],
            send_sem=b_send.at[0],
            recv_sem=b_recv.at[0],
            device_id={"rows": mate(k)},
            device_id_type=MESH,
        ).start()

    attend([early], (1,))
    done = finish(early, early_x[...])
    tests = done[n_mid:]
    for k in (2, 3):
        give_back(k, done[(k - 2) * n_train : (k - 1) * n_train], tests)
    attend([late], (1,))
    done = finish(late, late_x[...])
    for k in (1, 0):
        give_back(k, done[k * n_train : (k + 1) * n_train], tests)
    returned = pltpu.make_async_remote_copy(
        src_ref=back_out.at[pl.ds(1, quad - 1)],
        dst_ref=back_in.at[pl.ds(1, quad - 1)],
        send_sem=b_send.at[0],
        recv_sem=b_recv.at[0],
        device_id={"rows": mate(1)},
        device_id_type=MESH,
    )
    returned.wait()
    for c in [*moved[0], *moved[1]]:
        c.wait_send()

    def sent(i):
        pltpu.make_async_remote_copy(
            src_ref=ring.at[pl.ds(0, 2)],
            dst_ref=ring.at[pl.ds(0, 2)],
            send_sem=r_send.at[i],
            recv_sem=r_recv.at[0, 0],
            device_id={"rows": right},
            device_id_type=MESH,
        ).wait_send()

    sent(0)

    @pl.when(inner)
    def _():
        sent(1)


def place_halves(back_ref, train_out, test_out):
    quad = back_ref.shape[0]
    result = jnp.concatenate([unpack(back_ref[f]) for f in range(quad)], axis=1)
    mine = lax.axis_index("feat")
    begin = 0
    for out in (train_out, test_out):
        half = out.shape[0] // 2
        for j, place_of in enumerate((mine, 1 - mine)):
            to = pl.ds(pl.multiple_of(place_of * half, half), half)
            out[to] = result[begin + j * half : begin + (j + 1) * half]
        begin += 2 * half


def place(back_ref, train_out, test_out):
    quad = back_ref.shape[0]
    result = jnp.concatenate([unpack(back_ref[f]) for f in range(quad)], axis=1)
    n_train = train_out.shape[0]
    train_out[...] = result[:n_train]
    test_out[...] = result[n_train:]


def solution(mesh):
    rows_n = mesh.shape["rows"]
    feats_n = mesh.shape["feat"]

    def body(train, test, fw, rw, up, down):
        width = fw.shape[-1]
        quad = train.shape[1] // width
        heads = width // HD
        n_train, n_test = train.shape[0], test.shape[0]
        cell_rows = n_train + n_test
        groups_n = rows_n // quad
        half = groups_n // 2
        span = quad * n_train
        keys = min(groups_n, 4) * span
        packed = cell_rows * width // 128
        vmem = pltpu.VMEM
        dma = pltpu.SemaphoreType.DMA
        vspec = pl.BlockSpec(memory_space=pltpu.VMEM)
        aspec = pl.BlockSpec(memory_space=pl.ANY)
        weights = (fw, rw, up, down.T)
        place_fn = place
        fits = groups_n == 4 and quad == 4 and feats_n == 2
        if fits and n_train % 32 == 0 and n_test % 32 == 0:
            body_fn, place_fn = plane_kernel, place_halves
            n_half, n_quart = n_train // 2, n_test // 2
            swapped = [vmem((n_half, quad * width), BF), vmem((n_quart, quad * width), BF)]
            both = 2 * quad
            pair = both * 16
            lines = heads * (HD + 16)
            early, late = 2 * n_train + quad * n_test, 2 * n_train
            work = [
                vmem((width, heads * early), BF),
                vmem((width, heads * late), BF),
                vmem((width, early), F32),
                vmem((width, late), F32),
                vmem(fw.shape, BF),
                vmem((both * n_half, width), BF),
                vmem((both * n_half, width), BF),
                vmem((both * n_quart, width), BF),
                vmem((both * n_quart, width), BF),
                vmem((width, heads * both * n_half), BF),
                vmem((both * n_half, width), BF),
                vmem((lines, both * n_half), BF),
                vmem((both * n_half, heads * pair), F32),
                vmem((both * n_half, heads * pair), BF),
                vmem((width, both * n_half), BF),
                vmem(rw.shape, BF),
                vmem((heads * width, width), BF),
                vmem(up.shape[::-1], BF),
                vmem((2 * span, heads * early), F32),
                vmem((2 * span, heads * late), F32),
                vmem((2 * span, heads * early), BF),
                vmem((2 * span, heads * late), BF),
                vmem((heads * (HD + 16), early), F32),
                vmem((heads * (HD + 16), late), F32),
                vmem((8, heads * early), F32),
                vmem((8, heads * late), F32),
                vmem((2, span, width), BF),
                vmem((2, heads * (HD + 16), span), BF),
                vmem((up.shape[1], early), F32),
                vmem((up.shape[1], early), BF),
            ]
            boxes = [
                vmem((2, quad, n_train * width // 256, 128), BF),
                vmem((2, quad, n_train * width // 256, 128), BF),
                vmem((2, quad, n_train * width // 256, 128), BF),
                vmem((2, quad, n_test * width // 256, 128), BF),
                vmem((2, quad, n_test * width // 256, 128), BF),
                vmem((3, 2, quad, n_train * width // 256, 128), BF),
            ]
            flags = [
                dma((2,)),
                dma((2,)),
                dma((2, 2)),
                dma((2, 2)),
                dma((2,)),
                dma((3, 2)),
                dma((1,)),
                dma((1,)),
                pltpu.SemaphoreType.REGULAR((2,)),
            ]
        else:
            body_fn = kernel
            swapped = [vmem(train.shape, BF), vmem(test.shape, BF)]
            work = [
                vmem((heads, quad * cell_rows, keys), F32),
                vmem((keys, 256), BF),
                vmem((heads, quad * cell_rows, width), BF),
            ]
            boxes = [
                vmem((2, quad, n_train * width // 256, 128), BF),
                vmem((2, quad, n_train * width // 256, 128), BF),
                vmem((quad, n_test * width // 128, 128), BF),
                vmem((quad, n_test * width // 128, 128), BF),
                vmem((groups_n, 2, span * width // 256, 128), BF),
            ]
            flags = [
                dma((3,)),
                dma((3,)),
                dma((3, quad)),
                dma((3, quad)),
                dma((2, half, 2)),
                dma((2, half, 2)),
                dma((quad,)),
                dma((quad,)),
            ]
        back = pl.pallas_call(
            functools.partial(body_fn, rows_n, feats_n),
            out_shape=pltpu.VMEM((quad, packed, 128), BF),
            in_specs=[aspec, aspec, aspec, aspec, aspec, aspec],
            out_specs=vspec,
            scratch_shapes=[
                *(vmem(w.shape, BF) for w in weights),
                vmem(train.shape, BF),
                vmem(test.shape, BF),
                *swapped,
                *boxes,
                *work,
                vmem((quad, packed, 128), BF),
                dma((6,)),
                *flags,
            ],
            compiler_params=pltpu.CompilerParams(
                collective_id=0, has_side_effects=True, vmem_limit_bytes=60 * 1024 * 1024
            ),
            name="layer",
        )(train, test, *weights)
        return pl.pallas_call(
            place_fn,
            out_shape=(
                jax.ShapeDtypeStruct(train.shape, BF),
                jax.ShapeDtypeStruct(test.shape, BF),
            ),
            in_specs=[vspec],
            out_specs=(vspec, vspec),
            name="place",
        )(pltpu.with_memory_space_constraint(back, pltpu.VMEM))

    return jax.shard_map(
        body,
        mesh=mesh,
        in_specs=(P("rows", "feat"), P("rows", "feat"), P(), P(), P(), P()),
        out_specs=(P("rows", "feat"), P("rows", "feat")),
        check_vma=False,
    )
```

```python
import functools

import jax
import jax.numpy as jnp
from jax import lax
from jax.experimental import pallas as pl
from jax.experimental.pallas import tpu as pltpu
from jax.sharding import PartitionSpec as P

HD = 32
EPS = 1e-05
LOG2E = 1.4426950408889634
MESH = pl.DeviceIdType.MESH
BF = jnp.bfloat16
F32 = jnp.float32


def layer_norm(x):
    centred = x - jnp.mean(x, axis=-1, keepdims=True)
    spread = jnp.mean(centred * centred, axis=-1, keepdims=True)
    return centred * lax.rsqrt(spread + EPS)


def dot(a, b):
    return jnp.dot(a, b, preferred_element_type=F32)


def dot_t(a, b):
    return lax.dot_general(a, b, (((1,), (1,)), ((), ())), preferred_element_type=F32)


def pack(x):
    n = x.shape[0]
    low = jnp.concatenate([x[: n // 2, 128:], x[n // 2 :, 128:]], axis=1)
    return jnp.concatenate([x[:, :128], low], axis=0)


def unpack(p):
    n = p.shape[0] * 2 // 3
    low = p[n:]
    high = jnp.concatenate([low[:, :64], low[:, 64:]], axis=0)
    return jnp.concatenate([p[:n], high], axis=1)


def gelu(x):
    return 0.5 * x * (1.0 + lax.erf(x * (0.5**0.5)))


def kernel(
    rows_n,
    feats_n,
    train_hbm,
    test_hbm,
    fw_hbm,
    rw_hbm,
    up_hbm,
    down_hbm,
    back_in,
    fw,
    rw,
    up,
    down,
    train_ref,
    test_ref,
    o_train,
    o_test,
    outbox,
    inbox,
    t_outbox,
    t_inbox,
    ring,
    scores,
    values,
    queries,
    back_out,
    w_sem,
    f_send,
    f_recv,
    q_send,
    q_recv,
    r_send,
    r_recv,
    b_send,
    b_recv,
):
    width = fw.shape[-1]
    quad = t_outbox.shape[0]
    heads = width // HD
    groups_n = rows_n // quad
    half = groups_n // 2
    n_train = train_ref.shape[0]
    n_test = test_ref.shape[0]
    n_half = n_train // 2
    scale = LOG2E * HD ** (-0.5)

    my_row = lax.axis_index("rows")
    my_feat = lax.axis_index("feat")
    member = lax.rem(my_row, quad)
    group = my_row // quad

    def partner(k):
        low, high = lax.rem(member, 2), member // 2
        return (1 - high if k // 2 else high) * 2 + (1 - low if k % 2 else low)

    def mate(k):
        return group * quad + partner(k)

    right = lax.rem(group + 1, groups_n) * quad + member
    left = lax.rem(group + groups_n - 1, groups_n) * quad + member
    other = lax.rem(my_feat + 1, feats_n)

    loads = [
        pltpu.make_async_copy(s, d, w_sem.at[i])
        for i, (s, d) in enumerate(
            [
                (train_hbm, train_ref),
                (fw_hbm, fw),
                (test_hbm, test_ref),
                (rw_hbm, rw),
                (up_hbm, up),
                (down_hbm, down),
            ]
        )
    ]
    for c in loads:
        c.start()

    barrier = pltpu.get_barrier_semaphore()
    pl.semaphore_signal(barrier, inc=1, device_id={"feat": other}, device_id_type=MESH)
    for k in range(1, quad):
        pl.semaphore_signal(barrier, inc=1, device_id={"rows": mate(k)}, device_id_type=MESH)
    for d in (right, left):
        pl.semaphore_signal(barrier, inc=1, device_id={"rows": d}, device_id_type=MESH)
    pl.semaphore_wait(barrier, quad + 2)

    halves = [pl.ds(p * n_half, n_half) for p in range(2)]
    swaps = [
        pltpu.make_async_remote_copy(
            src_ref=s,
            dst_ref=d,
            send_sem=f_send.at[i],
            recv_sem=f_recv.at[i],
            device_id={"feat": other},
            device_id_type=MESH,
        )
        for i, (s, d) in enumerate(
            [(train_hbm.at[r], o_train.at[r]) for r in halves] + [(test_hbm, o_test)]
        )
    ]
    for c in swaps:
        c.start()

    def feature_rows(table):
        return jnp.concatenate(
            [table[:, f * width : (f + 1) * width].astype(F32) for f in range(quad)], axis=0
        )

    def split(x):
        n = x.shape[0] // quad
        return [x[f * n : (f + 1) * n] for f in range(quad)]

    def key_value(normed):
        return split(dot(normed, fw[1]).astype(BF)), split(dot(normed, fw[2]).astype(BF))

    same = (
        lax.broadcasted_iota(jnp.int32, (width, width), 0) // HD
        == lax.broadcasted_iota(jnp.int32, (width, width), 1) // HD
    )
    spread = jnp.where(same, 1.0, 0.0).astype(BF)

    def own_side(table):
        cells = feature_rows(table)
        normed = layer_norm(cells).astype(BF)
        q = split((dot(normed, fw[0]) * scale).astype(BF))
        ks, vs = key_value(normed)
        return cells, q, ks, vs

    def feature_attention(own, table):
        cells, q, ks, vs = own
        n = table.shape[0]
        more_k, more_v = key_value(layer_norm(feature_rows(table)).astype(BF))
        ks, vs = ks + more_k, vs + more_v
        mixes = []
        for f in range(quad):
            prod = jnp.concatenate([q[f] * k for k in ks], axis=0)
            s = dot(prod, spread)
            s = [s[g * n : (g + 1) * n] for g in range(len(ks))]
            top = functools.reduce(jnp.maximum, s)
            total = None
            mix = None
            for g in range(len(ks)):
                e = jnp.exp2(s[g] - top)
                t = e * vs[g].astype(F32)
                total = e if total is None else total + e
                mix = t if mix is None else mix + t
            mixes.append((mix / total).astype(BF))
        feat_out = dot(jnp.concatenate(mixes, axis=0), fw[3])
        return split((cells + feat_out).astype(BF))

    def to_mates(box, landing, stage):
        copies = {}
        for k in (2, 3, 1):
            copies[k] = pltpu.make_async_remote_copy(
                src_ref=box.at[partner(k)],
                dst_ref=landing.at[k],
                send_sem=q_send.at[stage, k],
                recv_sem=q_recv.at[stage, k],
                device_id={"rows": mate(k)},
                device_id_type=MESH,
            )
            copies[k].start()
        landing[0] = box[member]
        return copies

    loads[0].wait()
    loads[1].wait()
    own = [own_side(train_ref[p * n_half : (p + 1) * n_half]) for p in range(2)]
    moved = []
    boxes = [(outbox.at[p], inbox.at[p]) for p in range(2)] + [(t_outbox, t_inbox)]
    for p in range(2):
        swaps[p].wait()
        for f, x in enumerate(feature_attention(own[p], o_train[p * n_half : (p + 1) * n_half])):
            outbox[p, f] = pack(x)
        moved.append(to_mates(*boxes[p], p))
    loads[2].wait()
    own_test = own_side(test_ref[...])
    swaps[2].wait()
    for f, x in enumerate(feature_attention(own_test, o_test[...])):
        t_outbox[f] = pack(x)
    moved.append(to_mates(*boxes[2], 2))

    def hop(way, h, p):
        last = h == half - 1
        src = 0 if h == 0 else 2 * h - 1 + way
        dst = 2 * half - 1 if last else 1 + 2 * h + way
        return pltpu.make_async_remote_copy(
            src_ref=ring.at[src, p],
            dst_ref=ring.at[dst, p],
            send_sem=r_send.at[way, h, p],
            recv_sem=r_recv.at[way, h, p],
            device_id={"rows": left if way else right},
            device_id_type=MESH,
        )

    def pieces(way, h):
        return (way,) if h == half - 1 else (way, 1 - way)

    hops = {}
    after = []
    normed = []

    def arrive(stage):
        for k in range(1, quad):
            moved[stage][k].wait_recv()
        landing = boxes[stage][1]
        after.append(
            jnp.concatenate([unpack(landing[k]) for k in range(quad)], axis=0).astype(F32)
        )
        normed.append(layer_norm(after[stage]).astype(BF))

    for p in range(2):
        arrive(p)
        ring[0, p] = pack(normed[p])
        for way in (p, 1 - p):
            if p in pieces(way, 0):
                hops[way, 0, p] = hop(way, 0, p)
                hops[way, 0, p].start()

    loads[3].wait()
    lane_head = lax.broadcasted_iota(jnp.int32, (1, width), 1) // HD
    n_query = quad * (n_train + n_test)
    n_side = n_query // 2
    sizes = [2 * n_half, 2 * n_half, 2 * n_test]
    begins = [0, 2 * n_half, 4 * n_half]
    all_rows = [slice(0, n_query)]
    train_rows = [slice(i * n_side, i * n_side + begins[2]) for i in range(2)]
    test_rows = [slice(i * n_side + begins[2], (i + 1) * n_side) for i in range(2)]
    span = quad * n_train
    values[:, width:] = jnp.ones_like(values[:, width:])

    def ask(stage):
        q_all = (dot(normed[stage], rw[0]) * scale).astype(BF)
        n = sizes[stage]
        for h in range(heads):
            one = jnp.where(lane_head == h, q_all, jnp.zeros_like(q_all))
            for i in range(2):
                at = i * n_side + begins[stage]
                queries[h, at : at + n] = one[(1 - i) * n : (2 - i) * n]

    def take(slot, column):
        x = jnp.concatenate([unpack(ring[slot, 0]), unpack(ring[slot, 1])], axis=0)
        values[column * span : (column + 1) * span, :width] = dot(x, rw[2]).astype(BF)
        return dot(x, rw[1]).astype(BF)

    def score(key, column, rows):
        for h in range(heads):
            for r in rows:
                scores[h, r, column * span : (column + 1) * span] = dot_t(queries[h, r], key)

    def attend(h, rows, columns, carried):
        s = scores[h, rows, columns]
        top = jnp.max(s, axis=-1, keepdims=True)
        if carried is not None:
            top = jnp.maximum(top, carried[0])
        e = jnp.exp2(s - top).astype(BF)
        out = dot(e, values[columns])
        if carried is not None:
            out = out + carried[1] * jnp.exp2(carried[0] - top)
        return top, out

    ask(0)
    ask(1)
    everything = slice(0, n_query)
    if half <= 2:
        own_key = take(0, 0)
        score(own_key, 0, train_rows)
    arrive(2)
    ask(2)
    if half <= 2:
        score(own_key, 0, test_rows)
        states = [attend(h, everything, slice(0, span), None) for h in range(heads)]

    for h in range(half - 1):
        for way in range(2):
            for p in pieces(way, h + 1):
                hops[way, h, p].wait_recv()
                hops[way, h + 1, p] = hop(way, h + 1, p)
                hops[way, h + 1, p].start()
        for way in range(2):
            for p in pieces(way, h):
                if p not in pieces(way, h + 1):
                    hops[way, h, p].wait_recv()

    if half == 2:
        for slot in (1, 2):
            score(take(slot, slot), slot, all_rows)
        states = [
            attend(h, everything, slice(span, 3 * span), states[h]) for h in range(heads)
        ]

    for way in range(2):
        for p in pieces(way, half - 1):
            hops[way, half - 1, p].wait_recv()

    if half <= 2:
        last = 2 * half - 1
        last_key = take(last, last)
        columns = slice(last * span, (last + 1) * span)
    else:
        per = scores.shape[2] // span

        def step(i, states):
            for j in range(per):
                score(take(i * per + j, j), j, all_rows)
            return [attend(h, everything, slice(0, per * span), states[h]) for h in range(heads)]

        start = [
            (
                jnp.full((n_query, 1), -1e30, F32),
                jnp.zeros((n_query, values.shape[1]), F32),
            )
            for _ in range(heads)
        ]
        states = lax.fori_loop(0, groups_n // per, step, start)

    for c in loads[4:]:
        c.wait()
    returns = []
    for i, pair in enumerate(((2, 3), (0, 1))):
        rows = slice(i * n_side, (i + 1) * n_side)
        side = [tuple(x[rows] for x in states[h]) for h in range(heads)]
        if half <= 2:
            score(last_key, last, [rows])
            side = [attend(h, rows, columns, side[h]) for h in range(heads)]
        mixed = None
        for h in range(heads):
            out = side[h][1]
            part = out[:, :width] * (1.0 / out[:, width : width + 1])
            mixed = part if h == 0 else jnp.where(lane_head == h, part, mixed)
        before = [x[(1 - i) * n : (2 - i) * n] for x, n in zip(after, sizes)]
        after_row = jnp.concatenate(before, axis=0) + dot(mixed.astype(BF), rw[3])
        hidden = gelu(dot(layer_norm(after_row).astype(BF), up[...])).astype(BF)
        done = (after_row + dot_t(hidden, down[...])).astype(BF)
        for j, k in enumerate(pair):
            block = pack(
                jnp.concatenate(
                    [
                        done[b + j * (n // 2) : b + (j + 1) * (n // 2)]
                        for b, n in zip(begins, sizes)
                    ],
                    axis=0,
                )
            )
            back_out[k] = block
            if k == 0:
                c = pltpu.make_async_copy(back_out.at[0], back_in.at[member], b_send.at[0])
                c.start()
                returns.append(c)
                continue
            c = pltpu.make_async_remote_copy(
                src_ref=back_out.at[k],
                dst_ref=back_in.at[member],
                send_sem=b_send.at[k],
                recv_sem=b_recv.at[k],
                device_id={"rows": mate(k)},
                device_id_type=MESH,
            )
            c.start()
            returns.append(c)
    for c in returns:
        c.wait()
    for c in [*hops.values(), *(c for m in moved for c in m.values())]:
        c.wait_send()


def unpack_blocks(p):
    n = p.shape[1] * 2 // 3
    count = p.shape[0]
    low = p[:, n:]
    high = jnp.concatenate([low[:, :, :64], low[:, :, 64:]], axis=1)
    first = p[:, :n].reshape(count * n, 128)
    return jnp.concatenate([first, high.reshape(count * n, 64)], axis=1)


def plane_kernel(
    rows_n,
    feats_n,
    train_hbm,
    test_hbm,
    fw_hbm,
    rw_hbm,
    up_hbm,
    down_hbm,
    back_in,
    fw,
    rw,
    up,
    down,
    train_ref,
    test_ref,
    o_train,
    o_test,
    zbox,
    abox,
    a_in,
    t_box,
    t_in,
    ring,
    early_q,
    late_q,
    early_x,
    late_x,
    fw_t,
    f_cells,
    f_x,
    t_cells,
    t_x,
    fq,
    fk,
    fv,
    fs,
    fe,
    fm,
    rw_t,
    asks,
    up_t,
    early_s,
    late_s,
    early_e,
    late_e,
    early_sum,
    late_sum,
    early_top,
    late_top,
    keys,
    vals,
    raised,
    hidden,
    back_out,
    w_sem,
    f_send,
    f_recv,
    a_send,
    a_recv,
    r_send,
    r_recv,
    b_send,
    b_recv,
    gate,
):
    width = fw.shape[-1]
    quad = t_box.shape[1]
    heads = width // HD
    groups_n = rows_n // quad
    n_train = train_ref.shape[0]
    n_test = test_ref.shape[0]
    n_half, n_quart = n_train // 2, n_test // 2
    scale = LOG2E * HD ** (-0.5)

    my_row = lax.axis_index("rows")
    my_feat = lax.axis_index("feat")
    member = lax.rem(my_row, quad)
    group = my_row // quad

    def partner(k):
        low, high = lax.rem(member, 2), member // 2
        return (1 - high if k // 2 else high) * 2 + (1 - low if k % 2 else low)

    def mate(k):
        return group * quad + partner(k)

    right_group = lax.rem(group + 1, groups_n)
    left_group = lax.rem(group + groups_n - 1, groups_n)
    right = right_group * quad + member
    left = left_group * quad + member
    other = lax.rem(my_feat + 1, feats_n)

    loads = [
        pltpu.make_async_copy(s, d, w_sem.at[i])
        for i, (s, d) in enumerate(
            [
                (train_hbm, train_ref),
                (fw_hbm, fw),
                (test_hbm, test_ref),
                (rw_hbm, rw),
                (up_hbm, up),
                (down_hbm, down),
            ]
        )
    ]
    for c in loads:
        c.start()

    barrier = pltpu.get_barrier_semaphore()
    even = lax.rem(member, 2) == 0

    def greet(**where):
        pl.semaphore_signal(barrier, inc=1, device_id=where, device_id_type=MESH)

    def tell(i):
        pl.semaphore_signal(
            gate.at[i], inc=1, device_id={"rows": mate(1)}, device_id_type=MESH
        )

    @pl.when(even)
    def _():
        greet(rows=my_row, feat=other)
        for g in (group, right_group, left_group):
            for m in range(1, quad, 2):
                for y in (my_feat, other):
                    greet(rows=g * quad + m, feat=y)
        pl.semaphore_wait(barrier, 3)
        tell(0)

    @pl.when(jnp.logical_not(even))
    def _():
        greet(rows=mate(1))
        greet(rows=mate(1), feat=other)
        greet(rows=my_row, feat=other)
        for y in (my_feat, other):
            greet(rows=mate(2), feat=y)
            for g in (right_group, left_group):
                for m in range(1, quad, 2):
                    greet(rows=g * quad + m, feat=y)
        pl.semaphore_wait(gate.at[0], 1)

    swaps = [
        pltpu.make_async_remote_copy(
            src_ref=s,
            dst_ref=d,
            send_sem=f_send.at[i],
            recv_sem=f_recv.at[i],
            device_id={"feat": other},
            device_id_type=MESH,
        )
        for i, (s, d) in enumerate(
            [
                (train_ref.at[pl.ds(pl.multiple_of(other * n_half, n_half), n_half)], o_train),
                (test_ref.at[pl.ds(pl.multiple_of(other * n_quart, n_quart), n_quart)], o_test),
            ]
        )
    ]
    for i in range(2):
        loads[2 * i].wait()
        swaps[i].start()

    tile = 16
    cell = quad * tile
    pair = 2 * cell
    lines = HD + 16
    same_row = (
        lax.broadcasted_iota(jnp.int32, (pair, heads * pair), 0) % tile
        == lax.broadcasted_iota(jnp.int32, (pair, heads * pair), 1) % tile
    )

    def fill(table, side, cells_ref, x_ref):
        n = table.shape[0] // tile
        cells = jnp.concatenate(
            [
                table[b * tile : (b + 1) * tile, f * width : (f + 1) * width].astype(F32)
                for b in range(n)
                for f in range(quad)
            ],
            axis=0,
        )
        normed = layer_norm(cells).astype(BF)
        for b in range(n):
            to = slice((2 * b + side) * cell, (2 * b + side + 1) * cell)
            cells_ref[to] = cells[b * cell : (b + 1) * cell].astype(BF)
            x_ref[to] = normed[b * cell : (b + 1) * cell]

    def normed_columns(x):
        centred = x - jnp.mean(x, axis=0, keepdims=True)
        spread = jnp.mean(centred * centred, axis=0, keepdims=True)
        return centred * lax.rsqrt(spread + EPS)

    def feature_attention(cells_ref, x_ref):
        n = x_ref.shape[0]
        blocks = [slice(b * pair, (b + 1) * pair) for b in range(n // pair)]
        x = x_ref[...]
        q = (dot_t(fw_t[0], x) * scale).astype(BF)
        fk[:n] = dot(x, fw[1]).astype(BF)
        v = dot_t(fw_t[2], x).astype(BF)
        for h in range(heads):
            rows = slice(h * HD, (h + 1) * HD)
            fv[h * lines : h * lines + HD, :n] = v[rows]
            for b, at in enumerate(blocks):
                fq[rows, (b * heads + h) * pair : (b * heads + h + 1) * pair] = q[rows, at]
        for b, at in enumerate(blocks):
            fs[at] = dot(fk[at], fq[:, b * heads * pair : (b + 1) * heads * pair])
        for at in blocks:
            s = jnp.where(same_row, fs[at], -1e30)
            fe[at] = jnp.exp2(s - jnp.max(s, axis=0, keepdims=True)).astype(BF)
        for at in blocks:
            for h in range(heads):
                out = dot(
                    fv[h * lines : (h + 1) * lines, at], fe[at, h * pair : (h + 1) * pair]
                )
                part = out[:HD] * (1.0 / out[HD : HD + 1])
                fm[h * HD : (h + 1) * HD, at] = part.astype(BF)
        after = cells_ref[...].T.astype(F32) + dot(fw_t[3], fm[:, :n])
        return after, normed_columns(after)

    def sides(x):
        n = x.shape[0] // pair
        for j in range(2):
            for f in range(quad):
                at = [(2 * b + j) * cell + f * tile for b in range(n)]
                yield j, f, jnp.concatenate([x[i : i + tile] for i in at], axis=0)

    feats = (my_feat, other)

    def to_mates(box, landing, stage):
        copies = []
        for k, j in ((2, 0), (0, 1), (3, 0), (1, 1), (2, 1), (3, 1), (1, 0)):
            pltpu.make_async_remote_copy(
                src_ref=box.at[j, partner(k)],
                dst_ref=landing.at[j, k],
                send_sem=a_send.at[stage, j],
                recv_sem=a_recv.at[stage, j],
                device_id={"rows": mate(k), "feat": feats[j]},
                device_id_type=MESH,
            ).start()
        landing[0, 0] = box[0, member]
        return [
            pltpu.make_async_remote_copy(
                src_ref=part,
                dst_ref=part,
                send_sem=a_send.at[stage, j],
                recv_sem=a_recv.at[stage, j],
                device_id={"rows": mate(1)},
                device_id_type=MESH,
            )
            for j, part in enumerate((landing.at[0, pl.ds(1, quad - 1)], landing.at[1]))
        ]

    inner = jnp.logical_and(group > 0, group < groups_n - 1)

    def to_group(way, p, k):
        g = jnp.where(way == 1, left_group, right_group)
        return pltpu.make_async_remote_copy(
            src_ref=zbox.at[p, partner(k)],
            dst_ref=ring.at[way, p, k],
            send_sem=r_send.at[0],
            recv_sem=r_recv.at[way, p],
            device_id={"rows": g * quad + partner(k), "feat": feats[p]},
            device_id_type=MESH,
        )

    def whole(slot, p):
        return pltpu.make_async_remote_copy(
            src_ref=ring.at[slot, p],
            dst_ref=ring.at[slot, p],
            send_sem=r_send.at[0],
            recv_sem=r_recv.at[slot, p],
            device_id={"rows": right},
            device_id_type=MESH,
        )

    def onward(way, p):
        return pltpu.make_async_remote_copy(
            src_ref=ring.at[way, p],
            dst_ref=ring.at[2, p],
            send_sem=r_send.at[1],
            recv_sem=r_recv.at[2, p],
            device_id={"rows": left if way else right},
            device_id_type=MESH,
        )

    def relay(p):
        @pl.when(inner)
        def _():
            for way in (1, 0):
                whole(way, p).wait_recv()
                onward(way, p).start()

    loads[1].wait()
    fill(train_ref[pl.ds(pl.multiple_of(my_feat * n_half, n_half), n_half)], 0, f_cells, f_x)
    for i in (0, 2, 3):
        fw_t[i] = fw[i].astype(F32).T.astype(BF)
    fill(test_ref[pl.ds(pl.multiple_of(my_feat * n_quart, n_quart), n_quart)], 0, t_cells, t_x)
    fq[...] = jnp.zeros_like(fq)
    fv[...] = jnp.ones_like(fv)

    @pl.when(jnp.logical_not(even))
    def _():
        pl.semaphore_wait(barrier, 6 * quad - 1)
        tell(1)

    swaps[0].wait()
    fill(o_train[...], 1, f_cells, f_x)
    after_own, normed_own = feature_attention(f_cells, f_x)
    for j, f, x in sides(normed_own.astype(BF).T):
        zbox[j, f] = pack(x)

    @pl.when(even)
    def _():
        pl.semaphore_wait(gate.at[1], 1)

    near = jnp.where(group >= 1, 1, 0)
    at_end = group == groups_n - 1

    @pl.when(at_end)
    def _():
        for k in range(quad):
            pltpu.make_async_remote_copy(
                src_ref=zbox.at[my_feat, partner(k)],
                dst_ref=ring.at[0, my_feat, k],
                send_sem=r_send.at[0],
                recv_sem=r_recv.at[0, my_feat],
                device_id={"rows": right_group * quad + partner(k), "feat": 0},
                device_id_type=MESH,
            ).start()

    for k in range(2):
        to_group(near, 0, k).start()
    for j, f, x in sides(after_own.astype(BF).T):
        abox[j, f] = pack(x)
    moved = [to_mates(abox, a_in, 0)]
    for way in (near, 1 - near):
        for p in range(2):
            for k in range(quad):
                if way is near:
                    if p or k > 1:
                        to_group(way, p, k).start()
                    continue

                @pl.when(jnp.logical_not(jnp.logical_and(at_end, my_feat == p)))
                def _():
                    to_group(way, p, k).start()
    swaps[1].wait()
    fill(o_test[...], 1, t_cells, t_x)
    after_own, _ = feature_attention(t_cells, t_x)
    for j, f, x in sides(after_own.astype(BF).T):
        t_box[j, f] = pack(x)
    moved.append(to_mates(t_box, t_in, 1))

    loads[3].wait()
    for i in (2, 3):
        rw_t[i] = rw[i].astype(F32).T.astype(BF)
    lane_head = lax.broadcasted_iota(jnp.int32, (1, width), 1) // HD
    for h in range(heads):
        one = jnp.where(lane_head == h, rw[1], jnp.zeros_like(rw[1]))
        asks[h * width : (h + 1) * width] = (dot_t(one, rw[0]) * scale).astype(BF)
    loads[4].wait()
    up_t[...] = up[...].astype(F32).T.astype(BF)
    vals[...] = jnp.ones_like(vals)

    def arrived(landing):
        return [unpack(landing[j, k]) for k in range(quad) for j in range(2)]

    n_mid = 2 * n_train
    n_late = 2 * n_train
    n_early = n_mid + quad * n_test

    def place_queries(q, into, size, at):
        n = q.shape[1]
        for h in range(heads):
            into[:, h * size + at : h * size + at + n] = q[h * width : (h + 1) * width]

    late = (late_q, late_s, late_e, late_sum, late_top, n_late)
    early = (early_q, early_s, early_e, early_sum, early_top, n_early)

    def key_value_rows(x, i, begin=0):
        to = slice(begin, begin + x.shape[0])
        keys[i, to] = x
        value = dot_t(rw_t[2], x).astype(BF)
        for h in range(heads):
            vals[i, h * lines : h * lines + HD, to] = value[h * HD : (h + 1) * HD]

    span = quad * n_train

    def attend(asked, slots, first=False):
        per_head = [
            (part, h, slice(h * part[5], (h + 1) * part[5]), slice(h * lines, (h + 1) * lines))
            for part in asked
            for h in range(heads)
        ]
        spans = []
        for _, own in slots:
            begin = spans[-1].stop if spans else 0
            spans.append(slice(begin, begin + own.stop - own.start))
        for at, (i, own) in zip(spans, slots):
            key = keys[i, own]
            for (q, s, _, _, _, _), h, c, _ in per_head:
                s[at, c] = dot(key, q[:, c])
        whole_span = slice(0, spans[-1].stop)
        for (_, s, e, total, tops, _), h, c, r in per_head:
            top = jnp.max(s[whole_span, c], axis=0, keepdims=True)
            if not first:
                old = tops[0:1, c]
                top = jnp.maximum(top, old)
                total[r] = total[r] * jnp.exp2(old - top)
            e[whole_span, c] = jnp.exp2(s[whole_span, c] - top).astype(BF)
            tops[0:1, c] = top
        for (_, _, e, total, _, _), h, c, r in per_head:
            out = None if first else total[r]
            for at, (i, own) in zip(spans, slots):
                part = dot(vals[i, r, own], e[at, c])
                out = part if out is None else out + part
            total[r] = out

    def finish(part, before):
        total = part[3]
        mix = jnp.concatenate(
            [
                total[h * lines : h * lines + HD]
                * (1.0 / total[h * lines + HD : h * lines + HD + 1])
                for h in range(heads)
            ],
            axis=0,
        ).astype(BF)
        after_row = before + dot(rw_t[3], mix)
        normed = normed_columns(after_row).astype(BF)
        n = normed.shape[1]
        step = width
        for i in range(up_t.shape[0] // step):
            at = slice(i * step, (i + 1) * step)
            raised[at, :n] = dot(up_t[at], normed)
            hidden[at, :n] = gelu(raised[at, :n]).astype(BF)
        return (after_row + dot(down[...], hidden[:, :n])).astype(BF).T

    at_start = group == 0
    order = (jnp.where(at_start, 1, 0), jnp.where(at_start, 0, 1), 2)

    def landed(i):
        slot = order[i]

        @pl.when(jnp.logical_not(jnp.logical_and(inner, slot < 2)))
        def _():
            for p in range(2):
                whole(slot, p).wait_recv()

    def fetch(i):
        slot = order[i]
        x = jnp.concatenate([unpack_blocks(ring[slot, p]) for p in range(2)], axis=0)
        key_value_rows(x, (i + 1) % 2)

    relay(0)
    relay(1)
    for c in [*moved[0], *moved[1]]:
        c.wait_recv()
    landed(0)
    x = jnp.concatenate(arrived(a_in) + arrived(t_in), axis=0)
    early_x[...] = x[n_late:].T.astype(F32)
    late_x[...] = x[:n_late].T.astype(F32)
    for part, into, n in ((early_x, early_q, n_early), (late_x, late_q, n_late)):
        columns = normed_columns(part[...]).astype(BF)
        place_queries(dot(asks[...], columns).astype(BF), into, n, 0)
    key_value_rows(layer_norm(x[: quad * n_train].astype(F32)).astype(BF), 0)
    fetch(0)
    every = slice(0, span)
    attend([late, early], ((0, every), (1, every)), True)
    landed(1)
    fetch(1)
    attend([late, early], ((0, every),))
    halves = [(1, slice(p * span // 2, (p + 1) * span // 2)) for p in range(2)]

    @pl.when(at_start)
    def _():
        for p, half in enumerate(halves):
            whole(2, p).wait_recv()
            key_value_rows(unpack_blocks(ring[2, p]), 1, half[1].start)
            attend([early] if p else [late, early], (half,))

    @pl.when(jnp.logical_not(at_start))
    def _():
        landed(2)
        fetch(2)
        attend([early], ((1, every),))

    loads[5].wait()

    def give_back(k, done, tests):
        block = jnp.concatenate([done, tests[k * n_test : (k + 1) * n_test]], axis=0)
        if k == 0:
            back_in[member] = pack(block)
            return
        back_out[k] = pack(block)
        pltpu.make_async_remote_copy(
            src_ref=back_out.at[k],
            dst_ref=back_in.at[member],
            send_sem=b_send.at[0],
            recv_sem=b_recv.at[0],
            device_id={"rows": mate(k)},
            device_id_type=MESH,
        ).start()

    done = finish(early, early_x[...])
    tests = done[n_mid:]
    for k in (2, 3):
        give_back(k, done[(k - 2) * n_train : (k - 1) * n_train], tests)

    @pl.when(at_start)
    def _():
        attend([late], (halves[1],))

    @pl.when(jnp.logical_not(at_start))
    def _():
        attend([late], ((1, every),))

    done = finish(late, late_x[...])
    for k in (1, 0):
        give_back(k, done[k * n_train : (k + 1) * n_train], tests)
    returned = pltpu.make_async_remote_copy(
        src_ref=back_out.at[pl.ds(1, quad - 1)],
        dst_ref=back_in.at[pl.ds(1, quad - 1)],
        send_sem=b_send.at[0],
        recv_sem=b_recv.at[0],
        device_id={"rows": mate(1)},
        device_id_type=MESH,
    )
    returned.wait()
    for c in [*moved[0], *moved[1]]:
        c.wait_send()

    def sent(i):
        pltpu.make_async_remote_copy(
            src_ref=ring.at[pl.ds(0, 2)],
            dst_ref=ring.at[pl.ds(0, 2)],
            send_sem=r_send.at[i],
            recv_sem=r_recv.at[0, 0],
            device_id={"rows": right},
            device_id_type=MESH,
        ).wait_send()

    sent(0)

    @pl.when(inner)
    def _():
        sent(1)


def place_halves(back_ref, train_out, test_out):
    quad = back_ref.shape[0]
    result = jnp.concatenate([unpack(back_ref[f]) for f in range(quad)], axis=1)
    mine = lax.axis_index("feat")
    begin = 0
    for out in (train_out, test_out):
        half = out.shape[0] // 2
        for j, place_of in enumerate((mine, 1 - mine)):
            to = pl.ds(pl.multiple_of(place_of * half, half), half)
            out[to] = result[begin + j * half : begin + (j + 1) * half]
        begin += 2 * half


def place(back_ref, train_out, test_out):
    quad = back_ref.shape[0]
    result = jnp.concatenate([unpack(back_ref[f]) for f in range(quad)], axis=1)
    n_train = train_out.shape[0]
    train_out[...] = result[:n_train]
    test_out[...] = result[n_train:]


def solution(mesh):
    rows_n = mesh.shape["rows"]
    feats_n = mesh.shape["feat"]

    def body(train, test, fw, rw, up, down):
        width = fw.shape[-1]
        quad = train.shape[1] // width
        heads = width // HD
        n_train, n_test = train.shape[0], test.shape[0]
        cell_rows = n_train + n_test
        groups_n = rows_n // quad
        half = groups_n // 2
        span = quad * n_train
        keys = min(groups_n, 4) * span
        packed = cell_rows * width // 128
        vmem = pltpu.VMEM
        dma = pltpu.SemaphoreType.DMA
        vspec = pl.BlockSpec(memory_space=pltpu.VMEM)
        aspec = pl.BlockSpec(memory_space=pl.ANY)
        weights = (fw, rw, up, down.T)
        place_fn = place
        fits = groups_n == 4 and quad == 4 and feats_n == 2
        if fits and n_train % 32 == 0 and n_test % 32 == 0:
            body_fn, place_fn = plane_kernel, place_halves
            n_half, n_quart = n_train // 2, n_test // 2
            swapped = [vmem((n_half, quad * width), BF), vmem((n_quart, quad * width), BF)]
            both = 2 * quad
            pair = both * 16
            lines = heads * (HD + 16)
            early, late = 2 * n_train + quad * n_test, 2 * n_train
            work = [
                vmem((width, heads * early), BF),
                vmem((width, heads * late), BF),
                vmem((width, early), F32),
                vmem((width, late), F32),
                vmem(fw.shape, BF),
                vmem((both * n_half, width), BF),
                vmem((both * n_half, width), BF),
                vmem((both * n_quart, width), BF),
                vmem((both * n_quart, width), BF),
                vmem((width, heads * both * n_half), BF),
                vmem((both * n_half, width), BF),
                vmem((lines, both * n_half), BF),
                vmem((both * n_half, heads * pair), F32),
                vmem((both * n_half, heads * pair), BF),
                vmem((width, both * n_half), BF),
                vmem(rw.shape, BF),
                vmem((heads * width, width), BF),
                vmem(up.shape[::-1], BF),
                vmem((2 * span, heads * early), F32),
                vmem((2 * span, heads * late), F32),
                vmem((2 * span, heads * early), BF),
                vmem((2 * span, heads * late), BF),
                vmem((heads * (HD + 16), early), F32),
                vmem((heads * (HD + 16), late), F32),
                vmem((8, heads * early), F32),
                vmem((8, heads * late), F32),
                vmem((2, span, width), BF),
                vmem((2, heads * (HD + 16), span), BF),
                vmem((up.shape[1], early), F32),
                vmem((up.shape[1], early), BF),
            ]
            boxes = [
                vmem((2, quad, n_train * width // 256, 128), BF),
                vmem((2, quad, n_train * width // 256, 128), BF),
                vmem((2, quad, n_train * width // 256, 128), BF),
                vmem((2, quad, n_test * width // 256, 128), BF),
                vmem((2, quad, n_test * width // 256, 128), BF),
                vmem((3, 2, quad, n_train * width // 256, 128), BF),
            ]
            flags = [
                dma((2,)),
                dma((2,)),
                dma((2, 2)),
                dma((2, 2)),
                dma((2,)),
                dma((3, 2)),
                dma((1,)),
                dma((1,)),
                pltpu.SemaphoreType.REGULAR((2,)),
            ]
        else:
            body_fn = kernel
            swapped = [vmem(train.shape, BF), vmem(test.shape, BF)]
            work = [
                vmem((heads, quad * cell_rows, keys), F32),
                vmem((keys, 256), BF),
                vmem((heads, quad * cell_rows, width), BF),
            ]
            boxes = [
                vmem((2, quad, n_train * width // 256, 128), BF),
                vmem((2, quad, n_train * width // 256, 128), BF),
                vmem((quad, n_test * width // 128, 128), BF),
                vmem((quad, n_test * width // 128, 128), BF),
                vmem((groups_n, 2, span * width // 256, 128), BF),
            ]
            flags = [
                dma((3,)),
                dma((3,)),
                dma((3, quad)),
                dma((3, quad)),
                dma((2, half, 2)),
                dma((2, half, 2)),
                dma((quad,)),
                dma((quad,)),
            ]
        back = pl.pallas_call(
            functools.partial(body_fn, rows_n, feats_n),
            out_shape=pltpu.VMEM((quad, packed, 128), BF),
            in_specs=[aspec, aspec, aspec, aspec, aspec, aspec],
            out_specs=vspec,
            scratch_shapes=[
                *(vmem(w.shape, BF) for w in weights),
                vmem(train.shape, BF),
                vmem(test.shape, BF),
                *swapped,
                *boxes,
                *work,
                vmem((quad, packed, 128), BF),
                dma((6,)),
                *flags,
            ],
            compiler_params=pltpu.CompilerParams(
                collective_id=0, has_side_effects=True, vmem_limit_bytes=60 * 1024 * 1024
            ),
            name="layer",
        )(train, test, *weights)
        return pl.pallas_call(
            place_fn,
            out_shape=(
                jax.ShapeDtypeStruct(train.shape, BF),
                jax.ShapeDtypeStruct(test.shape, BF),
            ),
            in_specs=[vspec],
            out_specs=(vspec, vspec),
            name="place",
        )(pltpu.with_memory_space_constraint(back, pltpu.VMEM))

    return jax.shard_map(
        body,
        mesh=mesh,
        in_specs=(P("rows", "feat"), P("rows", "feat"), P(), P(), P(), P()),
        out_specs=(P("rows", "feat"), P("rows", "feat")),
        check_vma=False,
    )
```

```python
import functools

import jax
import jax.numpy as jnp
from jax import lax
from jax.experimental import pallas as pl
from jax.experimental.pallas import tpu as pltpu
from jax.sharding import PartitionSpec as P

HD = 32
EPS = 1e-05
LOG2E = 1.4426950408889634
MESH = pl.DeviceIdType.MESH
BF = jnp.bfloat16
F32 = jnp.float32


def layer_norm(x):
    centred = x - jnp.mean(x, axis=-1, keepdims=True)
    spread = jnp.mean(centred * centred, axis=-1, keepdims=True)
    return centred * lax.rsqrt(spread + EPS)


def dot(a, b):
    return jnp.dot(a, b, preferred_element_type=F32)


def dot_t(a, b):
    return lax.dot_general(a, b, (((1,), (1,)), ((), ())), preferred_element_type=F32)


def pack(x):
    n = x.shape[0]
    low = jnp.concatenate([x[: n // 2, 128:], x[n // 2 :, 128:]], axis=1)
    return jnp.concatenate([x[:, :128], low], axis=0)


def unpack(p):
    n = p.shape[0] * 2 // 3
    low = p[n:]
    high = jnp.concatenate([low[:, :64], low[:, 64:]], axis=0)
    return jnp.concatenate([p[:n], high], axis=1)


def gelu(x):
    return 0.5 * x * (1.0 + lax.erf(x * (0.5**0.5)))


def kernel(
    rows_n,
    feats_n,
    train_hbm,
    test_hbm,
    fw_hbm,
    rw_hbm,
    up_hbm,
    down_hbm,
    back_in,
    fw,
    rw,
    up,
    down,
    train_ref,
    test_ref,
    o_train,
    o_test,
    outbox,
    inbox,
    t_outbox,
    t_inbox,
    ring,
    scores,
    values,
    queries,
    back_out,
    w_sem,
    f_send,
    f_recv,
    q_send,
    q_recv,
    r_send,
    r_recv,
    b_send,
    b_recv,
):
    width = fw.shape[-1]
    quad = t_outbox.shape[0]
    heads = width // HD
    groups_n = rows_n // quad
    half = groups_n // 2
    n_train = train_ref.shape[0]
    n_test = test_ref.shape[0]
    n_half = n_train // 2
    scale = LOG2E * HD ** (-0.5)

    my_row = lax.axis_index("rows")
    my_feat = lax.axis_index("feat")
    member = lax.rem(my_row, quad)
    group = my_row // quad

    def partner(k):
        low, high = lax.rem(member, 2), member // 2
        return (1 - high if k // 2 else high) * 2 + (1 - low if k % 2 else low)

    def mate(k):
        return group * quad + partner(k)

    right = lax.rem(group + 1, groups_n) * quad + member
    left = lax.rem(group + groups_n - 1, groups_n) * quad + member
    other = lax.rem(my_feat + 1, feats_n)

    loads = [
        pltpu.make_async_copy(s, d, w_sem.at[i])
        for i, (s, d) in enumerate(
            [
                (train_hbm, train_ref),
                (fw_hbm, fw),
                (test_hbm, test_ref),
                (rw_hbm, rw),
                (up_hbm, up),
                (down_hbm, down),
            ]
        )
    ]
    for c in loads:
        c.start()

    barrier = pltpu.get_barrier_semaphore()
    pl.semaphore_signal(barrier, inc=1, device_id={"feat": other}, device_id_type=MESH)
    for k in range(1, quad):
        pl.semaphore_signal(barrier, inc=1, device_id={"rows": mate(k)}, device_id_type=MESH)
    for d in (right, left):
        pl.semaphore_signal(barrier, inc=1, device_id={"rows": d}, device_id_type=MESH)
    pl.semaphore_wait(barrier, quad + 2)

    halves = [pl.ds(p * n_half, n_half) for p in range(2)]
    swaps = [
        pltpu.make_async_remote_copy(
            src_ref=s,
            dst_ref=d,
            send_sem=f_send.at[i],
            recv_sem=f_recv.at[i],
            device_id={"feat": other},
            device_id_type=MESH,
        )
        for i, (s, d) in enumerate(
            [(train_hbm.at[r], o_train.at[r]) for r in halves] + [(test_hbm, o_test)]
        )
    ]
    for c in swaps:
        c.start()

    def feature_rows(table):
        return jnp.concatenate(
            [table[:, f * width : (f + 1) * width].astype(F32) for f in range(quad)], axis=0
        )

    def split(x):
        n = x.shape[0] // quad
        return [x[f * n : (f + 1) * n] for f in range(quad)]

    def key_value(normed):
        return split(dot(normed, fw[1]).astype(BF)), split(dot(normed, fw[2]).astype(BF))

    same = (
        lax.broadcasted_iota(jnp.int32, (width, width), 0) // HD
        == lax.broadcasted_iota(jnp.int32, (width, width), 1) // HD
    )
    spread = jnp.where(same, 1.0, 0.0).astype(BF)

    def own_side(table):
        cells = feature_rows(table)
        normed = layer_norm(cells).astype(BF)
        q = split((dot(normed, fw[0]) * scale).astype(BF))
        ks, vs = key_value(normed)
        return cells, q, ks, vs

    def feature_attention(own, table):
        cells, q, ks, vs = own
        n = table.shape[0]
        more_k, more_v = key_value(layer_norm(feature_rows(table)).astype(BF))
        ks, vs = ks + more_k, vs + more_v
        mixes = []
        for f in range(quad):
            prod = jnp.concatenate([q[f] * k for k in ks], axis=0)
            s = dot(prod, spread)
            s = [s[g * n : (g + 1) * n] for g in range(len(ks))]
            top = functools.reduce(jnp.maximum, s)
            total = None
            mix = None
            for g in range(len(ks)):
                e = jnp.exp2(s[g] - top)
                t = e * vs[g].astype(F32)
                total = e if total is None else total + e
                mix = t if mix is None else mix + t
            mixes.append((mix / total).astype(BF))
        feat_out = dot(jnp.concatenate(mixes, axis=0), fw[3])
        return split((cells + feat_out).astype(BF))

    def to_mates(box, landing, stage):
        copies = {}
        for k in (2, 3, 1):
            copies[k] = pltpu.make_async_remote_copy(
                src_ref=box.at[partner(k)],
                dst_ref=landing.at[k],
                send_sem=q_send.at[stage, k],
                recv_sem=q_recv.at[stage, k],
                device_id={"rows": mate(k)},
                device_id_type=MESH,
            )
            copies[k].start()
        landing[0] = box[member]
        return copies

    loads[0].wait()
    loads[1].wait()
    own = [own_side(train_ref[p * n_half : (p + 1) * n_half]) for p in range(2)]
    moved = []
    boxes = [(outbox.at[p], inbox.at[p]) for p in range(2)] + [(t_outbox, t_inbox)]
    for p in range(2):
        swaps[p].wait()
        for f, x in enumerate(feature_attention(own[p], o_train[p * n_half : (p + 1) * n_half])):
            outbox[p, f] = pack(x)
        moved.append(to_mates(*boxes[p], p))
    loads[2].wait()
    own_test = own_side(test_ref[...])
    swaps[2].wait()
    for f, x in enumerate(feature_attention(own_test, o_test[...])):
        t_outbox[f] = pack(x)
    moved.append(to_mates(*boxes[2], 2))

    def hop(way, h, p):
        last = h == half - 1
        src = 0 if h == 0 else 2 * h - 1 + way
        dst = 2 * half - 1 if last else 1 + 2 * h + way
        return pltpu.make_async_remote_copy(
            src_ref=ring.at[src, p],
            dst_ref=ring.at[dst, p],
            send_sem=r_send.at[way, h, p],
            recv_sem=r_recv.at[way, h, p],
            device_id={"rows": left if way else right},
            device_id_type=MESH,
        )

    def pieces(way, h):
        return (way,) if h == half - 1 else (way, 1 - way)

    hops = {}
    after = []
    normed = []

    def arrive(stage):
        for k in range(1, quad):
            moved[stage][k].wait_recv()
        landing = boxes[stage][1]
        after.append(
            jnp.concatenate([unpack(landing[k]) for k in range(quad)], axis=0).astype(F32)
        )
        normed.append(layer_norm(after[stage]).astype(BF))

    for p in range(2):
        arrive(p)
        ring[0, p] = pack(normed[p])
        for way in (p, 1 - p):
            if p in pieces(way, 0):
                hops[way, 0, p] = hop(way, 0, p)
                hops[way, 0, p].start()

    loads[3].wait()
    lane_head = lax.broadcasted_iota(jnp.int32, (1, width), 1) // HD
    n_query = quad * (n_train + n_test)
    n_side = n_query // 2
    sizes = [2 * n_half, 2 * n_half, 2 * n_test]
    begins = [0, 2 * n_half, 4 * n_half]
    all_rows = [slice(0, n_query)]
    train_rows = [slice(i * n_side, i * n_side + begins[2]) for i in range(2)]
    test_rows = [slice(i * n_side + begins[2], (i + 1) * n_side) for i in range(2)]
    span = quad * n_train
    values[:, width:] = jnp.ones_like(values[:, width:])

    def ask(stage):
        q_all = (dot(normed[stage], rw[0]) * scale).astype(BF)
        n = sizes[stage]
        for h in range(heads):
            one = jnp.where(lane_head == h, q_all, jnp.zeros_like(q_all))
            for i in range(2):
                at = i * n_side + begins[stage]
                queries[h, at : at + n] = one[(1 - i) * n : (2 - i) * n]

    def take(slot, column):
        x = jnp.concatenate([unpack(ring[slot, 0]), unpack(ring[slot, 1])], axis=0)
        values[column * span : (column + 1) * span, :width] = dot(x, rw[2]).astype(BF)
        return dot(x, rw[1]).astype(BF)

    def score(key, column, rows):
        for h in range(heads):
            for r in rows:
                scores[h, r, column * span : (column + 1) * span] = dot_t(queries[h, r], key)

    def attend(h, rows, columns, carried):
        s = scores[h, rows, columns]
        top = jnp.max(s, axis=-1, keepdims=True)
        if carried is not None:
            top = jnp.maximum(top, carried[0])
        e = jnp.exp2(s - top).astype(BF)
        out = dot(e, values[columns])
        if carried is not None:
            out = out + carried[1] * jnp.exp2(carried[0] - top)
        return top, out

    ask(0)
    ask(1)
    everything = slice(0, n_query)
    if half <= 2:
        own_key = take(0, 0)
        score(own_key, 0, train_rows)
    arrive(2)
    ask(2)
    if half <= 2:
        score(own_key, 0, test_rows)
        states = [attend(h, everything, slice(0, span), None) for h in range(heads)]

    for h in range(half - 1):
        for way in range(2):
            for p in pieces(way, h + 1):
                hops[way, h, p].wait_recv()
                hops[way, h + 1, p] = hop(way, h + 1, p)
                hops[way, h + 1, p].start()
        for way in range(2):
            for p in pieces(way, h):
                if p not in pieces(way, h + 1):
                    hops[way, h, p].wait_recv()

    if half == 2:
        for slot in (1, 2):
            score(take(slot, slot), slot, all_rows)
        states = [
            attend(h, everything, slice(span, 3 * span), states[h]) for h in range(heads)
        ]

    for way in range(2):
        for p in pieces(way, half - 1):
            hops[way, half - 1, p].wait_recv()

    if half <= 2:
        last = 2 * half - 1
        last_key = take(last, last)
        columns = slice(last * span, (last + 1) * span)
    else:
        per = scores.shape[2] // span

        def step(i, states):
            for j in range(per):
                score(take(i * per + j, j), j, all_rows)
            return [attend(h, everything, slice(0, per * span), states[h]) for h in range(heads)]

        start = [
            (
                jnp.full((n_query, 1), -1e30, F32),
                jnp.zeros((n_query, values.shape[1]), F32),
            )
            for _ in range(heads)
        ]
        states = lax.fori_loop(0, groups_n // per, step, start)

    for c in loads[4:]:
        c.wait()
    returns = []
    for i, pair in enumerate(((2, 3), (0, 1))):
        rows = slice(i * n_side, (i + 1) * n_side)
        side = [tuple(x[rows] for x in states[h]) for h in range(heads)]
        if half <= 2:
            score(last_key, last, [rows])
            side = [attend(h, rows, columns, side[h]) for h in range(heads)]
        mixed = None
        for h in range(heads):
            out = side[h][1]
            part = out[:, :width] * (1.0 / out[:, width : width + 1])
            mixed = part if h == 0 else jnp.where(lane_head == h, part, mixed)
        before = [x[(1 - i) * n : (2 - i) * n] for x, n in zip(after, sizes)]
        after_row = jnp.concatenate(before, axis=0) + dot(mixed.astype(BF), rw[3])
        hidden = gelu(dot(layer_norm(after_row).astype(BF), up[...])).astype(BF)
        done = (after_row + dot_t(hidden, down[...])).astype(BF)
        for j, k in enumerate(pair):
            block = pack(
                jnp.concatenate(
                    [
                        done[b + j * (n // 2) : b + (j + 1) * (n // 2)]
                        for b, n in zip(begins, sizes)
                    ],
                    axis=0,
                )
            )
            back_out[k] = block
            if k == 0:
                c = pltpu.make_async_copy(back_out.at[0], back_in.at[member], b_send.at[0])
                c.start()
                returns.append(c)
                continue
            c = pltpu.make_async_remote_copy(
                src_ref=back_out.at[k],
                dst_ref=back_in.at[member],
                send_sem=b_send.at[k],
                recv_sem=b_recv.at[k],
                device_id={"rows": mate(k)},
                device_id_type=MESH,
            )
            c.start()
            returns.append(c)
    for c in returns:
        c.wait()
    for c in [*hops.values(), *(c for m in moved for c in m.values())]:
        c.wait_send()


def unpack_blocks(p):
    n = p.shape[1] * 2 // 3
    count = p.shape[0]
    low = p[:, n:]
    high = jnp.concatenate([low[:, :, :64], low[:, :, 64:]], axis=1)
    first = p[:, :n].reshape(count * n, 128)
    return jnp.concatenate([first, high.reshape(count * n, 64)], axis=1)


def plane_kernel(
    rows_n,
    feats_n,
    train_hbm,
    test_hbm,
    fw_hbm,
    rw_hbm,
    up_hbm,
    down_hbm,
    back_in,
    fw,
    rw,
    up,
    down,
    train_ref,
    test_ref,
    o_train,
    o_test,
    zbox,
    abox,
    a_in,
    t_box,
    t_in,
    ring,
    early_q,
    late_q,
    early_x,
    late_x,
    fw_t,
    f_cells,
    f_x,
    t_cells,
    t_x,
    fq,
    fk,
    fv,
    fs,
    fe,
    fm,
    rw_t,
    asks,
    up_t,
    early_s,
    late_s,
    early_e,
    late_e,
    early_sum,
    late_sum,
    early_top,
    late_top,
    keys,
    vals,
    raised,
    hidden,
    back_out,
    w_sem,
    f_send,
    f_recv,
    a_send,
    a_recv,
    r_send,
    r_recv,
    b_send,
    b_recv,
    gate,
):
    width = fw.shape[-1]
    quad = t_box.shape[1]
    heads = width // HD
    groups_n = rows_n // quad
    n_train = train_ref.shape[0]
    n_test = test_ref.shape[0]
    n_half, n_quart = n_train // 2, n_test // 2
    scale = LOG2E * HD ** (-0.5)

    my_row = lax.axis_index("rows")
    my_feat = lax.axis_index("feat")
    member = lax.rem(my_row, quad)
    group = my_row // quad

    def partner(k):
        low, high = lax.rem(member, 2), member // 2
        return (1 - high if k // 2 else high) * 2 + (1 - low if k % 2 else low)

    def mate(k):
        return group * quad + partner(k)

    right_group = lax.rem(group + 1, groups_n)
    left_group = lax.rem(group + groups_n - 1, groups_n)
    right = right_group * quad + member
    left = left_group * quad + member
    other = lax.rem(my_feat + 1, feats_n)

    loads = [
        pltpu.make_async_copy(s, d, w_sem.at[i])
        for i, (s, d) in enumerate(
            [
                (train_hbm, train_ref),
                (fw_hbm, fw),
                (test_hbm, test_ref),
                (rw_hbm, rw),
                (up_hbm, up),
                (down_hbm, down),
            ]
        )
    ]
    for c in loads:
        c.start()

    barrier = pltpu.get_barrier_semaphore()
    even = lax.rem(member, 2) == 0

    def greet(**where):
        pl.semaphore_signal(barrier, inc=1, device_id=where, device_id_type=MESH)

    def tell(i):
        pl.semaphore_signal(
            gate.at[i], inc=1, device_id={"rows": mate(1)}, device_id_type=MESH
        )

    @pl.when(even)
    def _():
        greet(rows=my_row, feat=other)
        for g in (group, right_group, left_group):
            for m in range(1, quad, 2):
                for y in (my_feat, other):
                    greet(rows=g * quad + m, feat=y)
        pl.semaphore_wait(barrier, 3)
        tell(0)

    @pl.when(jnp.logical_not(even))
    def _():
        greet(rows=mate(1))
        greet(rows=mate(1), feat=other)
        greet(rows=my_row, feat=other)
        for y in (my_feat, other):
            greet(rows=mate(2), feat=y)
            for g in (right_group, left_group):
                for m in range(1, quad, 2):
                    greet(rows=g * quad + m, feat=y)
        pl.semaphore_wait(gate.at[0], 1)

    swaps = [
        pltpu.make_async_remote_copy(
            src_ref=s,
            dst_ref=d,
            send_sem=f_send.at[i],
            recv_sem=f_recv.at[i],
            device_id={"feat": other},
            device_id_type=MESH,
        )
        for i, (s, d) in enumerate(
            [
                (train_ref.at[pl.ds(pl.multiple_of(other * n_half, n_half), n_half)], o_train),
                (test_ref.at[pl.ds(pl.multiple_of(other * n_quart, n_quart), n_quart)], o_test),
            ]
        )
    ]
    loads[0].wait()
    swaps[0].start()

    tile = 16
    cell = quad * tile
    pair = 2 * cell
    lines = HD + 16
    same_row = (
        lax.broadcasted_iota(jnp.int32, (pair, heads * pair), 0) % tile
        == lax.broadcasted_iota(jnp.int32, (pair, heads * pair), 1) % tile
    )

    def fill(table, side, cells_ref, x_ref):
        n = table.shape[0] // tile
        cells = jnp.concatenate(
            [
                table[b * tile : (b + 1) * tile, f * width : (f + 1) * width].astype(F32)
                for b in range(n)
                for f in range(quad)
            ],
            axis=0,
        )
        normed = layer_norm(cells).astype(BF)
        for b in range(n):
            to = slice((2 * b + side) * cell, (2 * b + side + 1) * cell)
            cells_ref[to] = cells[b * cell : (b + 1) * cell].astype(BF)
            x_ref[to] = normed[b * cell : (b + 1) * cell]

    def normed_columns(x):
        centred = x - jnp.mean(x, axis=0, keepdims=True)
        spread = jnp.mean(centred * centred, axis=0, keepdims=True)
        return centred * lax.rsqrt(spread + EPS)

    def feature_attention(cells_ref, x_ref):
        n = x_ref.shape[0]
        blocks = [slice(b * pair, (b + 1) * pair) for b in range(n // pair)]
        x = x_ref[...]
        q = (dot_t(fw_t[0], x) * scale).astype(BF)
        fk[:n] = dot(x, fw[1]).astype(BF)
        v = dot_t(fw_t[2], x).astype(BF)
        for h in range(heads):
            rows = slice(h * HD, (h + 1) * HD)
            fv[h * lines : h * lines + HD, :n] = v[rows]
            for b, at in enumerate(blocks):
                fq[rows, (b * heads + h) * pair : (b * heads + h + 1) * pair] = q[rows, at]
        for b, at in enumerate(blocks):
            fs[at] = dot(fk[at], fq[:, b * heads * pair : (b + 1) * heads * pair])
        for at in blocks:
            s = jnp.where(same_row, fs[at], -1e30)
            fe[at] = jnp.exp2(s - jnp.max(s, axis=0, keepdims=True)).astype(BF)
        for at in blocks:
            for h in range(heads):
                out = dot(
                    fv[h * lines : (h + 1) * lines, at], fe[at, h * pair : (h + 1) * pair]
                )
                part = out[:HD] * (1.0 / out[HD : HD + 1])
                fm[h * HD : (h + 1) * HD, at] = part.astype(BF)
        after = cells_ref[...].T.astype(F32) + dot(fw_t[3], fm[:, :n])
        return after, normed_columns(after)

    def sides(x):
        n = x.shape[0] // pair
        for j in range(2):
            for f in range(quad):
                at = [(2 * b + j) * cell + f * tile for b in range(n)]
                yield j, f, jnp.concatenate([x[i : i + tile] for i in at], axis=0)

    feats = (my_feat, other)

    def to_mates(box, landing, stage):
        copies = []
        for k, j in ((2, 0), (0, 1), (3, 0), (1, 1), (2, 1), (3, 1), (1, 0)):
            pltpu.make_async_remote_copy(
                src_ref=box.at[j, partner(k)],
                dst_ref=landing.at[j, k],
                send_sem=a_send.at[stage, j],
                recv_sem=a_recv.at[stage, j],
                device_id={"rows": mate(k), "feat": feats[j]},
                device_id_type=MESH,
            ).start()
        landing[0, 0] = box[0, member]
        return [
            pltpu.make_async_remote_copy(
                src_ref=part,
                dst_ref=part,
                send_sem=a_send.at[stage, j],
                recv_sem=a_recv.at[stage, j],
                device_id={"rows": mate(1)},
                device_id_type=MESH,
            )
            for j, part in enumerate((landing.at[0, pl.ds(1, quad - 1)], landing.at[1]))
        ]

    inner = jnp.logical_and(group > 0, group < groups_n - 1)

    def to_group(way, p, k):
        g = jnp.where(way == 1, left_group, right_group)
        return pltpu.make_async_remote_copy(
            src_ref=zbox.at[p, partner(k)],
            dst_ref=ring.at[way, p, k],
            send_sem=r_send.at[0],
            recv_sem=r_recv.at[way, p],
            device_id={"rows": g * quad + partner(k), "feat": feats[p]},
            device_id_type=MESH,
        )

    def whole(slot, p):
        return pltpu.make_async_remote_copy(
            src_ref=ring.at[slot, p],
            dst_ref=ring.at[slot, p],
            send_sem=r_send.at[0],
            recv_sem=r_recv.at[slot, p],
            device_id={"rows": right},
            device_id_type=MESH,
        )

    def onward(way, p):
        return pltpu.make_async_remote_copy(
            src_ref=ring.at[way, p],
            dst_ref=ring.at[2, p],
            send_sem=r_send.at[1],
            recv_sem=r_recv.at[2, p],
            device_id={"rows": left if way else right},
            device_id_type=MESH,
        )

    def relay(p):
        @pl.when(inner)
        def _():
            for way in (1, 0):
                whole(way, p).wait_recv()
                onward(way, p).start()

    loads[1].wait()
    fill(train_ref[pl.ds(pl.multiple_of(my_feat * n_half, n_half), n_half)], 0, f_cells, f_x)
    for i in (0, 2, 3):
        fw_t[i] = fw[i].astype(F32).T.astype(BF)
    loads[2].wait()
    swaps[1].start()
    fill(test_ref[pl.ds(pl.multiple_of(my_feat * n_quart, n_quart), n_quart)], 0, t_cells, t_x)
    fq[...] = jnp.zeros_like(fq)
    fv[...] = jnp.ones_like(fv)

    @pl.when(jnp.logical_not(even))
    def _():
        pl.semaphore_wait(barrier, 6 * quad - 1)
        tell(1)

    swaps[0].wait()
    fill(o_train[...], 1, f_cells, f_x)
    after_own, normed_own = feature_attention(f_cells, f_x)
    for j, f, x in sides(normed_own.astype(BF).T):
        zbox[j, f] = pack(x)

    @pl.when(even)
    def _():
        pl.semaphore_wait(gate.at[1], 1)

    near = jnp.where(group >= 1, 1, 0)
    at_end = group == groups_n - 1

    @pl.when(at_end)
    def _():
        for k in range(quad):
            pltpu.make_async_remote_copy(
                src_ref=zbox.at[my_feat, partner(k)],
                dst_ref=ring.at[0, my_feat, k],
                send_sem=r_send.at[0],
                recv_sem=r_recv.at[0, my_feat],
                device_id={"rows": right_group * quad + partner(k), "feat": 0},
                device_id_type=MESH,
            ).start()

    for k in range(2):
        to_group(near, 0, k).start()
    for j, f, x in sides(after_own.astype(BF).T):
        abox[j, f] = pack(x)
    moved = [to_mates(abox, a_in, 0)]
    for way in (near, 1 - near):
        for p in range(2):
            for k in range(quad):
                if way is near:
                    if p or k > 1:
                        to_group(way, p, k).start()
                    continue

                @pl.when(jnp.logical_not(jnp.logical_and(at_end, my_feat == p)))
                def _():
                    to_group(way, p, k).start()
    swaps[1].wait()
    fill(o_test[...], 1, t_cells, t_x)
    after_own, _ = feature_attention(t_cells, t_x)
    for j, f, x in sides(after_own.astype(BF).T):
        t_box[j, f] = pack(x)
    moved.append(to_mates(t_box, t_in, 1))

    loads[3].wait()
    for i in (2, 3):
        rw_t[i] = rw[i].astype(F32).T.astype(BF)
    lane_head = lax.broadcasted_iota(jnp.int32, (1, width), 1) // HD
    for h in range(heads):
        one = jnp.where(lane_head == h, rw[1], jnp.zeros_like(rw[1]))
        asks[h * width : (h + 1) * width] = (dot_t(one, rw[0]) * scale).astype(BF)
    loads[4].wait()
    up_t[...] = up[...].astype(F32).T.astype(BF)
    vals[...] = jnp.ones_like(vals)

    def arrived(landing):
        return [unpack(landing[j, k]) for k in range(quad) for j in range(2)]

    n_mid = 2 * n_train
    n_late = 2 * n_train
    n_early = n_mid + quad * n_test

    def place_queries(q, into, size, at):
        n = q.shape[1]
        for h in range(heads):
            into[:, h * size + at : h * size + at + n] = q[h * width : (h + 1) * width]

    late = (late_q, late_s, late_e, late_sum, late_top, n_late)
    early = (early_q, early_s, early_e, early_sum, early_top, n_early)

    def key_value_rows(x, i, begin=0):
        to = slice(begin, begin + x.shape[0])
        keys[i, to] = x
        value = dot_t(rw_t[2], x).astype(BF)
        for h in range(heads):
            vals[i, h * lines : h * lines + HD, to] = value[h * HD : (h + 1) * HD]

    span = quad * n_train

    def attend(asked, slots, first=False):
        per_head = [
            (part, h, slice(h * part[5], (h + 1) * part[5]), slice(h * lines, (h + 1) * lines))
            for part in asked
            for h in range(heads)
        ]
        spans = []
        for _, own in slots:
            begin = spans[-1].stop if spans else 0
            spans.append(slice(begin, begin + own.stop - own.start))
        for at, (i, own) in zip(spans, slots):
            key = keys[i, own]
            for (q, s, _, _, _, _), h, c, _ in per_head:
                s[at, c] = dot(key, q[:, c])
        whole_span = slice(0, spans[-1].stop)
        for (_, s, e, total, tops, _), h, c, r in per_head:
            top = jnp.max(s[whole_span, c], axis=0, keepdims=True)
            if not first:
                old = tops[0:1, c]
                top = jnp.maximum(top, old)
                total[r] = total[r] * jnp.exp2(old - top)
            e[whole_span, c] = jnp.exp2(s[whole_span, c] - top).astype(BF)
            tops[0:1, c] = top
        for (_, _, e, total, _, _), h, c, r in per_head:
            out = None if first else total[r]
            for at, (i, own) in zip(spans, slots):
                part = dot(vals[i, r, own], e[at, c])
                out = part if out is None else out + part
            total[r] = out

    def finish(part, before):
        total = part[3]
        mix = jnp.concatenate(
            [
                total[h * lines : h * lines + HD]
                * (1.0 / total[h * lines + HD : h * lines + HD + 1])
                for h in range(heads)
            ],
            axis=0,
        ).astype(BF)
        after_row = before + dot(rw_t[3], mix)
        normed = normed_columns(after_row).astype(BF)
        n = normed.shape[1]
        step = width
        for i in range(up_t.shape[0] // step):
            at = slice(i * step, (i + 1) * step)
            raised[at, :n] = dot(up_t[at], normed)
            hidden[at, :n] = gelu(raised[at, :n]).astype(BF)
        return (after_row + dot(down[...], hidden[:, :n])).astype(BF).T

    at_start = group == 0
    order = (jnp.where(at_start, 1, 0), jnp.where(at_start, 0, 1), 2)

    def landed(i):
        slot = order[i]

        @pl.when(jnp.logical_not(jnp.logical_and(inner, slot < 2)))
        def _():
            for p in range(2):
                whole(slot, p).wait_recv()

    def fetch(i):
        slot = order[i]
        x = jnp.concatenate([unpack_blocks(ring[slot, p]) for p in range(2)], axis=0)
        key_value_rows(x, (i + 1) % 2)

    relay(0)
    relay(1)
    for c in [*moved[0], *moved[1]]:
        c.wait_recv()
    landed(0)
    x = jnp.concatenate(arrived(a_in) + arrived(t_in), axis=0)
    early_x[...] = x[n_late:].T.astype(F32)
    late_x[...] = x[:n_late].T.astype(F32)
    for part, into, n in ((early_x, early_q, n_early), (late_x, late_q, n_late)):
        columns = normed_columns(part[...]).astype(BF)
        place_queries(dot(asks[...], columns).astype(BF), into, n, 0)
    key_value_rows(layer_norm(x[: quad * n_train].astype(F32)).astype(BF), 0)
    fetch(0)
    every = slice(0, span)
    attend([late, early], ((0, every), (1, every)), True)
    landed(1)
    fetch(1)
    attend([late, early], ((0, every),))
    halves = [(1, slice(p * span // 2, (p + 1) * span // 2)) for p in range(2)]

    @pl.when(at_start)
    def _():
        for p, half in enumerate(halves):
            whole(2, p).wait_recv()
            key_value_rows(unpack_blocks(ring[2, p]), 1, half[1].start)
            attend([early] if p else [late, early], (half,))

    @pl.when(jnp.logical_not(at_start))
    def _():
        landed(2)
        fetch(2)
        attend([early], ((1, every),))

    loads[5].wait()

    def give_back(k, done, tests):
        block = jnp.concatenate([done, tests[k * n_test : (k + 1) * n_test]], axis=0)
        if k == 0:
            back_in[member] = pack(block)
            return
        back_out[k] = pack(block)
        pltpu.make_async_remote_copy(
            src_ref=back_out.at[k],
            dst_ref=back_in.at[member],
            send_sem=b_send.at[0],
            recv_sem=b_recv.at[0],
            device_id={"rows": mate(k)},
            device_id_type=MESH,
        ).start()

    done = finish(early, early_x[...])
    tests = done[n_mid:]
    for k in (2, 3):
        give_back(k, done[(k - 2) * n_train : (k - 1) * n_train], tests)

    @pl.when(at_start)
    def _():
        attend([late], (halves[1],))

    @pl.when(jnp.logical_not(at_start))
    def _():
        attend([late], ((1, every),))

    done = finish(late, late_x[...])
    for k in (1, 0):
        give_back(k, done[k * n_train : (k + 1) * n_train], tests)
    returned = pltpu.make_async_remote_copy(
        src_ref=back_out.at[pl.ds(1, quad - 1)],
        dst_ref=back_in.at[pl.ds(1, quad - 1)],
        send_sem=b_send.at[0],
        recv_sem=b_recv.at[0],
        device_id={"rows": mate(1)},
        device_id_type=MESH,
    )
    returned.wait()
    for c in [*moved[0], *moved[1]]:
        c.wait_send()

    def sent(i):
        pltpu.make_async_remote_copy(
            src_ref=ring.at[pl.ds(0, 2)],
            dst_ref=ring.at[pl.ds(0, 2)],
            send_sem=r_send.at[i],
            recv_sem=r_recv.at[0, 0],
            device_id={"rows": right},
            device_id_type=MESH,
        ).wait_send()

    sent(0)

    @pl.when(inner)
    def _():
        sent(1)


def place_halves(back_ref, train_out, test_out):
    quad = back_ref.shape[0]
    result = jnp.concatenate([unpack(back_ref[f]) for f in range(quad)], axis=1)
    mine = lax.axis_index("feat")
    begin = 0
    for out in (train_out, test_out):
        half = out.shape[0] // 2
        for j, place_of in enumerate((mine, 1 - mine)):
            to = pl.ds(pl.multiple_of(place_of * half, half), half)
            out[to] = result[begin + j * half : begin + (j + 1) * half]
        begin += 2 * half


def place(back_ref, train_out, test_out):
    quad = back_ref.shape[0]
    result = jnp.concatenate([unpack(back_ref[f]) for f in range(quad)], axis=1)
    n_train = train_out.shape[0]
    train_out[...] = result[:n_train]
    test_out[...] = result[n_train:]


def solution(mesh):
    rows_n = mesh.shape["rows"]
    feats_n = mesh.shape["feat"]

    def body(train, test, fw, rw, up, down):
        width = fw.shape[-1]
        quad = train.shape[1] // width
        heads = width // HD
        n_train, n_test = train.shape[0], test.shape[0]
        cell_rows = n_train + n_test
        groups_n = rows_n // quad
        half = groups_n // 2
        span = quad * n_train
        keys = min(groups_n, 4) * span
        packed = cell_rows * width // 128
        vmem = pltpu.VMEM
        dma = pltpu.SemaphoreType.DMA
        vspec = pl.BlockSpec(memory_space=pltpu.VMEM)
        aspec = pl.BlockSpec(memory_space=pl.ANY)
        weights = (fw, rw, up, down.T)
        place_fn = place
        fits = groups_n == 4 and quad == 4 and feats_n == 2
        if fits and n_train % 32 == 0 and n_test % 32 == 0:
            body_fn, place_fn = plane_kernel, place_halves
            n_half, n_quart = n_train // 2, n_test // 2
            swapped = [vmem((n_half, quad * width), BF), vmem((n_quart, quad * width), BF)]
            both = 2 * quad
            pair = both * 16
            lines = heads * (HD + 16)
            early, late = 2 * n_train + quad * n_test, 2 * n_train
            work = [
                vmem((width, heads * early), BF),
                vmem((width, heads * late), BF),
                vmem((width, early), F32),
                vmem((width, late), F32),
                vmem(fw.shape, BF),
                vmem((both * n_half, width), BF),
                vmem((both * n_half, width), BF),
                vmem((both * n_quart, width), BF),
                vmem((both * n_quart, width), BF),
                vmem((width, heads * both * n_half), BF),
                vmem((both * n_half, width), BF),
                vmem((lines, both * n_half), BF),
                vmem((both * n_half, heads * pair), F32),
                vmem((both * n_half, heads * pair), BF),
                vmem((width, both * n_half), BF),
                vmem(rw.shape, BF),
                vmem((heads * width, width), BF),
                vmem(up.shape[::-1], BF),
                vmem((2 * span, heads * early), F32),
                vmem((2 * span, heads * late), F32),
                vmem((2 * span, heads * early), BF),
                vmem((2 * span, heads * late), BF),
                vmem((heads * (HD + 16), early), F32),
                vmem((heads * (HD + 16), late), F32),
                vmem((8, heads * early), F32),
                vmem((8, heads * late), F32),
                vmem((2, span, width), BF),
                vmem((2, heads * (HD + 16), span), BF),
                vmem((up.shape[1], early), F32),
                vmem((up.shape[1], early), BF),
            ]
            boxes = [
                vmem((2, quad, n_train * width // 256, 128), BF),
                vmem((2, quad, n_train * width // 256, 128), BF),
                vmem((2, quad, n_train * width // 256, 128), BF),
                vmem((2, quad, n_test * width // 256, 128), BF),
                vmem((2, quad, n_test * width // 256, 128), BF),
                vmem((3, 2, quad, n_train * width // 256, 128), BF),
            ]
            flags = [
                dma((2,)),
                dma((2,)),
                dma((2, 2)),
                dma((2, 2)),
                dma((2,)),
                dma((3, 2)),
                dma((1,)),
                dma((1,)),
                pltpu.SemaphoreType.REGULAR((2,)),
            ]
        else:
            body_fn = kernel
            swapped = [vmem(train.shape, BF), vmem(test.shape, BF)]
            work = [
                vmem((heads, quad * cell_rows, keys), F32),
                vmem((keys, 256), BF),
                vmem((heads, quad * cell_rows, width), BF),
            ]
            boxes = [
                vmem((2, quad, n_train * width // 256, 128), BF),
                vmem((2, quad, n_train * width // 256, 128), BF),
                vmem((quad, n_test * width // 128, 128), BF),
                vmem((quad, n_test * width // 128, 128), BF),
                vmem((groups_n, 2, span * width // 256, 128), BF),
            ]
            flags = [
                dma((3,)),
                dma((3,)),
                dma((3, quad)),
                dma((3, quad)),
                dma((2, half, 2)),
                dma((2, half, 2)),
                dma((quad,)),
                dma((quad,)),
            ]
        back = pl.pallas_call(
            functools.partial(body_fn, rows_n, feats_n),
            out_shape=pltpu.VMEM((quad, packed, 128), BF),
            in_specs=[aspec, aspec, aspec, aspec, aspec, aspec],
            out_specs=vspec,
            scratch_shapes=[
                *(vmem(w.shape, BF) for w in weights),
                vmem(train.shape, BF),
                vmem(test.shape, BF),
                *swapped,
                *boxes,
                *work,
                vmem((quad, packed, 128), BF),
                dma((6,)),
                *flags,
            ],
            compiler_params=pltpu.CompilerParams(
                collective_id=0, has_side_effects=True, vmem_limit_bytes=60 * 1024 * 1024
            ),
            name="layer",
        )(train, test, *weights)
        return pl.pallas_call(
            place_fn,
            out_shape=(
                jax.ShapeDtypeStruct(train.shape, BF),
                jax.ShapeDtypeStruct(test.shape, BF),
            ),
            in_specs=[vspec],
            out_specs=(vspec, vspec),
            name="place",
        )(pltpu.with_memory_space_constraint(back, pltpu.VMEM))

    return jax.shard_map(
        body,
        mesh=mesh,
        in_specs=(P("rows", "feat"), P("rows", "feat"), P(), P(), P(), P()),
        out_specs=(P("rows", "feat"), P("rows", "feat")),
        check_vma=False,
    )
```
